32 devices in a mesh: layer: 1 (over z), col: 4 (over y), row: 8 (over x, core).
Axes of the slice: x: 4, y: 4, z: 1, core: 2. Of those that a mesh axis runs over, the one named last changes fastest.
The devices are a block of a 4x4x8 slice.
Arguments:
- weight: float32 [1024, 4096], P(('layer', 'row'), 'col')
- grad_in: float32 [1024, 4096], P(('layer', 'row'), 'col')
- mom_first: float32 [1024, 4096], P(('layer', 'row'), 'col')
- mom_second: float32 [1024, 4096], P(('layer', 'row'), 'col')
- stat_left: float32 [1024, 1024], P(('layer', 'row'), 'col')
- stat_right: float32 [4096, 4096], P(('layer', 'row'), 'col')
- basis_left: float32 [1024, 1024], P(('layer', 'row'), 'col')
- basis_right: float32 [4096, 4096], P(('layer', 'row'), 'col')
Outputs:
- output 1: float32 [1024, 4096], P(('layer', 'row'), 'col')
- output 2: float32 [1024, 4096], P(('layer', 'row'), 'col')
- output 3: float32 [1024, 4096], P(('layer', 'row'), 'col')
- output 4: float32 [1024, 1024], P(('layer', 'row'), 'col')
- output 5: float32 [4096, 4096], P(('layer', 'row'), 'col')
All inputs are finite; a program needn't handle non-finite values.
Results may differ from the reference program's by a relative error of at most 0.001.
Values are sent between devices in bfloat16 or wider.
A program may use at most 768 MiB of HBM per device.

```python
import jax
import jax.numpy as jnp
from jax import lax

D = 1024
FF = 4096
STEP = 10
RANK = 16
FACTOR_SIDE = 16

BETA1 = 0.9
BETA2 = 0.9
EPS = 1e-8
LR = 0.1
BIAS_ONE = 1.0 - BETA1 ** STEP
BIAS_TWO = 1.0 - BETA2 ** STEP


def random_basis(base_key, matrix_order):
    sub_keys = jax.random.split(base_key, 5)
    side_b = matrix_order // FACTOR_SIDE
    outer_a = jnp.linalg.qr(jax.random.normal(sub_keys[0], (FACTOR_SIDE, FACTOR_SIDE), jnp.float32))[0]
    outer_b = jnp.linalg.qr(jax.random.normal(sub_keys[1], (side_b, side_b), jnp.float32))[0]
    inner_a = jnp.linalg.qr(jax.random.normal(sub_keys[2], (FACTOR_SIDE, FACTOR_SIDE), jnp.float32))[0]
    inner_b = jnp.linalg.qr(jax.random.normal(sub_keys[3], (side_b, side_b), jnp.float32))[0]
    col_order = jax.random.permutation(sub_keys[4], matrix_order)
    first_kron = jnp.kron(outer_a, outer_b)[:, col_order]
    blocks = first_kron.reshape(matrix_order, FACTOR_SIDE, side_b)
    mixed_basis = jnp.einsum("rst,sp,tq->rpq", blocks, inner_a, inner_b)
    return mixed_basis.reshape(matrix_order, matrix_order)


def setup_inputs(seed: int = 0, part: int = 0) -> dict:
    base_key = jax.random.fold_in(jax.random.key(seed), part)
    sub_keys = jax.random.split(base_key, 12)
    grad_scale = (10.0 / FF) ** 0.5
    noise_part = jax.random.normal(sub_keys[0], (D, FF), jnp.float32)
    left_fac = jax.random.normal(sub_keys[1], (D, RANK), jnp.float32)
    right_fac = jax.random.normal(sub_keys[2], (RANK, FF), jnp.float32)
    low_rank = jnp.dot(left_fac, right_fac) * (3.0 / RANK ** 0.5)
    grad_in = (noise_part + low_rank) * FF ** -0.5
    weight = 0.5 * jax.random.normal(sub_keys[3], (D, FF), jnp.float32)
    mom_first = 0.1 * grad_scale * jax.random.normal(sub_keys[4], (D, FF), jnp.float32)
    mom_second = 0.1 * grad_scale ** 2 * (0.25 + jax.random.normal(sub_keys[5], (D, FF), jnp.float32) ** 2)
    stat_fac_left = jax.random.normal(sub_keys[6], (D, RANK), jnp.float32)
    stat_left = 0.5 * ((9.0 / RANK) * jnp.dot(stat_fac_left, stat_fac_left.T) + jnp.eye(D, dtype=jnp.float32))
    stat_fac_right = jax.random.normal(sub_keys[7], (RANK, FF), jnp.float32)
    stat_right = 0.5 * (D / FF) * ((9.0 / RANK) * jnp.dot(stat_fac_right.T, stat_fac_right) + jnp.eye(FF, dtype=jnp.float32))
    basis_left = random_basis(sub_keys[8], D)
    basis_right = random_basis(sub_keys[9], FF)
    return {"weight": weight, "grad_in": grad_in, "mom_first": mom_first, "mom_second": mom_second, "stat_left": stat_left, "stat_right": stat_right, "basis_left": basis_left, "basis_right": basis_right}


def reference(weight, grad_in, mom_first, mom_second, stat_left, stat_right, basis_left, basis_right):
    highest = lax.Precision.HIGHEST
    new_left = BETA2 * stat_left + (1.0 - BETA2) * jnp.dot(grad_in, grad_in.T, precision=highest, preferred_element_type=jnp.float32)
    new_right = BETA2 * stat_right + (1.0 - BETA2) * jnp.dot(grad_in.T, grad_in, precision=highest, preferred_element_type=jnp.float32)
    left_bf = basis_left.astype(jnp.bfloat16)
    right_bf = basis_right.astype(jnp.bfloat16)
    inner_rot = jnp.dot(grad_in.astype(jnp.bfloat16), right_bf, preferred_element_type=jnp.float32).astype(jnp.bfloat16)
    rotated = jnp.dot(left_bf.T, inner_rot, preferred_element_type=jnp.float32)
    new_first = BETA1 * mom_first + (1.0 - BETA1) * rotated
    new_second = BETA2 * mom_second + (1.0 - BETA2) * rotated * rotated
    direction = (new_first / BIAS_ONE) / (jnp.sqrt(new_second / BIAS_TWO) + EPS)
    back_inner = jnp.dot(left_bf, direction.astype(jnp.bfloat16), preferred_element_type=jnp.float32).astype(jnp.bfloat16)
    step_update = jnp.dot(back_inner, right_bf.T, preferred_element_type=jnp.float32)
    new_weight = weight - LR * step_update
    return (new_weight, new_first, new_second, new_left, new_right)
```

```python
import functools

import jax
import jax.numpy as jnp
from jax import lax
from jax.experimental import pallas as pl
from jax.experimental.pallas import tpu as pltpu
from jax.sharding import PartitionSpec as P

BETA1 = 0.9
BETA2 = 0.9
EPS = 1e-8
LR = 0.1
STEP = 10
BIAS_ONE = 1.0 - BETA1 ** STEP
BIAS_TWO = 1.0 - BETA2 ** STEP
MESH = pl.DeviceIdType.MESH
HIGHEST = lax.Precision.HIGHEST
F32 = jnp.float32
BF16 = jnp.bfloat16
NN = (((1,), (0,)), ((), ()))
TN = (((0,), (0,)), ((), ()))
NT = (((1,), (1,)), ((), ()))


def dot(a, b, dims, precision=None):
    return lax.dot_general(a, b, dims, precision=precision, preferred_element_type=F32)


def kernel(nx, ny, w_ref, g_ref, m_ref, v_ref, l_ref, r_ref, ql_ref, qr_ref,
           ow_ref, om_ref, ov_ref, ol_ref, or_ref,
           qr_f, qr_b, grow, growb, ql_f, ql_row, ql_send, ql_col, gx, gy, hb, nb,
           acc, gacc, up, rin, rbuf, lp, lrecv, lx, lbuf, wbuf, mbuf, vbuf, obuf,
           send_sem, recv_sem, local_sem):
    row = lax.axis_index("row")
    col = lax.axis_index("col")
    core = lax.rem(row, 2)
    x = lax.div(row, 2)
    nrow = 2 * nx
    rb, cb = w_ref.shape
    kb = qr_ref.shape[0]
    lb = ql_ref.shape[1]
    hr = rb // 2
    qb = rb // ny

    def wrap(v, n):
        return lax.rem(v + n, n)

    x_plus = {"row": wrap(row + 2, nrow)}
    x_minus = {"row": wrap(row - 2, nrow)}
    partner = {"row": row + 1 - 2 * core}
    y_plus = {"col": wrap(col + 1, ny)}
    y_minus = {"col": wrap(col - 1, ny)}
    prow = row + 1 - 2 * core
    counts = {"remote": 0, "local": 0}
    pending = []
    local_pending = []

    def remote(src, dst, device):
        i = counts["remote"]
        counts["remote"] += 1
        return pltpu.make_async_remote_copy(
            src_ref=src, dst_ref=dst, send_sem=send_sem.at[i], recv_sem=recv_sem.at[i],
            device_id=device, device_id_type=MESH)

    def go(copy):
        copy.start()
        pending.append(copy)

    def local(src, dst):
        i = counts["local"]
        counts["local"] += 1
        copy = pltpu.make_async_copy(src, dst, local_sem.at[i])
        copy.start()
        return copy

    class Gather8:
        def __init__(self, at, own):
            lft, rgt, far = wrap(row - 2, nrow), wrap(row + 2, nrow), wrap(row + 4, nrow)
            self.a0 = remote(own(0), at(row, 0), x_plus)
            self.a1 = remote(own(1), at(row, 1), x_plus)
            self.b1 = remote(own(1), at(row, 1), x_minus)
            self.b0 = remote(own(0), at(row, 0), x_minus)
            self.p = [remote(own(h), at(row, h), partner) for h in (0, 1)]
            self.f0 = remote(at(lft, 0), at(lft, 0), x_plus)
            self.f1 = remote(at(rgt, 1), at(rgt, 1), x_minus)
            self.near = [remote(at(s, h), at(s, h), partner) for s, h in ((lft, 0), (rgt, 1), (lft, 1), (rgt, 0))]
            self.last = [remote(at(far, h), at(far, h), partner) for h in (0, 1)]

        def start(self):
            for c in (self.a0, self.b1, self.a1, self.b0, *self.p):
                go(c)

        def forward(self):
            self.a0.wait_recv()
            go(self.f0)
            go(self.near[0])
            self.b1.wait_recv()
            go(self.f1)
            go(self.near[1])

        def second(self):
            self.a1.wait_recv()
            go(self.near[2])
            self.b0.wait_recv()
            go(self.near[3])

        def third(self):
            self.f0.wait_recv()
            go(self.last[0])
            self.f1.wait_recv()
            go(self.last[1])

        def own_ready(self):
            for c in self.p:
                c.wait_recv()

        def near_ready(self):
            for c in self.near:
                c.wait_recv()

        def far_ready(self):
            for c in self.last:
                c.wait_recv()

    class Gather4:
        def __init__(self, at, own):
            lft, rgt = wrap(col - 1, ny), wrap(col + 1, ny)
            self.a0 = remote(own(0), at(col, 0), y_plus)
            self.a1 = remote(own(1), at(col, 1), y_plus)
            self.b1 = remote(own(1), at(col, 1), y_minus)
            self.b0 = remote(own(0), at(col, 0), y_minus)
            self.f0 = remote(at(lft, 0), at(lft, 0), y_plus)
            self.f1 = remote(at(rgt, 1), at(rgt, 1), y_minus)

        def start(self):
            for c in (self.a0, self.b1, self.a1, self.b0):
                go(c)

        def forward(self):
            self.a0.wait_recv()
            go(self.f0)
            self.b1.wait_recv()
            go(self.f1)

        def second(self):
            self.a1.wait_recv()
            self.b0.wait_recv()

        def third(self):
            self.f0.wait_recv()
            self.f1.wait_recv()

    def peers():
        for dx in (1, nx - 1, 2, 0):
            for dc in (0, 1):
                if dx == 0 and dc == 0:
                    continue
                px = wrap(x + dx, nx)
                pc = core if dc == 0 else 1 - core
                yield 2 * px + pc, px, pc

    load_qr = [local(qr_ref.at[pl.ds(h * kb // 2, kb // 2)], qr_f.at[h]) for h in (0, 1)]
    load_ql = local(ql_ref, ql_f)
    load_g = [local(g_ref.at[:, pl.ds(h * kb, kb)], grow.at[2 * col + h]) for h in (0, 1)]

    barrier = pltpu.get_barrier_semaphore()
    others = [r for r, _, _ in peers()]
    for r in others:
        pl.semaphore_signal(barrier, inc=1, device_id={"row": r}, device_id_type=MESH)
    for d in (y_plus, y_minus):
        pl.semaphore_signal(barrier, inc=1, device_id=d, device_id_type=MESH)

    load_ql.wait()
    ql_row[col] = ql_f[...].astype(BF16).reshape(2, hr, lb)
    for h in (0, 1):
        load_qr[h].wait()
        qr_b[row, h] = qr_f[h].astype(BF16)
    pl.semaphore_wait(barrier, len(others) + 2)

    gather_qr = Gather8(lambda s, h: qr_b.at[s, h], lambda h: qr_b.at[row, h])
    gather_qr.start()
    gather_ql = Gather4(lambda s, h: ql_row.at[s, h], lambda h: ql_row.at[col, h])
    gather_ql.start()
    for c in load_g:
        c.wait()
    gather_g = Gather4(lambda s, h: grow.at[2 * s + h], lambda h: grow.at[2 * col + h])
    gather_g.start()

    load_m = local(m_ref, mbuf)
    load_v = local(v_ref, vbuf)
    load_own = [local(g_ref.at[:, pl.ds(h * kb, kb)], gy.at[row, h]) for h in (0, 1)]
    load_w = local(w_ref, wbuf)
    load_l = local(l_ref, lbuf)
    load_r = [local(r_ref.at[:, pl.ds(h * kb, kb)], rbuf.at[h]) for h in (0, 1)]

    def cast_block(s):
        growb[s] = grow[s].astype(BF16)

    for h in (0, 1):
        cast_block(2 * col + h)

    gather_ql.forward()
    gather_ql.second()
    gather_ql.third()
    half_l = lb // 2
    for k in range(ny):
        block = ql_row[k].reshape(rb, lb)
        for h in (0, 1):
            ql_send[2 * k + h] = block[:, h * half_l:(h + 1) * half_l]
    ql_col[row] = ql_send[row]
    send_ql = []
    for r, _, _ in peers():
        c = remote(ql_send.at[r], ql_col.at[row], {"row": r})
        go(c)
        send_ql.append(c)

    lft_c, rgt_c, far_c = wrap(col - 1, ny), wrap(col + 1, ny), wrap(col + 2, ny)
    gather_g.forward()
    cast_block(2 * lft_c)
    cast_block(2 * rgt_c + 1)
    gather_qr.forward()
    gather_g.second()
    cast_block(2 * lft_c + 1)
    cast_block(2 * rgt_c)
    gather_g.third()
    cast_block(2 * far_c)
    cast_block(2 * far_c + 1)

    def piece(r):
        return grow.at[r, pl.ds(pl.multiple_of(col * qb, qb), qb)]

    gx[row, col] = grow[row, pl.ds(pl.multiple_of(col * qb, qb), qb)]
    send_gx = []
    for r, _, _ in peers():
        c = remote(piece(r), gx.at[row, col], {"row": r})
        go(c)
        send_gx.append(c)

    def add_h(cx, first=False):
        part = dot(growb[2 * cx], qr_b[2 * cx].reshape(kb, cb), NN)
        part += dot(growb[2 * cx + 1], qr_b[2 * cx + 1].reshape(kb, cb), NN)
        if first:
            acc[...] = part
        else:
            acc[...] += part

    x_lft, x_rgt, x_far = wrap(x - 1, nx), wrap(x + 1, nx), wrap(x + 2, nx)
    gather_qr.own_ready()
    add_h(x, True)
    gather_qr.second()
    gather_qr.near_ready()
    add_h(x_lft)
    add_h(x_rgt)
    gather_qr.third()
    gather_qr.far_ready()
    add_h(x_far)
    hb[row] = acc[...].astype(BF16).reshape(2, hr, cb)
    gather_h = Gather8(lambda s, h: hb.at[s, h], lambda h: hb.at[row, h])
    gather_h.start()

    for c in send_gx:
        c.wait_recv()
    gather_gx = Gather4(
        lambda s, h: gx.at[pl.ds(h * (nrow // 2), nrow // 2), s],
        lambda h: gx.at[pl.ds(h * (nrow // 2), nrow // 2), col])
    gather_gx.start()
    for c in send_ql:
        c.wait_recv()

    def add_g(cx, first=False):
        left = ql_col[pl.ds(2 * cx, 2)].reshape(2 * rb, rb)
        part = dot(left, hb[pl.ds(2 * cx, 2)].reshape(2 * rb, cb), TN)
        if first:
            gacc[...] = part
        else:
            gacc[...] += part

    gather_h.own_ready()
    add_g(x, True)
    gather_h.forward()
    gather_h.second()
    gather_h.near_ready()
    add_g(x_lft)
    add_g(x_rgt)
    gather_h.third()
    gather_h.far_ready()
    add_g(x_far)

    load_m.wait()
    load_v.wait()
    rotated = gacc[...]
    new_first = BETA1 * mbuf[...] + (1.0 - BETA1) * rotated
    new_second = BETA2 * vbuf[...] + (1.0 - BETA2) * rotated * rotated
    direction = (new_first / BIAS_ONE) / (jnp.sqrt(new_second / BIAS_TWO) + EPS)
    nb[row] = direction.astype(BF16).reshape(2, hr, cb)
    gather_n = Gather8(lambda s, h: nb.at[s, h], lambda h: nb.at[row, h])
    gather_n.start()
    mbuf[...] = new_first
    vbuf[...] = new_second
    store_m = local(mbuf, om_ref)
    store_v = local(vbuf, ov_ref)

    gather_gx.forward()
    gather_n.forward()
    gather_y = Gather8(lambda s, h: gy.at[s, h], lambda h: grow.at[2 * col + h])
    gather_y.start()

    def add_k(cx, first=False):
        part = dot(ql_row[cx].reshape(rb, lb), nb[pl.ds(2 * cx, 2)].reshape(2 * rb, cb), NN)
        if first:
            acc[...] = part
        else:
            acc[...] += part

    gather_n.own_ready()
    add_k(x, True)
    gather_n.second()
    gather_n.near_ready()
    add_k(x_lft)
    add_k(x_rgt)
    gather_n.third()
    gather_n.far_ready()
    add_k(x_far)
    back = acc[...].astype(BF16)

    def make_u(k):
        for j in range(4):
            q = qr_b[2 * k + j // 2, j % 2]
            up[k, :, :, j * (cb // 4):(j + 1) * (cb // 4)] = dot(back, q, NT).reshape(2, hr, cb // 4)

    u_far = [remote(up.at[far_c, 0], rin.at[0], y_plus), remote(up.at[far_c, 1], rin.at[1], y_minus)]
    u_half = [remote(up.at[rgt_c, 1], rin.at[2], y_plus), remote(up.at[lft_c, 0], rin.at[3], y_minus)]
    u_sum = [remote(up.at[rgt_c, 0], rin.at[4], y_plus), remote(up.at[lft_c, 1], rin.at[5], y_minus)]
    make_u(far_c)
    for c in u_far:
        go(c)
    make_u(rgt_c)
    go(u_half[0])
    make_u(lft_c)
    go(u_half[1])
    make_u(col)

    gather_gx.second()
    gather_gx.third()
    gather_y.forward()

    right_g = gx[pl.ds(2 * col, 2)].reshape(2 * rb, kb)
    for r in range(nrow):
        lp[r] = dot(gx[r].reshape(rb, kb), right_g, NT, HIGHEST)
    swap = []
    for k in range(nx):
        c = remote(lp.at[2 * k + 1 - core], lrecv.at[k], partner)
        go(c)
        swap.append(c)

    u_far[0].wait_recv()
    up[rgt_c, 0] = up[rgt_c, 0] + rin[0]
    go(u_sum[0])
    u_far[1].wait_recv()
    up[lft_c, 1] = up[lft_c, 1] + rin[1]
    go(u_sum[1])

    for c in load_own + load_r:
        c.wait()

    for k in range(nx):
        swap[k].wait_recv()
        lp[2 * k + core] = lp[2 * k + core] + lrecv[k]
    send_l = []
    for dx in (1, nx - 1, 2):
        px = wrap(x + dx, nx)
        c = remote(lp.at[2 * px + core], lx.at[x], {"row": 2 * px + core})
        go(c)
        send_l.append(c)

    def add_r(cx, first=False):
        left = gx[pl.ds(2 * cx, 2)].reshape(2 * rb, kb)

        def body(h, _):
            part = dot(left, gy[pl.ds(2 * cx, 2), h].reshape(2 * rb, kb), TN, HIGHEST)
            old = rbuf[h]
            if first:
                old = BETA2 * old
            rbuf[h] = old + (1.0 - BETA2) * part
            return 0

        lax.fori_loop(0, 2, body, 0)

    gather_y.own_ready()
    add_r(x, True)
    gather_y.second()
    gather_y.near_ready()
    add_r(x_lft)
    add_r(x_rgt)

    for c in (*u_half, *u_sum):
        c.wait_recv()
    load_w.wait()
    obuf[:hr] = wbuf[:hr] - LR * (up[col, 0] + (rin[3] + rin[4]))
    obuf[hr:] = wbuf[hr:] - LR * (up[col, 1] + (rin[2] + rin[5]))
    store_w = local(obuf, ow_ref)

    load_l.wait()
    for c in send_l:
        c.wait_recv()
    total = lp[row]
    for dx in (1, 2, 3):
        total = total + lx[wrap(x + dx, nx)]
    lbuf[...] = BETA2 * lbuf[...] + (1.0 - BETA2) * total
    store_l = local(lbuf, ol_ref)

    gather_y.third()
    gather_y.far_ready()
    add_r(x_far)
    store_r = [local(rbuf.at[h], or_ref.at[:, pl.ds(h * kb, kb)]) for h in (0, 1)]

    for c in pending:
        c.wait_send()
    for c in (store_m, store_v, store_w, store_l, *store_r):
        c.wait()


def solution(mesh):
    nx, ny = mesh.shape["row"] // 2, mesh.shape["col"]
    tile_spec = P(("layer", "row"), "col")

    def local_step(*args):
        rb, cb = args[0].shape
        kb = args[7].shape[0]
        lb = args[6].shape[1]
        hr, nr = rb // 2, 2 * nx
        vm = pltpu.VMEM
        shapes = [args[0], args[2], args[3], args[4], args[5]]
        return pl.pallas_call(
            functools.partial(kernel, nx, ny),
            out_shape=tuple(jax.ShapeDtypeStruct(s.shape, s.dtype) for s in shapes),
            in_specs=[pl.BlockSpec(memory_space=pl.ANY)] * 8,
            out_specs=tuple([pl.BlockSpec(memory_space=pl.ANY)] * 5),
            scratch_shapes=[
                vm((2, kb // 2, cb), F32),
                vm((nr, 2, kb // 2, cb), BF16),
                vm((nr, rb, kb), F32),
                vm((nr, rb, kb), BF16),
                vm((rb, lb), F32),
                vm((ny, 2, hr, lb), BF16),
                vm((nr, rb, lb // 2), BF16),
                vm((nr, rb, lb // 2), BF16),
                vm((nr, ny, rb // ny, kb), F32),
                vm((nr, 2, rb, kb), F32),
                vm((nr, 2, hr, cb), BF16),
                vm((nr, 2, hr, cb), BF16),
                vm((rb, cb), F32),
                vm((rb, cb), F32),
                vm((ny, 2, hr, cb), F32),
                vm((6, hr, cb), F32),
                vm((2, kb, kb), F32),
                vm((nr, rb, lb), F32),
                vm((nx, rb, lb), F32),
                vm((nx, rb, lb), F32),
                vm((rb, lb), F32),
                vm((rb, cb), F32),
                vm((rb, cb), F32),
                vm((rb, cb), F32),
                vm((rb, cb), F32),
                pltpu.SemaphoreType.DMA((112,)),
                pltpu.SemaphoreType.DMA((112,)),
                pltpu.SemaphoreType.DMA((24,)),
            ],
            compiler_params=pltpu.CompilerParams(
                collective_id=0, has_side_effects=True, vmem_limit_bytes=62 * 1024 * 1024),
        )(*args)

    return jax.shard_map(local_step, mesh=mesh, in_specs=(tile_spec,) * 8, out_specs=(tile_spec,) * 5, check_vma=False)
```

```python
import functools

import jax
import jax.numpy as jnp
from jax import lax
from jax.experimental import pallas as pl
from jax.experimental.pallas import tpu as pltpu
from jax.sharding import PartitionSpec as P

BETA1 = 0.9
BETA2 = 0.9
EPS = 1e-8
LR = 0.1
STEP = 10
BIAS_ONE = 1.0 - BETA1 ** STEP
BIAS_TWO = 1.0 - BETA2 ** STEP
MESH = pl.DeviceIdType.MESH
HIGHEST = lax.Precision.HIGHEST
F32 = jnp.float32
BF16 = jnp.bfloat16
NN = (((1,), (0,)), ((), ()))
TN = (((0,), (0,)), ((), ()))
NT = (((1,), (1,)), ((), ()))


def dot(a, b, dims, precision=None):
    return lax.dot_general(a, b, dims, precision=precision, preferred_element_type=F32)


def kernel(nx, ny, w_ref, g_ref, m_ref, v_ref, l_ref, r_ref, ql_ref, qr_ref,
           ow_ref, om_ref, ov_ref, ol_ref, or_ref,
           qr_f, qr_b, grow, growb, ql_f, ql_row, ql_send, ql_col, gx, gy, hb, nb,
           acc, gacc, up, rin, lp, lrecv, lx, wbuf, mbuf, vbuf,
           send_sem, recv_sem, local_sem):
    row = lax.axis_index("row")
    col = lax.axis_index("col")
    core = lax.rem(row, 2)
    x = lax.div(row, 2)
    nrow = 2 * nx
    rb, cb = w_ref.shape
    kb = qr_ref.shape[0]
    lb = ql_ref.shape[1]
    hr = rb // 2
    qb = rb // ny

    def wrap(v, n):
        return lax.rem(v + n, n)

    x_plus = {"row": wrap(row + 2, nrow)}
    x_minus = {"row": wrap(row - 2, nrow)}
    partner = {"row": row + 1 - 2 * core}
    y_plus = {"col": wrap(col + 1, ny)}
    y_minus = {"col": wrap(col - 1, ny)}
    prow = row + 1 - 2 * core
    counts = {"remote": 0, "local": 0}
    pending = []
    local_pending = []

    def remote(src, dst, device):
        i = counts["remote"]
        counts["remote"] += 1
        return pltpu.make_async_remote_copy(
            src_ref=src, dst_ref=dst, send_sem=send_sem.at[i], recv_sem=recv_sem.at[i],
            device_id=device, device_id_type=MESH)

    def go(copy):
        copy.start()
        pending.append(copy)

    def local(src, dst):
        i = counts["local"]
        counts["local"] += 1
        copy = pltpu.make_async_copy(src, dst, local_sem.at[i])
        copy.start()
        return copy

    class Gather8:
        def __init__(self, at, own):
            lft, rgt, far = wrap(row - 2, nrow), wrap(row + 2, nrow), wrap(row + 4, nrow)
            self.a0 = remote(own(0), at(row, 0), x_plus)
            self.a1 = remote(own(1), at(row, 1), x_plus)
            self.b1 = remote(own(1), at(row, 1), x_minus)
            self.b0 = remote(own(0), at(row, 0), x_minus)
            self.p = [remote(own(h), at(row, h), partner) for h in (0, 1)]
            self.f0 = remote(at(lft, 0), at(lft, 0), x_plus)
            self.f1 = remote(at(rgt, 1), at(rgt, 1), x_minus)
            self.near = [remote(at(s, h), at(s, h), partner) for s, h in ((lft, 0), (rgt, 1), (lft, 1), (rgt, 0))]
            self.last = [remote(at(far, h), at(far, h), partner) for h in (0, 1)]

        def start(self):
            for c in (self.a0, self.b1, self.a1, self.b0, *self.p):
                go(c)

        def forward(self):
            self.a0.wait_recv()
            go(self.f0)
            go(self.near[0])
            self.b1.wait_recv()
            go(self.f1)
            go(self.near[1])

        def second(self):
            self.a1.wait_recv()
            go(self.near[2])
            self.b0.wait_recv()
            go(self.near[3])

        def third(self):
            self.f0.wait_recv()
            go(self.last[0])
            self.f1.wait_recv()
            go(self.last[1])

        def own_ready(self):
            for c in self.p:
                c.wait_recv()

        def near_ready(self):
            for c in self.near:
                c.wait_recv()

        def far_ready(self):
            for c in self.last:
                c.wait_recv()

    class Gather4:
        def __init__(self, at, own):
            lft, rgt = wrap(col - 1, ny), wrap(col + 1, ny)
            self.a0 = remote(own(0), at(col, 0), y_plus)
            self.a1 = remote(own(1), at(col, 1), y_plus)
            self.b1 = remote(own(1), at(col, 1), y_minus)
            self.b0 = remote(own(0), at(col, 0), y_minus)
            self.f0 = remote(at(lft, 0), at(lft, 0), y_plus)
            self.f1 = remote(at(rgt, 1), at(rgt, 1), y_minus)

        def start(self):
            for c in (self.a0, self.b1, self.a1, self.b0):
                go(c)

        def forward(self):
            self.a0.wait_recv()
            go(self.f0)
            self.b1.wait_recv()
            go(self.f1)

        def second(self):
            self.a1.wait_recv()
            self.b0.wait_recv()

        def third(self):
            self.f0.wait_recv()
            self.f1.wait_recv()

    def peers():
        for dx in (1, nx - 1, 2, 0):
            for dc in (0, 1):
                if dx == 0 and dc == 0:
                    continue
                px = wrap(x + dx, nx)
                pc = core if dc == 0 else 1 - core
                yield 2 * px + pc, px, pc

    load_qr = [local(qr_ref.at[pl.ds(h * kb // 2, kb // 2)], qr_f.at[h]) for h in (0, 1)]
    load_ql = local(ql_ref, ql_f)
    load_g = [local(g_ref.at[:, pl.ds(h * kb, kb)], grow.at[2 * col + h]) for h in (0, 1)]

    barrier = pltpu.get_barrier_semaphore()
    others = [r for r, _, _ in peers()]
    for r in others:
        pl.semaphore_signal(barrier, inc=1, device_id={"row": r}, device_id_type=MESH)
    with jax.named_scope("s000"):
        for d in (y_plus, y_minus):
            pl.semaphore_signal(barrier, inc=1, device_id=d, device_id_type=MESH)

    with jax.named_scope("s001"):
        load_ql.wait()
    ql_row[col] = ql_f[...].astype(BF16).reshape(2, hr, lb)
    with jax.named_scope("s002"):
        for h in (0, 1):
            load_qr[h].wait()
            qr_b[row, h] = qr_f[h].astype(BF16)
    with jax.named_scope("s003"):
        pl.semaphore_wait(barrier, len(others) + 2)

    gather_qr = Gather8(lambda s, h: qr_b.at[s, h], lambda h: qr_b.at[row, h])
    with jax.named_scope("s004"):
        gather_qr.start()
    gather_ql = Gather4(lambda s, h: ql_row.at[s, h], lambda h: ql_row.at[col, h])
    with jax.named_scope("s005"):
        gather_ql.start()
    with jax.named_scope("s006"):
        for c in load_g:
            c.wait()
    gather_g = Gather4(lambda s, h: grow.at[2 * s + h], lambda h: grow.at[2 * col + h])
    with jax.named_scope("s007"):
        gather_g.start()

    load_m = local(m_ref, mbuf)
    load_v = local(v_ref, vbuf)
    load_own = [local(g_ref.at[:, pl.ds(h * kb, kb)], gy.at[row, h]) for h in (0, 1)]
    load_w = local(w_ref, wbuf)
    load_l = local(l_ref, ol_ref)
    load_r = [local(r_ref.at[:, pl.ds(h * kb, kb)], or_ref.at[h]) for h in (0, 1)]

    def cast_block(s):
        growb[s] = grow[s].astype(BF16)

    with jax.named_scope("s008"):
        for h in (0, 1):
            cast_block(2 * col + h)

    lft_c, rgt_c, far_c = wrap(col - 1, ny), wrap(col + 1, ny), wrap(col + 2, ny)
    half_l = lb // 2
    with jax.named_scope("s009"):
        gather_g.forward()
    cast_block(2 * lft_c)
    cast_block(2 * rgt_c + 1)
    with jax.named_scope("s010"):
        gather_qr.forward()
    with jax.named_scope("s011"):
        gather_g.second()
    cast_block(2 * lft_c + 1)
    cast_block(2 * rgt_c)
    with jax.named_scope("s012"):
        gather_ql.forward()
    with jax.named_scope("s013"):
        gather_ql.second()
    with jax.named_scope("s014"):
        gather_g.third()
    cast_block(2 * far_c)
    cast_block(2 * far_c + 1)

    def piece(r):
        return grow.at[r, pl.ds(pl.multiple_of(col * qb, qb), qb)]

    gx[row, col] = grow[row, pl.ds(pl.multiple_of(col * qb, qb), qb)]
    send_gx = []
    for r, _, _ in peers():
        c = remote(piece(r), gx.at[row, col], {"row": r})
        go(c)
        send_gx.append(c)

    with jax.named_scope("s015"):
        gather_ql.third()
    with jax.named_scope("s016"):
        for k in range(ny):
            block = ql_row[k].reshape(rb, lb)
            for h in (0, 1):
                ql_send[2 * k + h] = block[:, h * half_l:(h + 1) * half_l]
    ql_col[row, col] = ql_send[row, pl.ds(pl.multiple_of(col * qb, qb), qb)]
    send_ql = []
    for r, _, _ in peers():
        c = remote(ql_send.at[r, pl.ds(pl.multiple_of(col * qb, qb), qb)], ql_col.at[row, col], {"row": r})
        go(c)
        send_ql.append(c)

    def add_h(cx, first=False):
        part = dot(growb[2 * cx], qr_b[2 * cx].reshape(kb, cb), NN)
        part += dot(growb[2 * cx + 1], qr_b[2 * cx + 1].reshape(kb, cb), NN)
        if first:
            acc[...] = part
        else:
            acc[...] += part

    x_lft, x_rgt, x_far = wrap(x - 1, nx), wrap(x + 1, nx), wrap(x + 2, nx)
    with jax.named_scope("s017"):
        gather_qr.own_ready()
    with jax.named_scope("s018"):
        add_h(x, True)
    with jax.named_scope("s019"):
        gather_qr.second()
    with jax.named_scope("s020"):
        gather_qr.near_ready()
    with jax.named_scope("s021"):
        add_h(x_lft)
    with jax.named_scope("s022"):
        add_h(x_rgt)
    with jax.named_scope("s023"):
        gather_qr.third()
    with jax.named_scope("s024"):
        gather_qr.far_ready()
    with jax.named_scope("s025"):
        add_h(x_far)
    with jax.named_scope("s026"):
        hb[row] = acc[...].astype(BF16).reshape(2, hr, cb)
    gather_h = Gather8(lambda s, h: hb.at[s, h], lambda h: hb.at[row, h])
    with jax.named_scope("s027"):
        gather_h.start()

    with jax.named_scope("s028"):
        for c in send_gx:
            c.wait_recv()
    gather_gx = Gather4(
        lambda s, h: gx.at[pl.ds(h * (nrow // 2), nrow // 2), s],
        lambda h: gx.at[pl.ds(h * (nrow // 2), nrow // 2), col])
    with jax.named_scope("s029"):
        for c in send_ql:
            c.wait_recv()
    gather_qc = Gather4(
        lambda s, h: ql_col.at[pl.ds(h * (nrow // 2), nrow // 2), s],
        lambda h: ql_col.at[pl.ds(h * (nrow // 2), nrow // 2), col])
    with jax.named_scope("s030"):
        gather_qc.start()
    with jax.named_scope("s031"):
        gather_qc.forward()
    with jax.named_scope("s032"):
        gather_qc.second()
    with jax.named_scope("s033"):
        gather_gx.start()
    with jax.named_scope("s034"):
        gather_qc.third()

    def add_g(cx, first=False):
        left = ql_col[pl.ds(2 * cx, 2)].reshape(2 * rb, rb)
        part = dot(left, hb[pl.ds(2 * cx, 2)].reshape(2 * rb, cb), TN)
        if first:
            gacc[...] = part
        else:
            gacc[...] += part

    with jax.named_scope("s035"):
        gather_h.own_ready()
    with jax.named_scope("s036"):
        add_g(x, True)
    with jax.named_scope("s037"):
        gather_h.forward()
    gather_y = Gather8(lambda s, h: gy.at[s, h], lambda h: grow.at[2 * col + h])
    go(gather_y.a0)
    go(gather_y.b1)
    with jax.named_scope("s038"):
        gather_h.second()
    with jax.named_scope("s039"):
        gather_h.near_ready()
    with jax.named_scope("s040"):
        add_g(x_lft)
    with jax.named_scope("s041"):
        add_g(x_rgt)
    with jax.named_scope("s042"):
        gather_h.third()
    with jax.named_scope("s043"):
        gather_h.far_ready()
    with jax.named_scope("s044"):
        add_g(x_far)

    with jax.named_scope("s045"):
        load_m.wait()
    with jax.named_scope("s046"):
        load_v.wait()
    rotated = gacc[...]
    new_first = BETA1 * mbuf[...] + (1.0 - BETA1) * rotated
    new_second = BETA2 * vbuf[...] + (1.0 - BETA2) * rotated * rotated
    direction = (new_first / BIAS_ONE) / (jnp.sqrt(new_second / BIAS_TWO) + EPS)
    with jax.named_scope("s047"):
        nb[row] = direction.astype(BF16).reshape(2, hr, cb)
    gather_n = Gather8(lambda s, h: nb.at[s, h], lambda h: nb.at[row, h])
    with jax.named_scope("s048"):
        gather_n.start()
    om_ref[...] = new_first
    ov_ref[...] = new_second

    with jax.named_scope("s049"):
        gather_gx.forward()
    with jax.named_scope("s050"):
        gather_n.forward()
    with jax.named_scope("s051"):
        for c in (gather_y.a1, gather_y.b0, *gather_y.p):
            go(c)

    def add_k(cx, first=False):
        part = dot(ql_row[cx].reshape(rb, lb), nb[pl.ds(2 * cx, 2)].reshape(2 * rb, cb), NN)
        if first:
            acc[...] = part
        else:
            acc[...] += part

    with jax.named_scope("s052"):
        gather_n.own_ready()
    with jax.named_scope("s053"):
        add_k(x, True)
    with jax.named_scope("s054"):
        gather_n.second()
    with jax.named_scope("s055"):
        gather_n.near_ready()
    with jax.named_scope("s056"):
        add_k(x_lft)
    with jax.named_scope("s057"):
        add_k(x_rgt)
    with jax.named_scope("s058"):
        gather_n.third()
    with jax.named_scope("s059"):
        gather_n.far_ready()
    with jax.named_scope("s060"):
        add_k(x_far)
    with jax.named_scope("s061"):
        back = acc[...].astype(BF16)

    def make_u(k):
        for j in range(4):
            q = qr_b[2 * k + j // 2, j % 2]
            up[k, :, :, j * (cb // 4):(j + 1) * (cb // 4)] = dot(back, q, NT).reshape(2, hr, cb // 4)

    u_far = [remote(up.at[far_c, 0], rin.at[0], y_plus), remote(up.at[far_c, 1], rin.at[1], y_minus)]
    u_half = [remote(up.at[rgt_c, 1], rin.at[2], y_plus), remote(up.at[lft_c, 0], rin.at[3], y_minus)]
    u_sum = [remote(up.at[rgt_c, 0], rin.at[4], y_plus), remote(up.at[lft_c, 1], rin.at[5], y_minus)]
    with jax.named_scope("s062"):
        gather_y.forward()
    with jax.named_scope("s063"):
        make_u(far_c)
    with jax.named_scope("s064"):
        for c in u_far:
            go(c)
    with jax.named_scope("s065"):
        make_u(rgt_c)
    go(u_half[0])
    with jax.named_scope("s066"):
        make_u(lft_c)
    go(u_half[1])
    with jax.named_scope("s067"):
        make_u(col)

    with jax.named_scope("s068"):
        gather_gx.second()
    with jax.named_scope("s069"):
        gather_gx.third()

    right_g = gx[pl.ds(2 * col, 2)].reshape(2 * rb, kb)
    with jax.named_scope("s070"):
        lp[...] = dot(gx[...].reshape(nrow * rb, kb), right_g, NT, HIGHEST).reshape(nrow, rb, lb)
    swap = []
    with jax.named_scope("s071"):
        for k in range(nx):
            c = remote(lp.at[2 * k + 1 - core], lrecv.at[k], partner)
            go(c)
            swap.append(c)

    with jax.named_scope("s072"):
        u_far[0].wait_recv()
    up[rgt_c, 0] = up[rgt_c, 0] + rin[0]
    go(u_sum[0])
    with jax.named_scope("s073"):
        u_far[1].wait_recv()
    up[lft_c, 1] = up[lft_c, 1] + rin[1]
    go(u_sum[1])

    with jax.named_scope("s074"):
        for c in load_own + load_r:
            c.wait()

    with jax.named_scope("s075"):
        for k in range(nx):
            swap[k].wait_recv()
            lp[2 * k + core] = lp[2 * k + core] + lrecv[k]
    send_l = []
    with jax.named_scope("s076"):
        for dx in (1, nx - 1, 2):
            px = wrap(x + dx, nx)
            c = remote(lp.at[2 * px + core], lx.at[x], {"row": 2 * px + core})
            go(c)
            send_l.append(c)

    def add_r_half(cx, h, first=False):
        left = gx[pl.ds(2 * cx, 2)].reshape(2 * rb, kb)
        part = dot(left, gy[pl.ds(2 * cx, 2), h].reshape(2 * rb, kb), TN, HIGHEST)
        old = or_ref[h]
        if first:
            old = BETA2 * old
        or_ref[h] = old + (1.0 - BETA2) * part

    def add_r(cx, first=False):
        lax.fori_loop(0, 2, lambda h, _: (add_r_half(cx, h, first), 0)[1], 0)

    with jax.named_scope("s077"):
        gather_y.own_ready()
    with jax.named_scope("s078"):
        add_r(x, True)
    with jax.named_scope("s079"):
        gather_y.second()
    with jax.named_scope("s080"):
        gather_y.near_ready()
    with jax.named_scope("s081"):
        add_r(x_lft)
    with jax.named_scope("s082"):
        add_r(x_rgt)

    with jax.named_scope("s083"):
        for c in (*u_half, *u_sum):
            c.wait_recv()
    with jax.named_scope("s084"):
        load_w.wait()
    ow_ref[:hr] = wbuf[:hr] - LR * (up[col, 0] + (rin[3] + rin[4]))
    ow_ref[hr:] = wbuf[hr:] - LR * (up[col, 1] + (rin[2] + rin[5]))

    with jax.named_scope("s085"):
        load_l.wait()
    with jax.named_scope("s086"):
        for c in send_l:
            c.wait_recv()
    total = lp[row]
    with jax.named_scope("s087"):
        for dx in (1, 2, 3):
            total = total + lx[wrap(x + dx, nx)]
    ol_ref[...] = BETA2 * ol_ref[...] + (1.0 - BETA2) * total

    with jax.named_scope("s088"):
        gather_y.third()
    with jax.named_scope("s089"):
        for h in (0, 1):
            gather_y.last[h].wait_recv()
            add_r_half(x_far, h)

    with jax.named_scope("s090"):
        for c in pending:
            c.wait_send()


def write_out(w_ref, m_ref, v_ref, l_ref, r_ref, ow_ref, om_ref, ov_ref, ol_ref, or_ref, sem):
    kb = r_ref.shape[1]
    moves = [(w_ref, ow_ref), (m_ref, om_ref), (v_ref, ov_ref), (l_ref, ol_ref)]
    moves += [(r_ref.at[h], or_ref.at[:, pl.ds(h * kb, kb)]) for h in (0, 1)]
    copies = [pltpu.make_async_copy(a, b, sem.at[i]) for i, (a, b) in enumerate(moves)]
    for c in copies:
        c.start()
    for c in copies:
        c.wait()


def solution(mesh):
    nx, ny = mesh.shape["row"] // 2, mesh.shape["col"]
    tile_spec = P(("layer", "row"), "col")

    def local_step(*args):
        rb, cb = args[0].shape
        kb = args[7].shape[0]
        lb = args[6].shape[1]
        hr, nr = rb // 2, 2 * nx
        vm = pltpu.VMEM
        shapes = [args[0], args[2], args[3], args[4], args[5]]
        held = pl.pallas_call(
            functools.partial(kernel, nx, ny),
            out_shape=tuple(vm(s, F32) for s in [(rb, cb)] * 3 + [(rb, lb), (2, kb, kb)]),
            in_specs=[pl.BlockSpec(memory_space=pl.ANY)] * 8,
            out_specs=tuple([pl.BlockSpec(memory_space=pltpu.VMEM)] * 5),
            scratch_shapes=[
                vm((2, kb // 2, cb), F32),
                vm((nr, 2, kb // 2, cb), BF16),
                vm((nr, rb, kb), F32),
                vm((nr, rb, kb), BF16),
                vm((rb, lb), F32),
                vm((ny, 2, hr, lb), BF16),
                vm((nr, rb, lb // 2), BF16),
                vm((nr, ny, rb // ny, lb // 2), BF16),
                vm((nr, ny, rb // ny, kb), F32),
                vm((nr, 2, rb, kb), F32),
                vm((nr, 2, hr, cb), BF16),
                vm((nr, 2, hr, cb), BF16),
                vm((rb, cb), F32),
                vm((rb, cb), F32),
                vm((ny, 2, hr, cb), F32),
                vm((6, hr, cb), F32),
                vm((nr, rb, lb), F32),
                vm((nx, rb, lb), F32),
                vm((nx, rb, lb), F32),
                vm((rb, cb), F32),
                vm((rb, cb), F32),
                vm((rb, cb), F32),
                pltpu.SemaphoreType.DMA((128,)),
                pltpu.SemaphoreType.DMA((128,)),
                pltpu.SemaphoreType.DMA((24,)),
            ],
            compiler_params=pltpu.CompilerParams(
                collective_id=0, has_side_effects=True, vmem_limit_bytes=61600 * 1024),
        )(*args)
        return pl.pallas_call(
            write_out,
            out_shape=tuple(jax.ShapeDtypeStruct(s.shape, s.dtype) for s in shapes),
            in_specs=[pl.BlockSpec(memory_space=pltpu.VMEM)] * 5,
            out_specs=tuple([pl.BlockSpec(memory_space=pl.ANY)] * 5),
            scratch_shapes=[pltpu.SemaphoreType.DMA((6,))],
            compiler_params=pltpu.CompilerParams(vmem_limit_bytes=4 * 1024 * 1024),
        )(*held)

    return jax.shard_map(local_step, mesh=mesh, in_specs=(tile_spec,) * 8, out_specs=(tile_spec,) * 5, check_vma=False)
```

```python
import functools

import jax
import jax.numpy as jnp
from jax import lax
from jax.experimental import pallas as pl
from jax.experimental.pallas import tpu as pltpu
from jax.sharding import PartitionSpec as P

BETA1 = 0.9
BETA2 = 0.9
EPS = 1e-8
LR = 0.1
STEP = 10
BIAS_ONE = 1.0 - BETA1 ** STEP
BIAS_TWO = 1.0 - BETA2 ** STEP
MESH = pl.DeviceIdType.MESH
HIGHEST = lax.Precision.HIGHEST
F32 = jnp.float32
BF16 = jnp.bfloat16
NN = (((1,), (0,)), ((), ()))
TN = (((0,), (0,)), ((), ()))
NT = (((1,), (1,)), ((), ()))
REMOTE = 107
LOCAL = 13


def dot(a, b, dims, precision=None):
    return lax.dot_general(a, b, dims, precision=precision, preferred_element_type=F32)


def kernel(nx, ny, w_ref, g_ref, m_ref, v_ref, l_ref, r_ref, ql_ref, qr_ref,
           ow_ref, om_ref, ov_ref, ol_ref, or_ref,
           qr_f, qr_b, grow, growb, ql_f, ql_row, ql_send, ql_col, gx, gy, hb, nb,
           acc, gacc, up, rin, lp, lrecv, lx, wbuf, mbuf, vbuf,
           send_sem, recv_sem, local_sem):
    row = lax.axis_index("row")
    col = lax.axis_index("col")
    core = lax.rem(row, 2)
    x = lax.div(row, 2)
    nrow = 2 * nx
    rb, cb = w_ref.shape
    kb = qr_ref.shape[0]
    lb = ql_ref.shape[1]
    hr = rb // 2
    qb = rb // ny

    def wrap(v, n):
        return lax.rem(v + n, n)

    x_plus = {"row": wrap(row + 2, nrow)}
    x_minus = {"row": wrap(row - 2, nrow)}
    partner = {"row": row + 1 - 2 * core}
    y_plus = {"col": wrap(col + 1, ny)}
    y_minus = {"col": wrap(col - 1, ny)}
    prow = row + 1 - 2 * core
    counts = {"remote": 0, "local": 0}
    pending = []
    local_pending = []

    def remote(src, dst, device):
        i = counts["remote"]
        counts["remote"] += 1
        return pltpu.make_async_remote_copy(
            src_ref=src, dst_ref=dst, send_sem=send_sem.at[i], recv_sem=recv_sem.at[i],
            device_id=device, device_id_type=MESH)

    def go(copy):
        copy.start()
        pending.append(copy)

    def local(src, dst):
        i = counts["local"]
        counts["local"] += 1
        copy = pltpu.make_async_copy(src, dst, local_sem.at[i])
        copy.start()
        return copy

    class Gather8:
        def __init__(self, at, own):
            lft, rgt, far = wrap(row - 2, nrow), wrap(row + 2, nrow), wrap(row + 4, nrow)
            self.a0 = remote(own(0), at(row, 0), x_plus)
            self.a1 = remote(own(1), at(row, 1), x_plus)
            self.b1 = remote(own(1), at(row, 1), x_minus)
            self.b0 = remote(own(0), at(row, 0), x_minus)
            self.p = [remote(own(h), at(row, h), partner) for h in (0, 1)]
            self.f0 = remote(at(lft, 0), at(lft, 0), x_plus)
            self.f1 = remote(at(rgt, 1), at(rgt, 1), x_minus)
            self.near = [remote(at(s, h), at(s, h), partner) for s, h in ((lft, 0), (rgt, 1), (lft, 1), (rgt, 0))]
            self.last = [remote(at(far, h), at(far, h), partner) for h in (0, 1)]

        def start(self):
            for c in (self.a0, self.b1, self.a1, self.b0, *self.p):
                go(c)

        def forward(self):
            self.a0.wait_recv()
            go(self.f0)
            go(self.near[0])
            self.b1.wait_recv()
            go(self.f1)
            go(self.near[1])

        def second(self):
            self.a1.wait_recv()
            go(self.near[2])
            self.b0.wait_recv()
            go(self.near[3])

        def third(self):
            self.f0.wait_recv()
            go(self.last[0])
            self.f1.wait_recv()
            go(self.last[1])

        def own_ready(self):
            for c in self.p:
                c.wait_recv()

        def near_ready(self):
            for c in self.near:
                c.wait_recv()

        def far_ready(self):
            for c in self.last:
                c.wait_recv()

    class Gather4:
        def __init__(self, at, own):
            lft, rgt = wrap(col - 1, ny), wrap(col + 1, ny)
            self.a0 = remote(own(0), at(col, 0), y_plus)
            self.a1 = remote(own(1), at(col, 1), y_plus)
            self.b1 = remote(own(1), at(col, 1), y_minus)
            self.b0 = remote(own(0), at(col, 0), y_minus)
            self.f0 = remote(at(lft, 0), at(lft, 0), y_plus)
            self.f1 = remote(at(rgt, 1), at(rgt, 1), y_minus)

        def start(self):
            for c in (self.a0, self.b1, self.a1, self.b0):
                go(c)

        def forward(self):
            self.a0.wait_recv()
            go(self.f0)
            self.b1.wait_recv()
            go(self.f1)

        def second(self):
            self.a1.wait_recv()
            self.b0.wait_recv()

        def third(self):
            self.f0.wait_recv()
            self.f1.wait_recv()

    def peers():
        for dx in (1, nx - 1, 2, 0):
            for dc in (0, 1):
                if dx == 0 and dc == 0:
                    continue
                px = wrap(x + dx, nx)
                pc = core if dc == 0 else 1 - core
                yield 2 * px + pc, px, pc

    load_qr = [local(qr_ref.at[pl.ds(h * kb // 2, kb // 2)], qr_f.at[h]) for h in (0, 1)]
    load_ql = local(ql_ref, ql_f)
    load_g = [local(g_ref.at[:, pl.ds(h * kb, kb)], grow.at[2 * col + h]) for h in (0, 1)]

    barrier = pltpu.get_barrier_semaphore()
    others = [r for r, _, _ in peers()]
    for r in others:
        pl.semaphore_signal(barrier, inc=1, device_id={"row": r}, device_id_type=MESH)
    with jax.named_scope("s000"):
        for d in (y_plus, y_minus):
            pl.semaphore_signal(barrier, inc=1, device_id=d, device_id_type=MESH)

    with jax.named_scope("s001"):
        load_ql.wait()
    ql_row[col] = ql_f[...].astype(BF16).reshape(2, hr, lb)
    with jax.named_scope("s002"):
        for h in (0, 1):
            load_qr[h].wait()
            qr_b[row, h] = qr_f[h].astype(BF16)
    with jax.named_scope("s003"):
        pl.semaphore_wait(barrier, len(others) + 2)

    gather_qr = Gather8(lambda s, h: qr_b.at[s, h], lambda h: qr_b.at[row, h])
    with jax.named_scope("s004"):
        gather_qr.start()
    gather_ql = Gather4(lambda s, h: ql_row.at[s, h], lambda h: ql_row.at[col, h])
    with jax.named_scope("s005"):
        gather_ql.start()
    with jax.named_scope("s006"):
        for c in load_g:
            c.wait()
    gather_g = Gather4(lambda s, h: grow.at[2 * s + h], lambda h: grow.at[2 * col + h])
    with jax.named_scope("s007"):
        gather_g.start()

    load_m = local(m_ref, mbuf)
    load_v = local(v_ref, vbuf)
    load_own = [local(g_ref.at[:, pl.ds(h * kb, kb)], gy.at[row, h]) for h in (0, 1)]
    load_w = local(w_ref, wbuf)
    load_l = local(l_ref, ol_ref)
    load_r = [local(r_ref.at[:, pl.ds(h * kb, kb)], or_ref.at[h]) for h in (0, 1)]

    def cast_block(s):
        growb[s] = grow[s].astype(BF16)

    with jax.named_scope("s008"):
        for h in (0, 1):
            cast_block(2 * col + h)

    lft_c, rgt_c, far_c = wrap(col - 1, ny), wrap(col + 1, ny), wrap(col + 2, ny)
    x_lft, x_rgt, x_far = wrap(x - 1, nx), wrap(x + 1, nx), wrap(x + 2, nx)
    half_l = lb // 2
    quarter = pl.ds(pl.multiple_of(col * qb, qb), qb)
    with jax.named_scope("s009"):
        gather_ql.forward()
    with jax.named_scope("s010"):
        gather_g.forward()
    with jax.named_scope("s011"):
        gather_qr.forward()
    with jax.named_scope("s012"):
        gather_ql.second()
    with jax.named_scope("s013"):
        gather_ql.third()

    with jax.named_scope("s014"):
        for k in range(ny):
            block = ql_row[k].reshape(rb, lb)
            for h in (0, 1):
                ql_send[2 * k + h] = block[:, h * half_l:(h + 1) * half_l]
    ql_col[row, col] = ql_send[row, quarter]
    send_ql = [remote(ql_send.at[r, quarter], ql_col.at[row, col], {"row": r}) for r, _, _ in peers()]
    with jax.named_scope("s015"):
        for c in send_ql:
            go(c)

    cast_block(2 * lft_c)
    cast_block(2 * rgt_c + 1)
    with jax.named_scope("s016"):
        gather_g.second()
    cast_block(2 * lft_c + 1)
    cast_block(2 * rgt_c)
    with jax.named_scope("s017"):
        gather_g.third()

    gx[row, col] = grow[row, quarter]
    send_gx = [remote(grow.at[r, quarter], gx.at[row, col], {"row": r}) for r, _, _ in peers()]
    with jax.named_scope("s018"):
        for c in send_gx:
            go(c)
    gather_y = Gather8(lambda s, h: gy.at[s, h], lambda h: grow.at[2 * col + h])
    with jax.named_scope("s019"):
        for c in gather_y.p:
            go(c)
    cast_block(2 * far_c)
    cast_block(2 * far_c + 1)

    def add_h(cx, first=False):
        part = dot(growb[2 * cx], qr_b[2 * cx].reshape(kb, cb), NN)
        part += dot(growb[2 * cx + 1], qr_b[2 * cx + 1].reshape(kb, cb), NN)
        if first:
            acc[...] = part
        else:
            acc[...] += part

    with jax.named_scope("s020"):
        gather_qr.own_ready()
    with jax.named_scope("s021"):
        add_h(x, True)
    with jax.named_scope("s022"):
        gather_qr.second()
    with jax.named_scope("s023"):
        gather_qr.near_ready()
    with jax.named_scope("s024"):
        add_h(x_lft)
    with jax.named_scope("s025"):
        add_h(x_rgt)
    with jax.named_scope("s026"):
        gather_qr.third()
    with jax.named_scope("s027"):
        gather_qr.far_ready()
    with jax.named_scope("s028"):
        add_h(x_far)
    with jax.named_scope("s029"):
        hb[row] = acc[...].astype(BF16).reshape(2, hr, cb)
    gather_h = Gather8(lambda s, h: hb.at[s, h], lambda h: hb.at[row, h])
    with jax.named_scope("s030"):
        gather_h.start()

    with jax.named_scope("s031"):
        for c in send_ql:
            c.wait_recv()
    gather_qc = Gather4(
        lambda s, h: ql_col.at[pl.ds(h * (nrow // 2), nrow // 2), s],
        lambda h: ql_col.at[pl.ds(h * (nrow // 2), nrow // 2), col])
    with jax.named_scope("s032"):
        gather_qc.start()
    with jax.named_scope("s033"):
        gather_qc.forward()
    with jax.named_scope("s034"):
        for c in send_gx:
            c.wait_recv()
    gather_gx = Gather4(
        lambda s, h: gx.at[pl.ds(h * (nrow // 2), nrow // 2), s],
        lambda h: gx.at[pl.ds(h * (nrow // 2), nrow // 2), col])
    with jax.named_scope("s035"):
        gather_gx.start()

    def add_g(cx, first=False):
        left = ql_col[pl.ds(2 * cx, 2)].reshape(2 * rb, rb)
        part = dot(left, hb[pl.ds(2 * cx, 2)].reshape(2 * rb, cb), TN)
        if first:
            gacc[...] = part
        else:
            gacc[...] += part

    with jax.named_scope("s036"):
        gather_h.forward()
    go(gather_y.a0)
    go(gather_y.b1)
    with jax.named_scope("s037"):
        gather_qc.second()
    with jax.named_scope("s038"):
        gather_qc.third()
    with jax.named_scope("s039"):
        gather_h.own_ready()
    with jax.named_scope("s040"):
        add_g(x, True)
    with jax.named_scope("s041"):
        gather_h.second()
    with jax.named_scope("s042"):
        gather_h.near_ready()
    with jax.named_scope("s043"):
        add_g(x_lft)
    with jax.named_scope("s044"):
        add_g(x_rgt)
    with jax.named_scope("s045"):
        gather_h.third()
    with jax.named_scope("s046"):
        gather_gx.forward()
    with jax.named_scope("s047"):
        gather_h.far_ready()
    with jax.named_scope("s048"):
        add_g(x_far)

    with jax.named_scope("s049"):
        load_m.wait()
    with jax.named_scope("s050"):
        load_v.wait()
    rotated = gacc[...]
    new_first = BETA1 * mbuf[...] + (1.0 - BETA1) * rotated
    new_second = BETA2 * vbuf[...] + (1.0 - BETA2) * rotated * rotated
    direction = (new_first / BIAS_ONE) / (jnp.sqrt(new_second / BIAS_TWO) + EPS)
    with jax.named_scope("s051"):
        nb[row] = direction.astype(BF16).reshape(2, hr, cb)
    gather_n = Gather8(lambda s, h: nb.at[s, h], lambda h: nb.at[row, h])
    with jax.named_scope("s052"):
        gather_n.start()
    om_ref[...] = new_first
    ov_ref[...] = new_second

    def add_k(cx, first=False):
        part = dot(ql_row[cx].reshape(rb, lb), nb[pl.ds(2 * cx, 2)].reshape(2 * rb, cb), NN)
        if first:
            acc[...] = part
        else:
            acc[...] += part

    with jax.named_scope("s053"):
        gather_n.own_ready()
    with jax.named_scope("s054"):
        add_k(x, True)
    with jax.named_scope("s055"):
        gather_n.forward()
    go(gather_y.a1)
    go(gather_y.b0)
    with jax.named_scope("s056"):
        gather_y.forward()
    with jax.named_scope("s057"):
        gather_n.second()
    with jax.named_scope("s058"):
        gather_n.near_ready()
    with jax.named_scope("s059"):
        add_k(x_lft)
    with jax.named_scope("s060"):
        add_k(x_rgt)
    with jax.named_scope("s061"):
        gather_n.third()
    with jax.named_scope("s062"):
        gather_n.far_ready()
    with jax.named_scope("s063"):
        add_k(x_far)
    with jax.named_scope("s064"):
        back = acc[...].astype(BF16)

    def make_u(k):
        for j in range(4):
            q = qr_b[2 * k + j // 2, j % 2]
            up[k, :, :, j * (cb // 4):(j + 1) * (cb // 4)] = dot(back, q, NT).reshape(2, hr, cb // 4)

    u_far = [remote(up.at[far_c, 0], rin.at[0], y_plus), remote(up.at[far_c, 1], rin.at[1], y_minus)]
    u_half = [remote(up.at[rgt_c, 1], rin.at[2], y_plus), remote(up.at[lft_c, 0], rin.at[3], y_minus)]
    u_sum = [remote(up.at[rgt_c, 0], rin.at[4], y_plus), remote(up.at[lft_c, 1], rin.at[5], y_minus)]
    with jax.named_scope("s065"):
        make_u(far_c)
    with jax.named_scope("s066"):
        for c in u_far:
            go(c)
    with jax.named_scope("s067"):
        make_u(rgt_c)
    go(u_half[0])
    with jax.named_scope("s068"):
        make_u(lft_c)
    go(u_half[1])
    with jax.named_scope("s069"):
        make_u(col)

    with jax.named_scope("s070"):
        gather_gx.second()
    with jax.named_scope("s071"):
        gather_gx.third()
    right_g = gx[pl.ds(2 * col, 2)].reshape(2 * rb, kb)
    with jax.named_scope("s072"):
        lp[...] = dot(gx[...].reshape(nrow * rb, kb), right_g, NT, HIGHEST).reshape(nrow, rb, lb)
    swap = [remote(lp.at[2 * k + 1 - core], lrecv.at[k], partner) for k in range(nx)]
    with jax.named_scope("s073"):
        for c in swap:
            go(c)

    def add_r(cx, first=False):
        left = gx[pl.ds(2 * cx, 2)].reshape(2 * rb, kb)

        def body(h, _):
            part = dot(left, gy[pl.ds(2 * cx, 2), h].reshape(2 * rb, kb), TN, HIGHEST)
            old = or_ref[h]
            if first:
                old = BETA2 * old
            or_ref[h] = old + (1.0 - BETA2) * part
            return 0

        lax.fori_loop(0, 2, body, 0)

    with jax.named_scope("s074"):
        for c in load_own + load_r:
            c.wait()
    with jax.named_scope("s075"):
        gather_y.own_ready()
    with jax.named_scope("s076"):
        add_r(x, True)

    with jax.named_scope("s077"):
        u_far[0].wait_recv()
    up[rgt_c, 0] = up[rgt_c, 0] + rin[0]
    go(u_sum[0])
    with jax.named_scope("s078"):
        u_far[1].wait_recv()
    up[lft_c, 1] = up[lft_c, 1] + rin[1]
    go(u_sum[1])

    with jax.named_scope("s079"):
        for k in range(nx):
            swap[k].wait_recv()
            lp[2 * k + core] = lp[2 * k + core] + lrecv[k]
    send_l = [remote(lp.at[2 * wrap(x + dx, nx) + core], lx.at[x], {"row": 2 * wrap(x + dx, nx) + core})
              for dx in (1, nx - 1, 2)]
    with jax.named_scope("s080"):
        for c in send_l:
            go(c)

    with jax.named_scope("s081"):
        gather_y.second()
    with jax.named_scope("s082"):
        gather_y.near_ready()
    with jax.named_scope("s083"):
        gather_y.third()
    with jax.named_scope("s084"):
        add_r(x_lft)
    with jax.named_scope("s085"):
        add_r(x_rgt)
    with jax.named_scope("s086"):
        gather_y.far_ready()
    with jax.named_scope("s087"):
        add_r(x_far)

    with jax.named_scope("s088"):
        load_l.wait()
    with jax.named_scope("s089"):
        for c in send_l:
            c.wait_recv()
    total = lp[row]
    with jax.named_scope("s090"):
        for dx in (1, 2, 3):
            total = total + lx[wrap(x + dx, nx)]
    ol_ref[...] = BETA2 * ol_ref[...] + (1.0 - BETA2) * total

    with jax.named_scope("s091"):
        load_w.wait()
    with jax.named_scope("s092"):
        for c in (*u_half, *u_sum):
            c.wait_recv()
    ow_ref[:hr] = wbuf[:hr] - LR * (up[col, 0] + (rin[3] + rin[4]))
    ow_ref[hr:] = wbuf[hr:] - LR * (up[col, 1] + (rin[2] + rin[5]))

    assert counts == {"remote": REMOTE, "local": LOCAL}
    with jax.named_scope("s093"):
        for c in pending:
            c.wait_send()


def write_out(w_ref, m_ref, v_ref, l_ref, r_ref, ow_ref, om_ref, ov_ref, ol_ref, or_ref, sem):
    kb = r_ref.shape[1]
    moves = [(w_ref, ow_ref), (m_ref, om_ref), (v_ref, ov_ref), (l_ref, ol_ref)]
    moves += [(r_ref.at[h], or_ref.at[:, pl.ds(h * kb, kb)]) for h in (0, 1)]
    copies = [pltpu.make_async_copy(a, b, sem.at[i]) for i, (a, b) in enumerate(moves)]
    for c in copies:
        c.start()
    for c in copies:
        c.wait()


def solution(mesh):
    nx, ny = mesh.shape["row"] // 2, mesh.shape["col"]
    tile_spec = P(("layer", "row"), "col")

    def local_step(*args):
        rb, cb = args[0].shape
        kb = args[7].shape[0]
        lb = args[6].shape[1]
        hr, nr = rb // 2, 2 * nx
        vm = pltpu.VMEM
        shapes = [args[0], args[2], args[3], args[4], args[5]]
        held = pl.pallas_call(
            functools.partial(kernel, nx, ny),
            out_shape=tuple(vm(s, F32) for s in [(rb, cb)] * 3 + [(rb, lb), (2, kb, kb)]),
            in_specs=[pl.BlockSpec(memory_space=pl.ANY)] * 8,
            out_specs=tuple([pl.BlockSpec(memory_space=pltpu.VMEM)] * 5),
            scratch_shapes=[
                vm((2, kb // 2, cb), F32),
                vm((nr, 2, kb // 2, cb), BF16),
                vm((nr, rb, kb), F32),
                vm((nr, rb, kb), BF16),
                vm((rb, lb), F32),
                vm((ny, 2, hr, lb), BF16),
                vm((nr, rb, lb // 2), BF16),
                vm((nr, ny, rb // ny, lb // 2), BF16),
                vm((nr, ny, rb // ny, kb), F32),
                vm((nr, 2, rb, kb), F32),
                vm((nr, 2, hr, cb), BF16),
                vm((nr, 2, hr, cb), BF16),
                vm((rb, cb), F32),
                vm((rb, cb), F32),
                vm((ny, 2, hr, cb), F32),
                vm((6, hr, cb), F32),
                vm((nr, rb, lb), F32),
                vm((nx, rb, lb), F32),
                vm((nx, rb, lb), F32),
                vm((rb, cb), F32),
                vm((rb, cb), F32),
                vm((rb, cb), F32),
                pltpu.SemaphoreType.DMA((REMOTE,)),
                pltpu.SemaphoreType.DMA((REMOTE,)),
                pltpu.SemaphoreType.DMA((LOCAL,)),
            ],
            compiler_params=pltpu.CompilerParams(
                collective_id=0, has_side_effects=True, vmem_limit_bytes=61600 * 1024),
        )(*args)
        return pl.pallas_call(
            write_out,
            out_shape=tuple(jax.ShapeDtypeStruct(s.shape, s.dtype) for s in shapes),
            in_specs=[pl.BlockSpec(memory_space=pltpu.VMEM)] * 5,
            out_specs=tuple([pl.BlockSpec(memory_space=pl.ANY)] * 5),
            scratch_shapes=[pltpu.SemaphoreType.DMA((6,))],
            compiler_params=pltpu.CompilerParams(vmem_limit_bytes=4 * 1024 * 1024),
        )(*held)

    return jax.shard_map(local_step, mesh=mesh, in_specs=(tile_spec,) * 8, out_specs=(tile_spec,) * 5, check_vma=False)
```

```python
import functools

import jax
import jax.numpy as jnp
from jax import lax
from jax.experimental import pallas as pl
from jax.experimental.pallas import tpu as pltpu
from jax.sharding import PartitionSpec as P

BETA1 = 0.9
BETA2 = 0.9
EPS = 1e-8
LR = 0.1
STEP = 10
BIAS_ONE = 1.0 - BETA1 ** STEP
BIAS_TWO = 1.0 - BETA2 ** STEP
MESH = pl.DeviceIdType.MESH
HIGHEST = lax.Precision.HIGHEST
F32 = jnp.float32
BF16 = jnp.bfloat16
NN = (((1,), (0,)), ((), ()))
TN = (((0,), (0,)), ((), ()))
NT = (((1,), (1,)), ((), ()))
COUNTS = (16, 70, 13)


def dot(a, b, dims, precision=None):
    return lax.dot_general(a, b, dims, precision=precision, preferred_element_type=F32)


def kernel(nx, ny, w_ref, g_ref, m_ref, v_ref, l_ref, r_ref, ql_ref, qr_ref,
           ow_ref, om_ref, ov_ref, ol_ref, or_ref,
           qr_f, qr_b, grow, growb, ql_f, ql_row, ql_send, ql_col, gx, gy, hb, nb,
           acc, gacc, up, rin, lp, lrecv, lx, wbuf, mbuf, vbuf,
           send_sem, recv_sem, local_sem):
    row = lax.axis_index("row")
    col = lax.axis_index("col")
    core = lax.rem(row, 2)
    x = lax.div(row, 2)
    nrow = 2 * nx
    rb, cb = w_ref.shape
    kb = qr_ref.shape[0]
    lb = ql_ref.shape[1]
    hr = rb // 2
    qb = rb // ny

    def wrap(v, n):
        return lax.rem(v + n, n)

    x_plus = {"row": wrap(row + 2, nrow)}
    x_minus = {"row": wrap(row - 2, nrow)}
    partner = {"row": row + 1 - 2 * core}
    y_plus = {"col": wrap(col + 1, ny)}
    y_minus = {"col": wrap(col - 1, ny)}
    prow = row + 1 - 2 * core
    counts = {"send": 0, "recv": 0, "local": 0}
    pending = []

    def new(kind):
        counts[kind] += 1
        return counts[kind] - 1

    def remote(src, dst, device, send, recv=None):
        recv = new("recv") if recv is None else recv
        return pltpu.make_async_remote_copy(
            src_ref=src, dst_ref=dst, send_sem=send_sem.at[send], recv_sem=recv_sem.at[recv],
            device_id=device, device_id_type=MESH)

    def sends(span):
        i = new("send")
        pending.append(remote(span, span, partner, i, 0))
        return i

    def arrived(span, recv):
        remote(span, span, partner, 0, recv).wait_recv()

    def local(src, dst, sem=None):
        copy = pltpu.make_async_copy(src, dst, local_sem.at[new("local") if sem is None else sem])
        copy.start()
        return copy

    class Gather8:
        def __init__(self, at, own, span, cut=lambda ref: [ref]):
            lft, rgt, far = wrap(row - 2, nrow), wrap(row + 2, nrow), wrap(row + 4, nrow)
            self.span = span
            snd = sends(span(7))
            self.second_sem, self.own_sem, self.near_sem, self.far_sem = (new("recv") for _ in range(4))
            self.a0 = remote(own(0), at(row, 0), x_plus, snd)
            self.b1 = remote(own(1), at(row, 1), x_minus, snd)
            self.a1 = remote(own(1), at(row, 1), x_plus, snd, self.second_sem)
            self.b0 = remote(own(0), at(row, 0), x_minus, snd, self.second_sem)
            self.p = [remote(own(h), at(row, h), partner, snd, self.own_sem) for h in (0, 1)]
            self.f0 = [remote(c, c, x_plus, snd) for c in cut(at(lft, 0))]
            self.f1 = [remote(c, c, x_minus, snd) for c in cut(at(rgt, 1))]
            self.near = [remote(at(s, h), at(s, h), partner, snd, self.near_sem)
                         for s, h in ((lft, 0), (rgt, 1), (lft, 1), (rgt, 0))]
            self.last = [[remote(c, c, partner, snd, self.far_sem) for c in cut(at(far, h))] for h in (0, 1)]

        def early(self):
            self.a0.start()
            self.b1.start()

        def later(self):
            self.a1.start()
            self.b0.start()

        def to_partner(self):
            for c in self.p:
                c.start()

        def start(self):
            self.early()
            self.later()
            self.to_partner()

        def forward(self):
            self.a0.wait_recv()
            for c in self.f0:
                c.start()
            self.near[0].start()
            self.b1.wait_recv()
            for c in self.f1:
                c.start()
            self.near[1].start()

        def second(self):
            arrived(self.span(1), self.second_sem)
            self.near[2].start()
            self.near[3].start()

        def third(self):
            for i in range(len(self.f0)):
                self.f0[i].wait_recv()
                self.last[0][i].start()
                self.f1[i].wait_recv()
                self.last[1][i].start()

        def own_ready(self):
            arrived(self.span(1), self.own_sem)

        def near_ready(self):
            arrived(self.span(2), self.near_sem)

        def far_ready(self):
            arrived(self.span(1), self.far_sem)

    class Gather4:
        def __init__(self, at, own, span):
            lft, rgt = wrap(col - 1, ny), wrap(col + 1, ny)
            self.span = span
            snd = sends(span(3))
            self.second_sem, self.third_sem = new("recv"), new("recv")
            self.a0 = remote(own(0), at(col, 0), y_plus, snd)
            self.b1 = remote(own(1), at(col, 1), y_minus, snd)
            self.a1 = remote(own(1), at(col, 1), y_plus, snd, self.second_sem)
            self.b0 = remote(own(0), at(col, 0), y_minus, snd, self.second_sem)
            self.f0 = remote(at(lft, 0), at(lft, 0), y_plus, snd, self.third_sem)
            self.f1 = remote(at(rgt, 1), at(rgt, 1), y_minus, snd, self.third_sem)

        def start(self):
            for c in (self.a0, self.b1, self.a1, self.b0):
                c.start()

        def forward(self):
            self.a0.wait_recv()
            self.f0.start()
            self.b1.wait_recv()
            self.f1.start()

        def second(self):
            arrived(self.span(1), self.second_sem)

        def third(self):
            arrived(self.span(1), self.third_sem)

    def peers():
        for dx in (1, nx - 1, 2, 0):
            for dc in (0, 1):
                if dx == 0 and dc == 0:
                    continue
                px = wrap(x + dx, nx)
                pc = core if dc == 0 else 1 - core
                yield 2 * px + pc, px, pc

    load_qr = [local(qr_ref.at[pl.ds(h * kb // 2, kb // 2)], qr_f.at[h]) for h in (0, 1)]
    load_ql = local(ql_ref, ql_f)
    load_g = [local(g_ref.at[:, pl.ds(h * kb, kb)], grow.at[2 * col + h]) for h in (0, 1)]

    barrier = pltpu.get_barrier_semaphore()
    others = [r for r, _, _ in peers()]
    for r in others:
        pl.semaphore_signal(barrier, inc=1, device_id={"row": r}, device_id_type=MESH)
    with jax.named_scope("s000"):
        for d in (y_plus, y_minus):
            pl.semaphore_signal(barrier, inc=1, device_id=d, device_id_type=MESH)

    with jax.named_scope("s001"):
        for h in (0, 1):
            load_qr[h].wait()
            qr_b[row, h] = qr_f[h].astype(BF16)
    with jax.named_scope("s002"):
        load_ql.wait()
    ql_row[col] = ql_f[...].astype(BF16).reshape(2, hr, lb)
    with jax.named_scope("s003"):
        pl.semaphore_wait(barrier, len(others) + 2)

    gather_qr = Gather8(lambda s, h: qr_b.at[s, h], lambda h: qr_b.at[row, h], lambda n: qr_b.at[pl.ds(0, n)],
                        lambda ref: [ref.at[pl.ds(j * kb // 4, kb // 4)] for j in (0, 1)])
    with jax.named_scope("s004"):
        gather_qr.start()
    gather_ql = Gather4(lambda s, h: ql_row.at[s, h], lambda h: ql_row.at[col, h], lambda n: ql_row.at[pl.ds(0, n)])
    with jax.named_scope("s005"):
        gather_ql.start()
    with jax.named_scope("s006"):
        for c in load_g:
            c.wait()
    gather_g = Gather4(lambda s, h: grow.at[2 * s + h], lambda h: grow.at[2 * col + h],
                       lambda n: grow.at[pl.ds(0, 2 * n)])
    with jax.named_scope("s007"):
        gather_g.start()

    load_m = local(m_ref, mbuf)
    load_v = local(v_ref, vbuf)
    load_own = [local(g_ref.at[:, pl.ds(h * kb, kb)], gy.at[row, h]) for h in (0, 1)]
    load_w = local(w_ref, wbuf)
    load_l = local(l_ref, ol_ref)
    load_r = [local(r_ref.at[:, pl.ds(h * kb, kb)], or_ref.at[h]) for h in (0, 1)]

    def cast_block(s):
        growb[s] = grow[s].astype(BF16)

    with jax.named_scope("s008"):
        for h in (0, 1):
            cast_block(2 * col + h)

    lft_c, rgt_c, far_c = wrap(col - 1, ny), wrap(col + 1, ny), wrap(col + 2, ny)
    x_lft, x_rgt, x_far = wrap(x - 1, nx), wrap(x + 1, nx), wrap(x + 2, nx)
    half_l = lb // 2
    quarter = pl.ds(pl.multiple_of(col * qb, qb), qb)
    row_far = wrap(row + 4, nrow)
    prow_far = row_far + 1 - 2 * core
    with jax.named_scope("s009"):
        gather_ql.forward()
    with jax.named_scope("s010"):
        gather_g.forward()
    with jax.named_scope("s011"):
        gather_qr.forward()
    with jax.named_scope("s012"):
        gather_ql.second()
    with jax.named_scope("s013"):
        gather_ql.third()

    with jax.named_scope("s014"):
        for k in range(ny):
            block = ql_row[k].reshape(rb, lb)
            for h in (0, 1):
                ql_send[2 * k + h] = block[:, h * half_l:(h + 1) * half_l]
    ql_col[row, col] = ql_send[row, quarter]
    snd_ql, rcv_ql = sends(ql_col.at[pl.ds(0, nrow - 1), 0]), new("recv")
    for r, _, _ in peers():
        remote(ql_send.at[r, quarter], ql_col.at[row, col], {"row": r}, snd_ql, rcv_ql).start()

    cast_block(2 * lft_c)
    cast_block(2 * rgt_c + 1)
    with jax.named_scope("s015"):
        gather_g.second()
    cast_block(2 * lft_c + 1)
    cast_block(2 * rgt_c)
    with jax.named_scope("s016"):
        gather_g.third()

    eb = qb // 2
    gx[row, col] = grow[row, quarter]
    snd_gx = [sends(gx.at[pl.ds(0, nrow - 1), 0, pl.ds(0, eb)]) for _ in (0, 1)]
    rcv_gx = [new("recv") for _ in (0, 1)]

    def send_gx(w):
        here = pl.ds(pl.multiple_of(col * qb + w * eb, eb), eb)
        for r, _, _ in peers():
            remote(grow.at[r, here], gx.at[row, col, pl.ds(w * eb, eb)], {"row": r}, snd_gx[w], rcv_gx[w]).start()

    def gather_wave(w):
        there, half = pl.ds(w * eb, eb), nrow // 2
        arrived(gx.at[pl.ds(0, nrow - 1), 0, pl.ds(0, eb)], rcv_gx[w])
        g = Gather4(lambda s, h: gx.at[pl.ds(h * half, half), s, there],
                    lambda h: gx.at[pl.ds(h * half, half), col, there],
                    lambda n: gx.at[:, pl.ds(0, n), there])
        g.start()
        return g

    send_gx(0)

    def rows_of(w):
        return pl.ds(w * hr, hr)

    gather_y = [Gather8(lambda s, h, w=w: gy.at[s, h, rows_of(w)], lambda h, w=w: grow.at[2 * col + h, rows_of(w)],
                        lambda n, w=w: gy.at[pl.ds(0, n), :, rows_of(w)]) for w in (0, 1)]
    with jax.named_scope("s017"):
        for g in gather_y:
            g.to_partner()
    cast_block(2 * far_c)
    cast_block(2 * far_c + 1)

    def h_part(r):
        return dot(growb[r], qr_b[r].reshape(kb, cb), NN)

    with jax.named_scope("s018"):
        gather_qr.own_ready()
    acc[...] = h_part(2 * x) + h_part(2 * x + 1)
    with jax.named_scope("s019"):
        gather_qr.second()
    with jax.named_scope("s020"):
        gather_qr.near_ready()
    acc[...] += h_part(2 * x_lft) + h_part(2 * x_lft + 1)
    acc[...] += h_part(2 * x_rgt) + h_part(2 * x_rgt + 1)
    with jax.named_scope("s021"):
        gather_qr.third()
    acc[...] += h_part(row_far)
    with jax.named_scope("s022"):
        gather_qr.far_ready()
    with jax.named_scope("s023"):
        hb[row] = (acc[...] + h_part(prow_far)).astype(BF16).reshape(2, hr, cb)
    gather_h = Gather8(lambda s, h: hb.at[s, h], lambda h: hb.at[row, h], lambda n: hb.at[pl.ds(0, n)])
    with jax.named_scope("s024"):
        gather_h.start()

    arrived(ql_col.at[pl.ds(0, nrow - 1), 0], rcv_ql)
    gather_qc = Gather4(
        lambda s, h: ql_col.at[pl.ds(h * (nrow // 2), nrow // 2), s],
        lambda h: ql_col.at[pl.ds(h * (nrow // 2), nrow // 2), col],
        lambda n: ql_col.at[:, pl.ds(0, n)])
    with jax.named_scope("s025"):
        gather_qc.start()
    with jax.named_scope("s026"):
        gather_qc.forward()
    gather_gx0 = gather_wave(0)

    def g_part(r):
        return dot(ql_col[r].reshape(rb, rb), hb[r].reshape(rb, cb), TN)

    def g_pair(cx):
        left = ql_col[pl.ds(2 * cx, 2)].reshape(2 * rb, rb)
        return dot(left, hb[pl.ds(2 * cx, 2)].reshape(2 * rb, cb), TN)

    with jax.named_scope("s027"):
        gather_h.forward()
    send_gx(1)
    gather_y[0].early()
    with jax.named_scope("s028"):
        gather_qc.second()
    with jax.named_scope("s029"):
        gather_qc.third()
    with jax.named_scope("s030"):
        gather_h.own_ready()
    gacc[...] = g_pair(x)
    with jax.named_scope("s031"):
        gather_h.second()
    with jax.named_scope("s032"):
        gather_gx0.forward()
    with jax.named_scope("s033"):
        gather_h.near_ready()
    gacc[...] += g_pair(x_lft)
    gacc[...] += g_pair(x_rgt)
    with jax.named_scope("s034"):
        gather_h.third()
    gacc[...] += g_part(row_far)
    with jax.named_scope("s035"):
        gather_h.far_ready()
    rotated = gacc[...] + g_part(prow_far)

    with jax.named_scope("s036"):
        load_m.wait()
    with jax.named_scope("s037"):
        load_v.wait()
    new_first = BETA1 * mbuf[...] + (1.0 - BETA1) * rotated
    new_second = BETA2 * vbuf[...] + (1.0 - BETA2) * rotated * rotated
    direction = (new_first / BIAS_ONE) / (jnp.sqrt(new_second / BIAS_TWO) + EPS)
    with jax.named_scope("s038"):
        nb[row] = direction.astype(BF16).reshape(2, hr, cb)
    gather_n = Gather8(lambda s, h: nb.at[s, h], lambda h: nb.at[row, h], lambda n: nb.at[pl.ds(0, n)])
    with jax.named_scope("s039"):
        gather_n.start()
    om_ref[...] = new_first
    ov_ref[...] = new_second
    gather_gx1 = gather_wave(1)

    def k_part(r):
        return dot(ql_send[r], nb[r].reshape(rb, cb), NN)

    def k_pair(cx):
        return dot(ql_row[cx].reshape(rb, lb), nb[pl.ds(2 * cx, 2)].reshape(2 * rb, cb), NN)

    with jax.named_scope("s040"):
        gather_n.own_ready()
    acc[...] = k_pair(x)
    with jax.named_scope("s041"):
        gather_n.forward()
    gather_y[0].later()
    gather_y[0].forward()
    gather_y[1].early()
    gather_y[1].later()
    with jax.named_scope("s042"):
        gather_gx1.forward()
    with jax.named_scope("s043"):
        gather_n.second()
    with jax.named_scope("s044"):
        gather_n.near_ready()
    acc[...] += k_pair(x_lft)
    acc[...] += k_pair(x_rgt)
    with jax.named_scope("s045"):
        gather_n.third()
    acc[...] += k_part(row_far)
    with jax.named_scope("s046"):
        gather_n.far_ready()
    with jax.named_scope("s047"):
        back = (acc[...] + k_part(prow_far)).astype(BF16)

    def make_u(k):
        for j in range(4):
            q = qr_b[2 * k + j // 2, j % 2]
            up[k, :, :, j * (cb // 4):(j + 1) * (cb // 4)] = dot(back, q, NT).reshape(2, hr, cb // 4)

    snd_u, rcv_u = sends(rin), new("recv")
    u_far = [remote(up.at[far_c, 0], rin.at[0], y_plus, snd_u), remote(up.at[far_c, 1], rin.at[1], y_minus, snd_u)]
    u_half = [remote(up.at[rgt_c, 1], rin.at[2], y_plus, snd_u, rcv_u),
              remote(up.at[lft_c, 0], rin.at[3], y_minus, snd_u, rcv_u)]
    u_sum = [remote(up.at[rgt_c, 0], rin.at[4], y_plus, snd_u, rcv_u),
             remote(up.at[lft_c, 1], rin.at[5], y_minus, snd_u, rcv_u)]
    with jax.named_scope("s048"):
        make_u(far_c)
    with jax.named_scope("s049"):
        for c in u_far:
            c.start()
    with jax.named_scope("s050"):
        make_u(rgt_c)
    u_half[0].start()
    with jax.named_scope("s051"):
        make_u(lft_c)
    u_half[1].start()
    with jax.named_scope("s052"):
        make_u(col)

    with jax.named_scope("s053"):
        for g in (gather_gx0, gather_gx1):
            g.second()
            g.third()
    right_g = gx[pl.ds(2 * col, 2)].reshape(2 * rb, kb)
    with jax.named_scope("s054"):
        lp[...] = dot(gx[...].reshape(nrow * rb, kb), right_g, NT, HIGHEST).reshape(nrow, rb, lb)
    snd_s, rcv_s = sends(lrecv), new("recv")
    with jax.named_scope("s055"):
        for k in range(nx):
            remote(lp.at[2 * k + 1 - core], lrecv.at[k], partner, snd_s, rcv_s).start()

    def add_r(cx, first=False):
        left = gx[pl.ds(2 * cx, 2)].reshape(2 * rb, kb)

        def body(h, _):
            part = dot(left, gy[pl.ds(2 * cx, 2), h].reshape(2 * rb, kb), TN, HIGHEST)
            old = or_ref[h]
            if first:
                old = BETA2 * old
            or_ref[h] = old + (1.0 - BETA2) * part
            return 0

        lax.fori_loop(0, 2, body, 0)

    gather_y[0].second()
    gather_y[1].forward()
    with jax.named_scope("s056"):
        for c in load_own + load_r:
            c.wait()
    with jax.named_scope("s057"):
        for g in gather_y:
            g.own_ready()
    with jax.named_scope("s058"):
        add_r(x, True)

    with jax.named_scope("s059"):
        u_far[0].wait_recv()
    up[rgt_c, 0] = up[rgt_c, 0] + rin[0]
    u_sum[0].start()
    with jax.named_scope("s060"):
        u_far[1].wait_recv()
    up[lft_c, 1] = up[lft_c, 1] + rin[1]
    u_sum[1].start()

    arrived(lrecv, rcv_s)
    with jax.named_scope("s061"):
        for k in range(nx):
            lp[2 * k + core] = lp[2 * k + core] + lrecv[k]
    snd_l, rcv_l = sends(lx.at[pl.ds(0, nx - 1)]), new("recv")
    with jax.named_scope("s062"):
        for dx in (1, nx - 1, 2):
            to = 2 * wrap(x + dx, nx) + core
            remote(lp.at[to], lx.at[x], {"row": to}, snd_l, rcv_l).start()

    gather_y[0].third()
    gather_y[1].second()
    with jax.named_scope("s063"):
        for g in gather_y:
            g.near_ready()
    with jax.named_scope("s064"):
        add_r(x_lft)
    gather_y[1].third()
    with jax.named_scope("s065"):
        add_r(x_rgt)
    with jax.named_scope("s066"):
        for g in gather_y:
            g.far_ready()
    with jax.named_scope("s067"):
        add_r(x_far)

    with jax.named_scope("s068"):
        load_l.wait()
    arrived(lx.at[pl.ds(0, nx - 1)], rcv_l)
    total = lp[row]
    with jax.named_scope("s069"):
        for dx in (1, 2, 3):
            total = total + lx[wrap(x + dx, nx)]
    ol_ref[...] = BETA2 * ol_ref[...] + (1.0 - BETA2) * total

    with jax.named_scope("s070"):
        load_w.wait()
    arrived(rin.at[pl.ds(0, 4)], rcv_u)
    ow_ref[:hr] = wbuf[:hr] - LR * (up[col, 0] + (rin[3] + rin[4]))
    ow_ref[hr:] = wbuf[hr:] - LR * (up[col, 1] + (rin[2] + rin[5]))

    assert tuple(counts.values()) == COUNTS
    with jax.named_scope("s071"):
        for c in pending:
            c.wait_send()


def write_out(w_ref, m_ref, v_ref, l_ref, r_ref, ow_ref, om_ref, ov_ref, ol_ref, or_ref, sem):
    kb = r_ref.shape[1]
    moves = [(w_ref, ow_ref), (m_ref, om_ref), (v_ref, ov_ref), (l_ref, ol_ref)]
    moves += [(r_ref.at[h], or_ref.at[:, pl.ds(h * kb, kb)]) for h in (0, 1)]
    copies = [pltpu.make_async_copy(a, b, sem.at[i]) for i, (a, b) in enumerate(moves)]
    for c in copies:
        c.start()
    for c in copies:
        c.wait()


def solution(mesh):
    nx, ny = mesh.shape["row"] // 2, mesh.shape["col"]
    tile_spec = P(("layer", "row"), "col")

    def local_step(*args):
        rb, cb = args[0].shape
        kb = args[7].shape[0]
        lb = args[6].shape[1]
        hr, nr = rb // 2, 2 * nx
        vm = pltpu.VMEM
        shapes = [args[0], args[2], args[3], args[4], args[5]]
        held = pl.pallas_call(
            functools.partial(kernel, nx, ny),
            out_shape=tuple(vm(s, F32) for s in [(rb, cb)] * 3 + [(rb, lb), (2, kb, kb)]),
            in_specs=[pl.BlockSpec(memory_space=pl.ANY)] * 8,
            out_specs=tuple([pl.BlockSpec(memory_space=pltpu.VMEM)] * 5),
            scratch_shapes=[
                vm((2, kb // 2, cb), F32),
                vm((nr, 2, kb // 2, cb), BF16),
                vm((nr, rb, kb), F32),
                vm((nr, rb, kb), BF16),
                vm((rb, lb), F32),
                vm((ny, 2, hr, lb), BF16),
                vm((nr, rb, lb // 2), BF16),
                vm((nr, ny, rb // ny, lb // 2), BF16),
                vm((nr, ny, rb // ny, kb), F32),
                vm((nr, 2, rb, kb), F32),
                vm((nr, 2, hr, cb), BF16),
                vm((nr, 2, hr, cb), BF16),
                vm((rb, cb), F32),
                vm((rb, cb), F32),
                vm((ny, 2, hr, cb), F32),
                vm((6, hr, cb), F32),
                vm((nr, rb, lb), F32),
                vm((nx, rb, lb), F32),
                vm((nx, rb, lb), F32),
                vm((rb, cb), F32),
                vm((rb, cb), F32),
                vm((rb, cb), F32),
                *[pltpu.SemaphoreType.DMA((n,)) for n in COUNTS],
            ],
            compiler_params=pltpu.CompilerParams(
                collective_id=0, has_side_effects=True, vmem_limit_bytes=61600 * 1024),
        )(*args)
        return pl.pallas_call(
            write_out,
            out_shape=tuple(jax.ShapeDtypeStruct(s.shape, s.dtype) for s in shapes),
            in_specs=[pl.BlockSpec(memory_space=pltpu.VMEM)] * 5,
            out_specs=tuple([pl.BlockSpec(memory_space=pl.ANY)] * 5),
            scratch_shapes=[pltpu.SemaphoreType.DMA((6,))],
            compiler_params=pltpu.CompilerParams(vmem_limit_bytes=4 * 1024 * 1024),
        )(*held)

    return jax.shard_map(local_step, mesh=mesh, in_specs=(tile_spec,) * 8, out_specs=(tile_spec,) * 5, check_vma=False)
```

```python
import functools

import jax
import jax.numpy as jnp
from jax import lax
from jax.experimental import pallas as pl
from jax.experimental.pallas import tpu as pltpu
from jax.sharding import PartitionSpec as P

BETA1 = 0.9
BETA2 = 0.9
EPS = 1e-8
LR = 0.1
STEP = 10
BIAS_ONE = 1.0 - BETA1 ** STEP
BIAS_TWO = 1.0 - BETA2 ** STEP
MESH = pl.DeviceIdType.MESH
HIGHEST = lax.Precision.HIGHEST
F32 = jnp.float32
BF16 = jnp.bfloat16
NN = (((1,), (0,)), ((), ()))
TN = (((0,), (0,)), ((), ()))
NT = (((1,), (1,)), ((), ()))
COUNTS = (16, 78, 13)


def dot(a, b, dims, precision=None):
    return lax.dot_general(a, b, dims, precision=precision, preferred_element_type=F32)


def kernel(nx, ny, w_ref, g_ref, m_ref, v_ref, l_ref, r_ref, ql_ref, qr_ref,
           ow_ref, om_ref, ov_ref, ol_ref, or_ref,
           qr_f, qr_b, grow, growb, ql_f, ql_row, ql_send, ql_col, gx, gy, hb, nb,
           acc, gacc, up, rin, lp, lrecv, lx, wbuf, mbuf, vbuf,
           send_sem, recv_sem, local_sem):
    row = lax.axis_index("row")
    col = lax.axis_index("col")
    core = lax.rem(row, 2)
    x = lax.div(row, 2)
    nrow = 2 * nx
    rb, cb = w_ref.shape
    kb = qr_ref.shape[0]
    lb = ql_ref.shape[1]
    hr = rb // 2
    qb = rb // ny

    def wrap(v, n):
        return lax.rem(v + n, n)

    x_plus = {"row": wrap(row + 2, nrow)}
    x_minus = {"row": wrap(row - 2, nrow)}
    partner = {"row": row + 1 - 2 * core}
    y_plus = {"col": wrap(col + 1, ny)}
    y_minus = {"col": wrap(col - 1, ny)}
    prow = row + 1 - 2 * core
    counts = {"send": 0, "recv": 0, "local": 0}
    pending = []

    def new(kind):
        counts[kind] += 1
        return counts[kind] - 1

    def remote(src, dst, device, send, recv=None):
        recv = new("recv") if recv is None else recv
        return pltpu.make_async_remote_copy(
            src_ref=src, dst_ref=dst, send_sem=send_sem.at[send], recv_sem=recv_sem.at[recv],
            device_id=device, device_id_type=MESH)

    def sends(span):
        i = new("send")
        pending.append(remote(span, span, partner, i, 0))
        return i

    def arrived(span, recv):
        remote(span, span, partner, 0, recv).wait_recv()

    def local(src, dst, sem=None):
        copy = pltpu.make_async_copy(src, dst, local_sem.at[new("local") if sem is None else sem])
        copy.start()
        return copy

    class Gather8:
        def __init__(self, at, own, span, cut=lambda ref: [ref]):
            lft, rgt, far = wrap(row - 2, nrow), wrap(row + 2, nrow), wrap(row + 4, nrow)
            self.span = span
            snd = sends(span(7))
            self.second_sem, self.own_sem, self.near_sem, self.far_sem = (new("recv") for _ in range(4))
            self.a0 = remote(own(0), at(row, 0), x_plus, snd)
            self.b1 = remote(own(1), at(row, 1), x_minus, snd)
            self.a1 = remote(own(1), at(row, 1), x_plus, snd, self.second_sem)
            self.b0 = remote(own(0), at(row, 0), x_minus, snd, self.second_sem)
            self.p = [remote(own(h), at(row, h), partner, snd, self.own_sem) for h in (0, 1)]
            self.f0 = [remote(c, c, x_plus, snd) for c in cut(at(lft, 0))]
            self.f1 = [remote(c, c, x_minus, snd) for c in cut(at(rgt, 1))]
            self.near = [remote(at(s, h), at(s, h), partner, snd, self.near_sem)
                         for s, h in ((lft, 0), (rgt, 1), (lft, 1), (rgt, 0))]
            self.last = [[remote(c, c, partner, snd, self.far_sem) for c in cut(at(far, h))] for h in (0, 1)]

        def early(self):
            self.a0.start()
            self.b1.start()

        def later(self):
            self.a1.start()
            self.b0.start()

        def to_partner(self):
            for c in self.p:
                c.start()

        def start(self):
            self.early()
            self.later()
            self.to_partner()

        def forward(self):
            self.a0.wait_recv()
            for c in self.f0:
                c.start()
            self.near[0].start()
            self.b1.wait_recv()
            for c in self.f1:
                c.start()
            self.near[1].start()

        def second(self):
            arrived(self.span(1), self.second_sem)
            self.near[2].start()
            self.near[3].start()

        def third(self):
            for i in range(len(self.f0)):
                self.f0[i].wait_recv()
                self.last[0][i].start()
                self.f1[i].wait_recv()
                self.last[1][i].start()

        def own_ready(self):
            arrived(self.span(1), self.own_sem)

        def near_ready(self):
            arrived(self.span(2), self.near_sem)

        def far_ready(self):
            arrived(self.span(1), self.far_sem)

    class Gather4:
        def __init__(self, at, own, span):
            lft, rgt = wrap(col - 1, ny), wrap(col + 1, ny)
            self.span = span
            snd = sends(span(3))
            self.second_sem, self.third_sem = new("recv"), new("recv")
            self.a0 = remote(own(0), at(col, 0), y_plus, snd)
            self.b1 = remote(own(1), at(col, 1), y_minus, snd)
            self.a1 = remote(own(1), at(col, 1), y_plus, snd, self.second_sem)
            self.b0 = remote(own(0), at(col, 0), y_minus, snd, self.second_sem)
            self.f0 = remote(at(lft, 0), at(lft, 0), y_plus, snd, self.third_sem)
            self.f1 = remote(at(rgt, 1), at(rgt, 1), y_minus, snd, self.third_sem)

        def start(self):
            for c in (self.a0, self.b1, self.a1, self.b0):
                c.start()

        def forward(self):
            self.a0.wait_recv()
            self.f0.start()
            self.b1.wait_recv()
            self.f1.start()

        def second(self):
            arrived(self.span(1), self.second_sem)

        def third(self):
            arrived(self.span(1), self.third_sem)

    def peers():
        for dx in (1, nx - 1, 2, 0):
            for dc in (0, 1):
                if dx == 0 and dc == 0:
                    continue
                px = wrap(x + dx, nx)
                pc = core if dc == 0 else 1 - core
                yield 2 * px + pc, px, pc

    load_qr = [local(qr_ref.at[pl.ds(h * kb // 2, kb // 2)], qr_f.at[h]) for h in (0, 1)]

    barrier = pltpu.get_barrier_semaphore()
    others = [r for r, _, _ in peers()]
    for r in others:
        pl.semaphore_signal(barrier, inc=1, device_id={"row": r}, device_id_type=MESH)
    with jax.named_scope("s000"):
        for d in (y_plus, y_minus):
            pl.semaphore_signal(barrier, inc=1, device_id=d, device_id_type=MESH)

    load_qr[0].wait()
    load_ql = local(ql_ref, ql_f)
    load_g = [local(g_ref.at[:, pl.ds(h * kb, kb)], grow.at[2 * col + h]) for h in (0, 1)]
    qr_b[row, 0] = qr_f[0].astype(BF16)
    load_qr[1].wait()
    qr_b[row, 1] = qr_f[1].astype(BF16)
    with jax.named_scope("s001"):
        pl.semaphore_wait(barrier, len(others) + 2)

    gather_qr = Gather8(lambda s, h: qr_b.at[s, h], lambda h: qr_b.at[row, h], lambda n: qr_b.at[pl.ds(0, n)],
                        lambda ref: [ref.at[pl.ds(j * kb // 8, kb // 8)] for j in range(4)])
    with jax.named_scope("s002"):
        gather_qr.start()
    gather_ql = Gather4(lambda s, h: ql_row.at[s, h], lambda h: ql_row.at[col, h], lambda n: ql_row.at[pl.ds(0, n)])
    with jax.named_scope("s003"):
        load_ql.wait()
    ql_row[col] = ql_f[...].astype(BF16).reshape(2, hr, lb)
    with jax.named_scope("s004"):
        gather_ql.start()
    with jax.named_scope("s005"):
        for c in load_g:
            c.wait()
    gather_g = Gather4(lambda s, h: grow.at[2 * s + h], lambda h: grow.at[2 * col + h],
                       lambda n: grow.at[pl.ds(0, 2 * n)])
    with jax.named_scope("s006"):
        gather_g.start()

    load_m = local(m_ref, mbuf)
    load_v = local(v_ref, vbuf)
    load_own = [local(g_ref.at[:, pl.ds(h * kb, kb)], gy.at[row, h]) for h in (0, 1)]
    load_w = local(w_ref, wbuf)
    load_l = local(l_ref, ol_ref)
    load_r = [local(r_ref.at[:, pl.ds(h * kb, kb)], or_ref.at[h]) for h in (0, 1)]

    def cast_block(s):
        growb[s] = grow[s].astype(BF16)

    with jax.named_scope("s007"):
        for h in (0, 1):
            cast_block(2 * col + h)

    lft_c, rgt_c, far_c = wrap(col - 1, ny), wrap(col + 1, ny), wrap(col + 2, ny)
    x_lft, x_rgt, x_far = wrap(x - 1, nx), wrap(x + 1, nx), wrap(x + 2, nx)
    half_l = lb // 2
    quarter = pl.ds(pl.multiple_of(col * qb, qb), qb)
    row_far = wrap(row + 4, nrow)
    prow_far = row_far + 1 - 2 * core
    with jax.named_scope("s008"):
        gather_ql.forward()
    with jax.named_scope("s009"):
        gather_g.forward()
    with jax.named_scope("s010"):
        gather_qr.forward()
    with jax.named_scope("s011"):
        gather_ql.second()
    with jax.named_scope("s012"):
        gather_ql.third()

    with jax.named_scope("s013"):
        for k in range(ny):
            block = ql_row[k].reshape(rb, lb)
            for h in (0, 1):
                ql_send[2 * k + h] = block[:, h * half_l:(h + 1) * half_l]
    ql_col[row, col] = ql_send[row, quarter]
    snd_ql, rcv_ql = sends(ql_col.at[pl.ds(0, nrow - 1), 0]), new("recv")
    for r, _, _ in peers():
        remote(ql_send.at[r, quarter], ql_col.at[row, col], {"row": r}, snd_ql, rcv_ql).start()

    cast_block(2 * lft_c)
    cast_block(2 * rgt_c + 1)
    with jax.named_scope("s014"):
        gather_g.second()
    cast_block(2 * lft_c + 1)
    cast_block(2 * rgt_c)
    with jax.named_scope("s015"):
        gather_g.third()

    eb = qb // 2
    gx[row, col] = grow[row, quarter]
    snd_gx = [sends(gx.at[pl.ds(0, nrow - 1), 0, pl.ds(0, eb)]) for _ in (0, 1)]
    rcv_gx = [new("recv") for _ in (0, 1)]

    def send_gx(w):
        here = pl.ds(pl.multiple_of(col * qb + w * eb, eb), eb)
        for r, _, _ in peers():
            remote(grow.at[r, here], gx.at[row, col, pl.ds(w * eb, eb)], {"row": r}, snd_gx[w], rcv_gx[w]).start()

    def gather_wave(w):
        there, half = pl.ds(w * eb, eb), nrow // 2
        arrived(gx.at[pl.ds(0, nrow - 1), 0, pl.ds(0, eb)], rcv_gx[w])
        g = Gather4(lambda s, h: gx.at[pl.ds(h * half, half), s, there],
                    lambda h: gx.at[pl.ds(h * half, half), col, there],
                    lambda n: gx.at[:, pl.ds(0, n), there])
        g.start()
        return g

    send_gx(0)

    def rows_of(w):
        return pl.ds(w * hr, hr)

    gather_y = [Gather8(lambda s, h, w=w: gy.at[s, h, rows_of(w)], lambda h, w=w: grow.at[2 * col + h, rows_of(w)],
                        lambda n, w=w: gy.at[pl.ds(0, n), :, rows_of(w)]) for w in (0, 1)]
    with jax.named_scope("s016"):
        for g in gather_y:
            g.to_partner()
    cast_block(2 * far_c)
    cast_block(2 * far_c + 1)

    def h_part(r):
        return dot(growb[r], qr_b[r].reshape(kb, cb), NN)

    with jax.named_scope("s017"):
        gather_qr.own_ready()
    acc[...] = h_part(2 * x) + h_part(2 * x + 1)
    with jax.named_scope("s018"):
        gather_qr.second()
    with jax.named_scope("s019"):
        gather_qr.near_ready()
    acc[...] += h_part(2 * x_lft) + h_part(2 * x_lft + 1)
    acc[...] += h_part(2 * x_rgt) + h_part(2 * x_rgt + 1)
    with jax.named_scope("s020"):
        gather_qr.third()
    acc[...] += h_part(row_far)
    with jax.named_scope("s021"):
        gather_qr.far_ready()
    with jax.named_scope("s022"):
        hb[row] = (acc[...] + h_part(prow_far)).astype(BF16).reshape(2, hr, cb)

    def halves(ref):
        return [ref.at[pl.ds(j * hr // 2, hr // 2)] for j in (0, 1)]

    gather_h = Gather8(lambda s, h: hb.at[s, h], lambda h: hb.at[row, h], lambda n: hb.at[pl.ds(0, n)], halves)
    with jax.named_scope("s023"):
        gather_h.start()

    arrived(ql_col.at[pl.ds(0, nrow - 1), 0], rcv_ql)
    gather_qc = Gather4(
        lambda s, h: ql_col.at[pl.ds(h * (nrow // 2), nrow // 2), s],
        lambda h: ql_col.at[pl.ds(h * (nrow // 2), nrow // 2), col],
        lambda n: ql_col.at[:, pl.ds(0, n)])
    with jax.named_scope("s024"):
        gather_qc.start()
    with jax.named_scope("s025"):
        gather_qc.forward()
    gather_gx0 = gather_wave(0)

    def g_part(r):
        return dot(ql_col[r].reshape(rb, rb), hb[r].reshape(rb, cb), TN)

    def g_pair(cx):
        left = ql_col[pl.ds(2 * cx, 2)].reshape(2 * rb, rb)
        return dot(left, hb[pl.ds(2 * cx, 2)].reshape(2 * rb, cb), TN)

    with jax.named_scope("s026"):
        gather_h.forward()
    send_gx(1)
    with jax.named_scope("s027"):
        gather_qc.second()
    with jax.named_scope("s028"):
        gather_qc.third()
    with jax.named_scope("s029"):
        gather_h.own_ready()
    gacc[...] = g_pair(x)
    with jax.named_scope("s030"):
        gather_h.second()
    with jax.named_scope("s031"):
        gather_gx0.forward()
    with jax.named_scope("s032"):
        gather_h.near_ready()
    gacc[...] += g_pair(x_lft)
    gacc[...] += g_pair(x_rgt)
    with jax.named_scope("s033"):
        gather_h.third()
    gacc[...] += g_part(row_far)
    with jax.named_scope("s034"):
        gather_h.far_ready()
    rotated = gacc[...] + g_part(prow_far)

    with jax.named_scope("s035"):
        load_m.wait()
    with jax.named_scope("s036"):
        load_v.wait()
    new_first = BETA1 * mbuf[...] + (1.0 - BETA1) * rotated
    new_second = BETA2 * vbuf[...] + (1.0 - BETA2) * rotated * rotated
    direction = new_first / (BIAS_ONE * jnp.sqrt(new_second * (1.0 / BIAS_TWO)) + BIAS_ONE * EPS)
    with jax.named_scope("s037"):
        nb[row] = direction.astype(BF16).reshape(2, hr, cb)
    gather_n = Gather8(lambda s, h: nb.at[s, h], lambda h: nb.at[row, h], lambda n: nb.at[pl.ds(0, n)], halves)
    with jax.named_scope("s038"):
        gather_n.start()
    om_ref[...] = new_first
    ov_ref[...] = new_second
    gather_gx1 = gather_wave(1)

    def k_part(r):
        return dot(ql_send[r], nb[r].reshape(rb, cb), NN)

    def k_pair(cx):
        return dot(ql_row[cx].reshape(rb, lb), nb[pl.ds(2 * cx, 2)].reshape(2 * rb, cb), NN)

    with jax.named_scope("s039"):
        gather_n.own_ready()
    acc[...] = k_pair(x)
    with jax.named_scope("s040"):
        gather_n.forward()
    gather_y[0].early()
    gather_y[0].later()
    gather_y[1].early()
    gather_y[1].later()
    with jax.named_scope("s041"):
        gather_gx1.forward()
    with jax.named_scope("s042"):
        gather_n.second()
    with jax.named_scope("s043"):
        gather_n.near_ready()
    acc[...] += k_pair(x_lft)
    acc[...] += k_pair(x_rgt)
    with jax.named_scope("s044"):
        gather_n.third()
    acc[...] += k_part(row_far)
    with jax.named_scope("s045"):
        gather_n.far_ready()
    with jax.named_scope("s046"):
        back = (acc[...] + k_part(prow_far)).astype(BF16)

    snd_u, rcv_u, rcv_f = sends(rin), new("recv"), [new("recv"), new("recv")]

    def half(k, h):
        return up.at[k, pl.ds(2 * h, 2)]

    u_far = [remote(up.at[far_c, j], rin.at[j // 2, j % 2], y_minus if j > 1 else y_plus, snd_u, rcv_f[j // 2])
             for j in range(4)]
    u_half = [remote(half(rgt_c, 1), rin.at[2], y_plus, snd_u, rcv_u),
              remote(half(lft_c, 0), rin.at[3], y_minus, snd_u, rcv_u)]
    u_sum = [remote(half(rgt_c, 0), rin.at[4], y_plus, snd_u, rcv_u),
             remote(half(lft_c, 1), rin.at[5], y_minus, snd_u, rcv_u)]

    def make_u(k):
        for j in (0, 2, 1, 3):
            up[k, j] = dot(back, qr_b[2 * k + j // 2, j % 2], NT)
            if k is far_c:
                u_far[j].start()

    with jax.named_scope("s047"):
        make_u(far_c)
    with jax.named_scope("s048"):
        make_u(rgt_c)
    u_half[0].start()
    with jax.named_scope("s049"):
        make_u(lft_c)
    u_half[1].start()
    with jax.named_scope("s050"):
        make_u(col)

    gather_y[0].forward()

    with jax.named_scope("s051"):
        for g in (gather_gx0, gather_gx1):
            g.second()
            g.third()
    right_g = gx[pl.ds(2 * col, 2)].reshape(2 * rb, kb)
    with jax.named_scope("s052"):
        lp[...] = dot(gx[...].reshape(nrow * rb, kb), right_g, NT, HIGHEST).reshape(nrow, rb, lb)
    snd_s, rcv_s = sends(lrecv), new("recv")
    with jax.named_scope("s053"):
        for k in range(nx):
            remote(lp.at[2 * k + 1 - core], lrecv.at[k], partner, snd_s, rcv_s).start()

    def add_r(cx, first=False):
        left = gx[pl.ds(2 * cx, 2)].reshape(2 * rb, kb)

        def body(h, _):
            part = dot(left, gy[pl.ds(2 * cx, 2), h].reshape(2 * rb, kb), TN, HIGHEST)
            old = or_ref[h]
            if first:
                old = BETA2 * old
            or_ref[h] = old + (1.0 - BETA2) * part
            return 0

        lax.fori_loop(0, 2, body, 0)

    gather_y[0].second()
    gather_y[1].forward()
    with jax.named_scope("s054"):
        for c in load_own + load_r:
            c.wait()
    with jax.named_scope("s055"):
        for g in gather_y:
            g.own_ready()
    with jax.named_scope("s056"):
        add_r(x, True)

    arrived(rin.at[0], rcv_f[0])
    up[rgt_c, :2] = up[rgt_c, :2] + rin[0]
    u_sum[0].start()
    arrived(rin.at[1], rcv_f[1])
    up[lft_c, 2:] = up[lft_c, 2:] + rin[1]
    u_sum[1].start()

    arrived(lrecv, rcv_s)
    with jax.named_scope("s057"):
        for k in range(nx):
            lp[2 * k + core] = lp[2 * k + core] + lrecv[k]
    snd_l, rcv_l = sends(lx.at[pl.ds(0, nx - 1)]), new("recv")
    with jax.named_scope("s058"):
        for dx in (1, nx - 1, 2):
            to = 2 * wrap(x + dx, nx) + core
            remote(lp.at[to], lx.at[x], {"row": to}, snd_l, rcv_l).start()

    gather_y[0].third()
    gather_y[1].second()
    with jax.named_scope("s059"):
        for g in gather_y:
            g.near_ready()
    with jax.named_scope("s060"):
        add_r(x_lft)
    gather_y[1].third()
    with jax.named_scope("s061"):
        add_r(x_rgt)
    with jax.named_scope("s062"):
        for g in gather_y:
            g.far_ready()
    with jax.named_scope("s063"):
        add_r(x_far)

    with jax.named_scope("s064"):
        load_l.wait()
    arrived(lx.at[pl.ds(0, nx - 1)], rcv_l)
    total = lp[row]
    with jax.named_scope("s065"):
        for dx in (1, 2, 3):
            total = total + lx[wrap(x + dx, nx)]
    ol_ref[...] = BETA2 * ol_ref[...] + (1.0 - BETA2) * total

    with jax.named_scope("s066"):
        load_w.wait()
    arrived(rin.at[pl.ds(0, 4)], rcv_u)
    with jax.named_scope("s067"):
        for j in range(4):
            cols = pl.ds(j * (cb // 4), cb // 4)
            others_sum = (rin[3, j] + rin[4, j]) if j < 2 else (rin[2, j - 2] + rin[5, j - 2])
            ow_ref[:, cols] = wbuf[:, cols] - LR * (up[col, j] + others_sum)

    assert tuple(counts.values()) == COUNTS
    with jax.named_scope("s068"):
        for c in pending:
            c.wait_send()


def write_out(w_ref, m_ref, v_ref, l_ref, r_ref, ow_ref, om_ref, ov_ref, ol_ref, or_ref, sem):
    kb = r_ref.shape[1]
    moves = [(w_ref, ow_ref), (m_ref, om_ref), (v_ref, ov_ref), (l_ref, ol_ref)]
    moves += [(r_ref.at[h], or_ref.at[:, pl.ds(h * kb, kb)]) for h in (0, 1)]
    copies = [pltpu.make_async_copy(a, b, sem.at[i]) for i, (a, b) in enumerate(moves)]
    for c in copies:
        c.start()
    for c in copies:
        c.wait()


def solution(mesh):
    nx, ny = mesh.shape["row"] // 2, mesh.shape["col"]
    tile_spec = P(("layer", "row"), "col")

    def local_step(*args):
        rb, cb = args[0].shape
        kb = args[7].shape[0]
        lb = args[6].shape[1]
        hr, nr = rb // 2, 2 * nx
        vm = pltpu.VMEM
        shapes = [args[0], args[2], args[3], args[4], args[5]]
        held = pl.pallas_call(
            functools.partial(kernel, nx, ny),
            out_shape=tuple(vm(s, F32) for s in [(rb, cb)] * 3 + [(rb, lb), (2, kb, kb)]),
            in_specs=[pl.BlockSpec(memory_space=pl.ANY)] * 8,
            out_specs=tuple([pl.BlockSpec(memory_space=pltpu.VMEM)] * 5),
            scratch_shapes=[
                vm((2, kb // 2, cb), F32),
                vm((nr, 2, kb // 2, cb), BF16),
                vm((nr, rb, kb), F32),
                vm((nr, rb, kb), BF16),
                vm((rb, lb), F32),
                vm((ny, 2, hr, lb), BF16),
                vm((nr, rb, lb // 2), BF16),
                vm((nr, ny, rb // ny, lb // 2), BF16),
                vm((nr, ny, rb // ny, kb), F32),
                vm((nr, 2, rb, kb), F32),
                vm((nr, 2, hr, cb), BF16),
                vm((nr, 2, hr, cb), BF16),
                vm((rb, cb), F32),
                vm((rb, cb), F32),
                vm((ny, 4, rb, cb // 4), F32),
                vm((6, 2, rb, cb // 4), F32),
                vm((nr, rb, lb), F32),
                vm((nx, rb, lb), F32),
                vm((nx, rb, lb), F32),
                vm((rb, cb), F32),
                vm((rb, cb), F32),
                vm((rb, cb), F32),
                *[pltpu.SemaphoreType.DMA((n,)) for n in COUNTS],
            ],
            compiler_params=pltpu.CompilerParams(
                collective_id=0, has_side_effects=True, vmem_limit_bytes=61600 * 1024),
        )(*args)
        return pl.pallas_call(
            write_out,
            out_shape=tuple(jax.ShapeDtypeStruct(s.shape, s.dtype) for s in shapes),
            in_specs=[pl.BlockSpec(memory_space=pltpu.VMEM)] * 5,
            out_specs=tuple([pl.BlockSpec(memory_space=pl.ANY)] * 5),
            scratch_shapes=[pltpu.SemaphoreType.DMA((6,))],
            compiler_params=pltpu.CompilerParams(vmem_limit_bytes=4 * 1024 * 1024),
        )(*held)

    return jax.shard_map(local_step, mesh=mesh, in_specs=(tile_spec,) * 8, out_specs=(tile_spec,) * 5, check_vma=False)
```

```python
import functools

import jax
import jax.numpy as jnp
from jax import lax
from jax.experimental import pallas as pl
from jax.experimental.pallas import tpu as pltpu
from jax.sharding import PartitionSpec as P

BETA1 = 0.9
BETA2 = 0.9
EPS = 1e-8
LR = 0.1
STEP = 10
BIAS_ONE = 1.0 - BETA1 ** STEP
BIAS_TWO = 1.0 - BETA2 ** STEP
MESH = pl.DeviceIdType.MESH
HIGHEST = lax.Precision.HIGHEST
F32 = jnp.float32
BF16 = jnp.bfloat16
NN = (((1,), (0,)), ((), ()))
TN = (((0,), (0,)), ((), ()))
NT = (((1,), (1,)), ((), ()))
COUNTS = (16, 80, 15)


def dot(a, b, dims, precision=None):
    return lax.dot_general(a, b, dims, precision=precision, preferred_element_type=F32)


def kernel(nx, ny, w_ref, g_ref, m_ref, v_ref, l_ref, r_ref, ql_ref, qr_ref,
           ow_ref, om_ref, ov_ref, ol_ref, or_ref,
           qr_f, qr_b, qr_t, grow, growb, ql_f, ql_row, ql_send, ql_col, gx, gy, hb, nb,
           acc, gacc, up, rin, lp, lrecv, lx, wbuf, mbuf, vbuf,
           send_sem, recv_sem, local_sem):
    row = lax.axis_index("row")
    col = lax.axis_index("col")
    core = lax.rem(row, 2)
    x = lax.div(row, 2)
    nrow = 2 * nx
    rb, cb = w_ref.shape
    kb = qr_ref.shape[0]
    lb = ql_ref.shape[1]
    hr = rb // 2
    qb = rb // ny

    def wrap(v, n):
        return lax.rem(v + n, n)

    x_plus = {"row": wrap(row + 2, nrow)}
    x_minus = {"row": wrap(row - 2, nrow)}
    partner = {"row": row + 1 - 2 * core}
    y_plus = {"col": wrap(col + 1, ny)}
    y_minus = {"col": wrap(col - 1, ny)}
    prow = row + 1 - 2 * core
    counts = {"send": 0, "recv": 0, "local": 0}
    pending = []

    def new(kind):
        counts[kind] += 1
        return counts[kind] - 1

    def remote(src, dst, device, send, recv=None):
        recv = new("recv") if recv is None else recv
        return pltpu.make_async_remote_copy(
            src_ref=src, dst_ref=dst, send_sem=send_sem.at[send], recv_sem=recv_sem.at[recv],
            device_id=device, device_id_type=MESH)

    def sends(span):
        i = new("send")
        pending.append(remote(span, span, partner, i, 0))
        return i

    def arrived(span, recv):
        remote(span, span, partner, 0, recv).wait_recv()

    def local(src, dst, sem=None):
        copy = pltpu.make_async_copy(src, dst, local_sem.at[new("local") if sem is None else sem])
        copy.start()
        return copy

    class Gather8:
        def __init__(self, at, own, span, cut=lambda ref: [ref], first=lambda ref: [ref]):
            lft, rgt, far = wrap(row - 2, nrow), wrap(row + 2, nrow), wrap(row + 4, nrow)
            self.span = span
            snd = sends(span(7))
            self.second_sem, self.own_sem, self.near_sem, self.far_sem = (new("recv") for _ in range(4))
            self.a0 = [remote(c, d, x_plus, snd) for c, d in zip(first(own(0)), first(at(row, 0)))]
            self.b1 = [remote(c, d, x_minus, snd) for c, d in zip(first(own(1))[::-1], first(at(row, 1))[::-1])]
            self.a1 = remote(own(1), at(row, 1), x_plus, snd, self.second_sem)
            self.b0 = remote(own(0), at(row, 0), x_minus, snd, self.second_sem)
            self.p = [remote(own(h), at(row, h), partner, snd, self.own_sem) for h in (0, 1)]
            self.f0 = [remote(c, c, x_plus, snd) for c in cut(at(lft, 0))]
            self.f1 = [remote(c, c, x_minus, snd) for c in cut(at(rgt, 1))]
            self.near = [remote(at(s, h), at(s, h), partner, snd, self.near_sem)
                         for s, h in ((lft, 0), (rgt, 1), (lft, 1), (rgt, 0))]
            self.last = [[remote(c, c, partner, snd, self.far_sem) for c in cut(at(far, h))] for h in (0, 1)]

        def early(self):
            for c in (*self.a0, *self.b1):
                c.start()

        def later(self):
            self.a1.start()
            self.b0.start()

        def to_partner(self):
            for c in self.p:
                c.start()

        def start(self):
            self.early()
            self.later()
            self.to_partner()

        def forward(self):
            for c in self.a0:
                c.wait_recv()
            for c in self.f0:
                c.start()
            self.near[0].start()
            for c in self.b1:
                c.wait_recv()
            for c in self.f1:
                c.start()
            self.near[1].start()

        def second(self):
            arrived(self.span(1), self.second_sem)
            self.near[2].start()
            self.near[3].start()

        def third(self):
            for i in range(len(self.f0)):
                self.f0[i].wait_recv()
                self.last[0][i].start()
                self.f1[i].wait_recv()
                self.last[1][i].start()

        def own_ready(self):
            arrived(self.span(1), self.own_sem)

        def near_ready(self):
            arrived(self.span(2), self.near_sem)

        def far_ready(self):
            arrived(self.span(1), self.far_sem)

    class Gather4:
        def __init__(self, at, own, span):
            lft, rgt = wrap(col - 1, ny), wrap(col + 1, ny)
            self.span = span
            snd = sends(span(3))
            self.second_sem, self.third_sem = new("recv"), new("recv")
            self.a0 = remote(own(0), at(col, 0), y_plus, snd)
            self.b1 = remote(own(1), at(col, 1), y_minus, snd)
            self.a1 = remote(own(1), at(col, 1), y_plus, snd, self.second_sem)
            self.b0 = remote(own(0), at(col, 0), y_minus, snd, self.second_sem)
            self.f0 = remote(at(lft, 0), at(lft, 0), y_plus, snd, self.third_sem)
            self.f1 = remote(at(rgt, 1), at(rgt, 1), y_minus, snd, self.third_sem)

        def start(self):
            for c in (self.a0, self.b1, self.a1, self.b0):
                c.start()

        def forward(self):
            self.a0.wait_recv()
            self.f0.start()
            self.b1.wait_recv()
            self.f1.start()

        def second(self):
            arrived(self.span(1), self.second_sem)

        def third(self):
            arrived(self.span(1), self.third_sem)

    def peers():
        for dx in (1, nx - 1, 2, 0):
            for dc in (0, 1):
                if dx == 0 and dc == 0:
                    continue
                px = wrap(x + dx, nx)
                pc = core if dc == 0 else 1 - core
                yield 2 * px + pc, px, pc

    hk, qk = kb // 2, kb // 4
    load_qr = {(h, j): local(qr_ref.at[pl.ds(h * hk + j * qk, qk)], qr_f.at[h, pl.ds(j * qk, qk)])
               for h, j in ((0, 0), (1, 1), (0, 1), (1, 0))}

    barrier = pltpu.get_barrier_semaphore()
    others = [r for r, _, _ in peers()]
    for r in others:
        pl.semaphore_signal(barrier, inc=1, device_id={"row": r}, device_id_type=MESH)
    with jax.named_scope("s000"):
        for d in (y_plus, y_minus):
            pl.semaphore_signal(barrier, inc=1, device_id=d, device_id_type=MESH)

    load_ql = local(ql_ref, ql_f)
    load_g = [local(g_ref.at[:, pl.ds(h * kb, kb)], grow.at[2 * col + h]) for h in (0, 1)]

    def round_qr(h, j):
        load_qr[h, j].wait()
        qr_b[row, h, pl.ds(j * qk, qk)] = qr_f[h, pl.ds(j * qk, qk)].astype(BF16)

    round_qr(0, 0)
    round_qr(1, 1)
    with jax.named_scope("s001"):
        pl.semaphore_wait(barrier, len(others) + 2)

    gather_qr = Gather8(lambda s, h: qr_b.at[s, h], lambda h: qr_b.at[row, h], lambda n: qr_b.at[pl.ds(0, n)],
                        lambda ref: [ref.at[pl.ds(j * kb // 8, kb // 8)] for j in range(4)],
                        lambda ref: [ref.at[pl.ds(j * qk, qk)] for j in (0, 1)])
    gather_qr.a0[0].start()
    gather_qr.b1[0].start()
    round_qr(0, 1)
    round_qr(1, 0)
    gather_qr.a0[1].start()
    gather_qr.b1[1].start()
    with jax.named_scope("s002"):
        gather_qr.later()
    with jax.named_scope("s003"):
        gather_qr.to_partner()
    gather_ql = Gather4(lambda s, h: ql_row.at[s, h], lambda h: ql_row.at[col, h], lambda n: ql_row.at[pl.ds(0, n)])
    with jax.named_scope("s004"):
        load_ql.wait()
    ql_row[col] = ql_f[...].astype(BF16).reshape(2, hr, lb)
    with jax.named_scope("s005"):
        gather_ql.start()
    with jax.named_scope("s006"):
        for c in load_g:
            c.wait()
    gather_g = Gather4(lambda s, h: grow.at[2 * s + h], lambda h: grow.at[2 * col + h],
                       lambda n: grow.at[pl.ds(0, 2 * n)])
    with jax.named_scope("s007"):
        gather_g.start()

    load_m = local(m_ref, mbuf)
    load_v = local(v_ref, vbuf)
    load_own = [local(g_ref.at[:, pl.ds(h * kb, kb)], gy.at[row, h]) for h in (0, 1)]
    load_w = local(w_ref, wbuf)
    load_l = local(l_ref, ol_ref)
    load_r = [local(r_ref.at[:, pl.ds(h * kb, kb)], or_ref.at[h]) for h in (0, 1)]

    def cast_block(s):
        growb[s] = grow[s].astype(BF16)

    with jax.named_scope("s008"):
        for h in (0, 1):
            cast_block(2 * col + h)

    lft_c, rgt_c, far_c = wrap(col - 1, ny), wrap(col + 1, ny), wrap(col + 2, ny)
    x_lft, x_rgt, x_far = wrap(x - 1, nx), wrap(x + 1, nx), wrap(x + 2, nx)
    half_l = lb // 2
    quarter = pl.ds(pl.multiple_of(col * qb, qb), qb)
    row_far = wrap(row + 4, nrow)
    prow_far = row_far + 1 - 2 * core
    with jax.named_scope("s009"):
        gather_ql.forward()
    with jax.named_scope("s010"):
        gather_g.forward()
    with jax.named_scope("s011"):
        gather_qr.forward()
    with jax.named_scope("s012"):
        gather_ql.second()
    with jax.named_scope("s013"):
        gather_ql.third()

    with jax.named_scope("s014"):
        for k in range(ny):
            block = ql_row[k].reshape(rb, lb)
            for h in (0, 1):
                ql_send[2 * k + h] = block[:, h * half_l:(h + 1) * half_l]
    ql_col[row, col] = ql_send[row, quarter]
    snd_ql, rcv_ql = sends(ql_col.at[pl.ds(0, nrow - 1), 0]), new("recv")
    for r, _, _ in peers():
        remote(ql_send.at[r, quarter], ql_col.at[row, col], {"row": r}, snd_ql, rcv_ql).start()

    cast_block(2 * lft_c)
    cast_block(2 * rgt_c + 1)
    with jax.named_scope("s015"):
        gather_g.second()
    cast_block(2 * lft_c + 1)
    cast_block(2 * rgt_c)
    with jax.named_scope("s016"):
        gather_g.third()

    eb = qb // 2
    gx[row, col] = grow[row, quarter]
    snd_gx = [sends(gx.at[pl.ds(0, nrow - 1), 0, pl.ds(0, eb)]) for _ in (0, 1)]
    rcv_gx = [new("recv") for _ in (0, 1)]

    def send_gx(w):
        here = pl.ds(pl.multiple_of(col * qb + w * eb, eb), eb)
        for r, _, _ in peers():
            remote(grow.at[r, here], gx.at[row, col, pl.ds(w * eb, eb)], {"row": r}, snd_gx[w], rcv_gx[w]).start()

    def gather_wave(w):
        there, half = pl.ds(w * eb, eb), nrow // 2
        arrived(gx.at[pl.ds(0, nrow - 1), 0, pl.ds(0, eb)], rcv_gx[w])
        g = Gather4(lambda s, h: gx.at[pl.ds(h * half, half), s, there],
                    lambda h: gx.at[pl.ds(h * half, half), col, there],
                    lambda n: gx.at[:, pl.ds(0, n), there])
        g.start()
        return g

    send_gx(0)

    def rows_of(w):
        return pl.ds(w * hr, hr)

    gather_y = [Gather8(lambda s, h, w=w: gy.at[s, h, rows_of(w)], lambda h, w=w: grow.at[2 * col + h, rows_of(w)],
                        lambda n, w=w: gy.at[pl.ds(0, n), :, rows_of(w)]) for w in (0, 1)]
    with jax.named_scope("s017"):
        for g in gather_y:
            g.to_partner()
    cast_block(2 * far_c)
    cast_block(2 * far_c + 1)

    def turn(k):
        for j in range(4):
            qr_t[k, j] = qr_b[2 * k + j // 2, j % 2].T

    def h_part(r):
        return dot(growb[r], qr_b[r].reshape(kb, cb), NN)

    with jax.named_scope("s018"):
        gather_qr.own_ready()
    acc[...] = h_part(2 * x) + h_part(2 * x + 1)
    with jax.named_scope("s019"):
        gather_qr.second()
    with jax.named_scope("s020"):
        gather_qr.near_ready()
    acc[...] += h_part(2 * x_lft) + h_part(2 * x_lft + 1)
    acc[...] += h_part(2 * x_rgt) + h_part(2 * x_rgt + 1)
    turn(x)
    turn(x_lft)
    turn(x_rgt)
    with jax.named_scope("s021"):
        gather_qr.third()
    acc[...] += h_part(row_far)
    with jax.named_scope("s022"):
        gather_qr.far_ready()
    with jax.named_scope("s023"):
        hb[row] = (acc[...] + h_part(prow_far)).astype(BF16).reshape(2, hr, cb)

    def halves(ref):
        return [ref.at[pl.ds(j * hr // 2, hr // 2)] for j in (0, 1)]

    gather_h = Gather8(lambda s, h: hb.at[s, h], lambda h: hb.at[row, h], lambda n: hb.at[pl.ds(0, n)], halves)
    with jax.named_scope("s024"):
        gather_h.start()

    arrived(ql_col.at[pl.ds(0, nrow - 1), 0], rcv_ql)
    gather_qc = Gather4(
        lambda s, h: ql_col.at[pl.ds(h * (nrow // 2), nrow // 2), s],
        lambda h: ql_col.at[pl.ds(h * (nrow // 2), nrow // 2), col],
        lambda n: ql_col.at[:, pl.ds(0, n)])
    with jax.named_scope("s025"):
        gather_qc.start()
    with jax.named_scope("s026"):
        gather_qc.forward()
    gather_gx0 = gather_wave(0)

    def g_part(r):
        return dot(ql_col[r].reshape(rb, rb), hb[r].reshape(rb, cb), TN)

    def g_pair(cx):
        left = ql_col[pl.ds(2 * cx, 2)].reshape(2 * rb, rb)
        return dot(left, hb[pl.ds(2 * cx, 2)].reshape(2 * rb, cb), TN)

    with jax.named_scope("s027"):
        gather_h.forward()
    send_gx(1)
    turn(x_far)
    with jax.named_scope("s028"):
        gather_qc.second()
    with jax.named_scope("s029"):
        gather_qc.third()
    with jax.named_scope("s030"):
        gather_h.own_ready()
    gacc[...] = g_pair(x)
    with jax.named_scope("s031"):
        gather_h.second()
    with jax.named_scope("s032"):
        gather_gx0.forward()
    with jax.named_scope("s033"):
        gather_h.near_ready()
    gacc[...] += g_pair(x_lft)
    gacc[...] += g_pair(x_rgt)
    with jax.named_scope("s034"):
        gather_h.third()
    gacc[...] += g_part(row_far)
    with jax.named_scope("s035"):
        gather_h.far_ready()
    rotated = gacc[...] + g_part(prow_far)

    with jax.named_scope("s036"):
        load_m.wait()
    with jax.named_scope("s037"):
        load_v.wait()
    new_first = BETA1 * mbuf[...] + (1.0 - BETA1) * rotated
    new_second = BETA2 * vbuf[...] + (1.0 - BETA2) * rotated * rotated
    direction = new_first / (BIAS_ONE * jnp.sqrt(new_second * (1.0 / BIAS_TWO)) + BIAS_ONE * EPS)
    with jax.named_scope("s038"):
        nb[row] = direction.astype(BF16).reshape(2, hr, cb)
    gather_n = Gather8(lambda s, h: nb.at[s, h], lambda h: nb.at[row, h], lambda n: nb.at[pl.ds(0, n)], halves)
    with jax.named_scope("s039"):
        gather_n.start()
    om_ref[...] = new_first
    ov_ref[...] = new_second
    gather_gx1 = gather_wave(1)

    def k_part(r):
        return dot(ql_send[r], nb[r].reshape(rb, cb), NN)

    def k_pair(cx):
        return dot(ql_row[cx].reshape(rb, lb), nb[pl.ds(2 * cx, 2)].reshape(2 * rb, cb), NN)

    with jax.named_scope("s040"):
        gather_n.own_ready()
    acc[...] = k_pair(x)
    with jax.named_scope("s041"):
        gather_n.forward()
    gather_y[0].early()
    gather_y[0].later()
    gather_y[1].early()
    gather_y[1].later()
    with jax.named_scope("s042"):
        gather_gx1.forward()
    with jax.named_scope("s043"):
        gather_n.second()
    with jax.named_scope("s044"):
        gather_n.near_ready()
    acc[...] += k_pair(x_lft)
    acc[...] += k_pair(x_rgt)
    with jax.named_scope("s045"):
        gather_n.third()
    acc[...] += k_part(row_far)
    with jax.named_scope("s046"):
        gather_n.far_ready()
    with jax.named_scope("s047"):
        back = (acc[...] + k_part(prow_far)).astype(BF16)

    snd_u, rcv_u, rcv_f = sends(rin), new("recv"), [new("recv"), new("recv")]

    def half(k, h):
        return up.at[k, pl.ds(2 * h, 2)]

    u_far = [remote(half(far_c, 0), rin.at[0], y_plus, snd_u, rcv_f[0]),
             remote(half(far_c, 1), rin.at[1], y_minus, snd_u, rcv_f[1])]
    u_half = [remote(half(rgt_c, 1), rin.at[2], y_plus, snd_u, rcv_u),
              remote(half(lft_c, 0), rin.at[3], y_minus, snd_u, rcv_u)]
    u_sum = [remote(half(rgt_c, 0), rin.at[4], y_plus, snd_u, rcv_u),
             remote(half(lft_c, 1), rin.at[5], y_minus, snd_u, rcv_u)]

    def make_u(k):
        for j in range(4):
            up[k, j] = dot(back, qr_t[k, j], NN)

    with jax.named_scope("s048"):
        make_u(far_c)
    with jax.named_scope("s049"):
        for c in u_far:
            c.start()
    with jax.named_scope("s050"):
        make_u(rgt_c)
    u_half[0].start()
    with jax.named_scope("s051"):
        make_u(lft_c)
    u_half[1].start()
    gather_y[0].forward()
    with jax.named_scope("s052"):
        make_u(col)

    with jax.named_scope("s053"):
        for g in (gather_gx0, gather_gx1):
            g.second()
            g.third()
    right_g = gx[pl.ds(2 * col, 2)].reshape(2 * rb, kb)
    with jax.named_scope("s054"):
        lp[...] = dot(gx[...].reshape(nrow * rb, kb), right_g, NT, HIGHEST).reshape(nrow, rb, lb)
    snd_s, rcv_s = sends(lrecv), new("recv")
    with jax.named_scope("s055"):
        for k in range(nx):
            remote(lp.at[2 * k + 1 - core], lrecv.at[k], partner, snd_s, rcv_s).start()

    def add_r(cx, first=False):
        left = gx[pl.ds(2 * cx, 2)].reshape(2 * rb, kb)

        def body(h, _):
            part = dot(left, gy[pl.ds(2 * cx, 2), h].reshape(2 * rb, kb), TN, HIGHEST)
            old = or_ref[h]
            if first:
                old = BETA2 * old
            or_ref[h] = old + (1.0 - BETA2) * part
            return 0

        lax.fori_loop(0, 2, body, 0)

    gather_y[0].second()
    gather_y[1].forward()
    with jax.named_scope("s056"):
        for c in load_own + load_r:
            c.wait()
    with jax.named_scope("s057"):
        for g in gather_y:
            g.own_ready()
    with jax.named_scope("s058"):
        add_r(x, True)

    arrived(rin.at[0], rcv_f[0])
    up[rgt_c, :2] = up[rgt_c, :2] + rin[0]
    u_sum[0].start()
    arrived(rin.at[1], rcv_f[1])
    up[lft_c, 2:] = up[lft_c, 2:] + rin[1]
    u_sum[1].start()

    arrived(lrecv, rcv_s)
    with jax.named_scope("s059"):
        for k in range(nx):
            lp[2 * k + core] = lp[2 * k + core] + lrecv[k]
    snd_l, rcv_l = sends(lx.at[pl.ds(0, nx - 1)]), new("recv")
    with jax.named_scope("s060"):
        for dx in (1, nx - 1, 2):
            to = 2 * wrap(x + dx, nx) + core
            remote(lp.at[to], lx.at[x], {"row": to}, snd_l, rcv_l).start()

    gather_y[1].second()
    with jax.named_scope("s061"):
        for g in gather_y:
            g.near_ready()
    with jax.named_scope("s062"):
        add_r(x_lft)
    gather_y[0].third()
    with jax.named_scope("s063"):
        add_r(x_rgt)
    gather_y[1].third()
    with jax.named_scope("s064"):
        for g in gather_y:
            g.far_ready()
    with jax.named_scope("s065"):
        add_r(x_far)

    with jax.named_scope("s066"):
        load_l.wait()
    arrived(lx.at[pl.ds(0, nx - 1)], rcv_l)
    total = lp[row]
    with jax.named_scope("s067"):
        for dx in (1, 2, 3):
            total = total + lx[wrap(x + dx, nx)]
    ol_ref[...] = BETA2 * ol_ref[...] + (1.0 - BETA2) * total

    with jax.named_scope("s068"):
        load_w.wait()
    arrived(rin.at[pl.ds(0, 4)], rcv_u)
    with jax.named_scope("s069"):
        for j in range(4):
            cols = pl.ds(j * (cb // 4), cb // 4)
            others_sum = (rin[3, j] + rin[4, j]) if j < 2 else (rin[2, j - 2] + rin[5, j - 2])
            ow_ref[:, cols] = wbuf[:, cols] - LR * (up[col, j] + others_sum)

    assert tuple(counts.values()) == COUNTS
    with jax.named_scope("s070"):
        for c in pending:
            c.wait_send()


def write_out(w_ref, m_ref, v_ref, l_ref, r_ref, ow_ref, om_ref, ov_ref, ol_ref, or_ref, sem):
    kb = r_ref.shape[1]
    moves = [(w_ref, ow_ref), (m_ref, om_ref), (v_ref, ov_ref), (l_ref, ol_ref)]
    moves += [(r_ref.at[h], or_ref.at[:, pl.ds(h * kb, kb)]) for h in (0, 1)]
    copies = [pltpu.make_async_copy(a, b, sem.at[i]) for i, (a, b) in enumerate(moves)]
    for c in copies:
        c.start()
    for c in copies:
        c.wait()


def solution(mesh):
    nx, ny = mesh.shape["row"] // 2, mesh.shape["col"]
    tile_spec = P(("layer", "row"), "col")

    def local_step(*args):
        rb, cb = args[0].shape
        kb = args[7].shape[0]
        lb = args[6].shape[1]
        hr, nr = rb // 2, 2 * nx
        vm = pltpu.VMEM
        shapes = [args[0], args[2], args[3], args[4], args[5]]
        held = pl.pallas_call(
            functools.partial(kernel, nx, ny),
            out_shape=tuple(vm(s, F32) for s in [(rb, cb)] * 3 + [(rb, lb), (2, kb, kb)]),
            in_specs=[pl.BlockSpec(memory_space=pl.ANY)] * 8,
            out_specs=tuple([pl.BlockSpec(memory_space=pltpu.VMEM)] * 5),
            scratch_shapes=[
                vm((2, kb // 2, cb), F32),
                vm((nr, 2, kb // 2, cb), BF16),
                vm((nx, 4, cb, kb // 2), BF16),
                vm((nr, rb, kb), F32),
                vm((nr, rb, kb), BF16),
                vm((rb, lb), F32),
                vm((ny, 2, hr, lb), BF16),
                vm((nr, rb, lb // 2), BF16),
                vm((nr, ny, rb // ny, lb // 2), BF16),
                vm((nr, ny, rb // ny, kb), F32),
                vm((nr, 2, rb, kb), F32),
                vm((nr, 2, hr, cb), BF16),
                vm((nr, 2, hr, cb), BF16),
                vm((rb, cb), F32),
                vm((rb, cb), F32),
                vm((ny, 4, rb, cb // 4), F32),
                vm((6, 2, rb, cb // 4), F32),
                vm((nr, rb, lb), F32),
                vm((nx, rb, lb), F32),
                vm((nx, rb, lb), F32),
                vm((rb, cb), F32),
                vm((rb, cb), F32),
                vm((rb, cb), F32),
                *[pltpu.SemaphoreType.DMA((n,)) for n in COUNTS],
            ],
            compiler_params=pltpu.CompilerParams(
                collective_id=0, has_side_effects=True, vmem_limit_bytes=61600 * 1024),
        )(*args)
        return pl.pallas_call(
            write_out,
            out_shape=tuple(jax.ShapeDtypeStruct(s.shape, s.dtype) for s in shapes),
            in_specs=[pl.BlockSpec(memory_space=pltpu.VMEM)] * 5,
            out_specs=tuple([pl.BlockSpec(memory_space=pl.ANY)] * 5),
            scratch_shapes=[pltpu.SemaphoreType.DMA((6,))],
            compiler_params=pltpu.CompilerParams(vmem_limit_bytes=4 * 1024 * 1024),
        )(*held)

    return jax.shard_map(local_step, mesh=mesh, in_specs=(tile_spec,) * 8, out_specs=(tile_spec,) * 5, check_vma=False)
```

```python
import functools

import jax
import jax.numpy as jnp
from jax import lax
from jax.experimental import pallas as pl
from jax.experimental.pallas import tpu as pltpu
from jax.sharding import PartitionSpec as P

BETA1 = 0.9
BETA2 = 0.9
EPS = 1e-8
LR = 0.1
STEP = 10
BIAS_ONE = 1.0 - BETA1 ** STEP
BIAS_TWO = 1.0 - BETA2 ** STEP
MESH = pl.DeviceIdType.MESH
HIGHEST = lax.Precision.HIGHEST
F32 = jnp.float32
BF16 = jnp.bfloat16
NN = (((1,), (0,)), ((), ()))
TN = (((0,), (0,)), ((), ()))
NT = (((1,), (1,)), ((), ()))
COUNTS = (7, 55, 7)


def dot(a, b, dims, precision=None):
    return lax.dot_general(a, b, dims, precision=precision, preferred_element_type=F32)


def kernel(nx, ny, w_ref, g_ref, m_ref, v_ref, l_ref, r_ref, ql_ref, qr_ref,
           ow_ref, om_ref, ov_ref, ol_ref, or_ref,
           qr_f, qr_b, qr_t, grow, growb, ql_f, ql_row, ql_send, ql_col, gx, gy, hb, nb,
           acc, gacc, up, rin, lp, lrecv, lx, wbuf, mbuf, vbuf,
           send_sem, recv_sem, local_sem):
    row = lax.axis_index("row")
    col = lax.axis_index("col")
    core = lax.rem(row, 2)
    x = lax.div(row, 2)
    nrow = 2 * nx
    rb, cb = w_ref.shape
    kb = qr_ref.shape[0]
    lb = ql_ref.shape[1]
    hr = rb // 2
    qb = rb // ny

    def wrap(v, n):
        return lax.rem(v + n, n)

    x_plus = {"row": wrap(row + 2, nrow)}
    x_minus = {"row": wrap(row - 2, nrow)}
    partner = {"row": row + 1 - 2 * core}
    y_plus = {"col": wrap(col + 1, ny)}
    y_minus = {"col": wrap(col - 1, ny)}
    prow = row + 1 - 2 * core
    counts = {"send": 0, "recv": 0, "local": 0}
    pending = []

    def new(kind):
        counts[kind] += 1
        return counts[kind] - 1

    def remote(src, dst, device, send, recv=None):
        recv = new("recv") if recv is None else recv
        return pltpu.make_async_remote_copy(
            src_ref=src, dst_ref=dst, send_sem=send_sem.at[send], recv_sem=recv_sem.at[recv],
            device_id=device, device_id_type=MESH)

    def sends(span):
        i = new("send")
        pending.append(remote(span, span, partner, i, 0))
        return i

    snd_qr, snd_rows = sends(qr_b.at[pl.ds(0, nrow - 1)]), sends(qr_b.at[pl.ds(0, nrow - 1)])
    snd_g, snd_small = sends(qr_b.at[pl.ds(0, 3)]), sends(gx.at[pl.ds(0, 5)])
    snd_ql, snd_gx = sends(ql_col.at[pl.ds(0, nrow - 1), 0]), sends(gx.at[pl.ds(0, nrow - 1), 0])
    snd_u = sends(rin)

    def arrived(span, recv):
        remote(span, span, partner, 0, recv).wait_recv()

    def local(src, dst, sem=None):
        copy = pltpu.make_async_copy(src, dst, local_sem.at[new("local") if sem is None else sem])
        copy.start()
        return copy

    class Gather8:
        def __init__(self, at, own, span, snd, cut=lambda ref: [ref], first=lambda ref: [ref], share=None):
            lft, rgt, far = wrap(row - 2, nrow), wrap(row + 2, nrow), wrap(row + 4, nrow)
            self.span = span
            self.at, self.lft, self.rgt = at, lft, rgt
            self.second_sem, self.a0_sem, self.b1_sem = (new("recv") for _ in range(3))
            self.own_sem, self.near_sem, self.far_sem = share or [new("recv") for _ in range(3)]
            self.a0 = [remote(c, d, x_plus, snd, self.a0_sem) for c, d in zip(first(own(0)), first(at(row, 0)))]
            self.b1 = [remote(c, d, x_minus, snd, self.b1_sem) for c, d in zip(first(own(1)), first(at(row, 1)))]
            self.a1 = remote(own(1), at(row, 1), x_plus, snd, self.second_sem)
            self.b0 = remote(own(0), at(row, 0), x_minus, snd, self.second_sem)
            self.p = [remote(own(h), at(row, h), partner, snd, self.own_sem) for h in (0, 1)]
            self.f_sem = [new("recv") for _ in cut(at(lft, 0))]
            self.f0 = [remote(c, c, x_plus, snd, i) for c, i in zip(cut(at(lft, 0)), self.f_sem)]
            self.f1 = [remote(c, c, x_minus, snd, i) for c, i in zip(cut(at(rgt, 1)), self.f_sem)]
            self.part = cut(at(far, 0))
            if len(self.part) > 1:
                self.two = at(far, 0).at[pl.ds(0, 2 * self.part[0].shape[0])]
            self.near = [remote(at(s, h), at(s, h), partner, snd, self.near_sem)
                         for s, h in ((lft, 0), (rgt, 1), (lft, 1), (rgt, 0))]
            self.last = [[remote(c, c, partner, snd, self.far_sem) for c in cut(at(far, h))] for h in (0, 1)]

        def early(self):
            for c in (*self.a0, *self.b1):
                c.start()

        def later(self):
            self.a1.start()
            self.b0.start()

        def to_partner(self):
            for c in self.p:
                c.start()

        def start(self):
            self.early()
            self.later()
            self.to_partner()

        def forward(self):
            arrived(self.at(self.lft, 0), self.a0_sem)
            for c in self.f0:
                c.start()
            self.near[0].start()
            arrived(self.at(self.rgt, 1), self.b1_sem)
            for c in self.f1:
                c.start()
            self.near[1].start()

        def second(self):
            arrived(self.span(1), self.second_sem)
            self.near[2].start()
            self.near[3].start()

        def third(self):
            for i, (c, d) in enumerate(zip(*self.last)):
                both = self.f_span(i)
                arrived(both, self.f_sem[i])
                c.start()
                d.start()

        def f_span(self, i):
            return self.span(1) if len(self.part) == 1 else self.two

        def own_ready(self):
            arrived(self.span(1), self.own_sem)

        def near_ready(self):
            arrived(self.span(2), self.near_sem)

        def far_ready(self):
            arrived(self.span(1), self.far_sem)

    class Gather4:
        def __init__(self, at, own, span, snd, share=None):
            lft, rgt = wrap(col - 1, ny), wrap(col + 1, ny)
            self.span = span
            first = new("recv")
            self.first_sem = first
            self.second_sem, self.third_sem = (new("recv"), new("recv")) if share is None else (share, share)
            self.a0 = remote(own(0), at(col, 0), y_plus, snd, first)
            self.b1 = remote(own(1), at(col, 1), y_minus, snd, first)
            self.a1 = remote(own(1), at(col, 1), y_plus, snd, self.second_sem)
            self.b0 = remote(own(0), at(col, 0), y_minus, snd, self.second_sem)
            self.f0 = remote(at(lft, 0), at(lft, 0), y_plus, snd, self.third_sem)
            self.f1 = remote(at(rgt, 1), at(rgt, 1), y_minus, snd, self.third_sem)

        def start(self):
            for c in (self.a0, self.b1, self.a1, self.b0):
                c.start()

        def forward(self):
            arrived(self.span(1), self.first_sem)
            self.f0.start()
            self.f1.start()

        def second(self):
            arrived(self.span(1), self.second_sem)

        def third(self):
            arrived(self.span(1), self.third_sem)

        def rest(self):
            arrived(self.span(2), self.second_sem)

    def peers():
        for dx in (1, nx - 1, 2, 0):
            for dc in (0, 1):
                if dx == 0 and dc == 0:
                    continue
                px = wrap(x + dx, nx)
                pc = core if dc == 0 else 1 - core
                yield 2 * px + pc, px, pc

    hk, qk = kb // 2, kb // 4
    sem_qr, sem_g, sem_mid, sem_r = [new("local"), new("local")], new("local"), new("local"), new("local")
    with jax.named_scope("s000"):
        for i, (h, j) in enumerate(((0, 0), (1, 0), (0, 1), (1, 1))):
            local(qr_ref.at[pl.ds(h * hk + j * qk, qk)], qr_f.at[h, pl.ds(j * qk, qk)], sem_qr[i // 2])

    barrier = pltpu.get_barrier_semaphore()
    others = [r for r, _, _ in peers()]
    for r in others:
        pl.semaphore_signal(barrier, inc=1, device_id={"row": r}, device_id_type=MESH)
    with jax.named_scope("s001"):
        for d in (y_plus, y_minus):
            pl.semaphore_signal(barrier, inc=1, device_id=d, device_id_type=MESH)

    load_ql = local(ql_ref, ql_f)
    with jax.named_scope("s002"):
        for h in (0, 1):
            local(g_ref.at[:, pl.ds(h * kb, kb)], grow.at[2 * col + h], sem_g)

    def loaded(ref, sem):
        pltpu.make_async_remote_copy(
            src_ref=ref, dst_ref=ref, send_sem=send_sem.at[0], recv_sem=local_sem.at[sem],
            device_id=partner, device_id_type=MESH).wait_recv()

    def round_qr(j):
        loaded(qr_f.at[0], sem_qr[j])
        for h in (0, 1):
            qr_b[row, h, pl.ds(j * qk, qk)] = qr_f[h, pl.ds(j * qk, qk)].astype(BF16)

    round_qr(0)
    with jax.named_scope("s003"):
        pl.semaphore_wait(barrier, len(others) + 2)

    gather_qr = Gather8(lambda s, h: qr_b.at[s, h], lambda h: qr_b.at[row, h], lambda n: qr_b.at[pl.ds(0, n)], snd_qr,
                        lambda ref: [ref.at[pl.ds(j * kb // 8, kb // 8)] for j in range(4)],
                        lambda ref: [ref.at[pl.ds(j * qk, qk)] for j in (0, 1)])
    gather_qr.a0[0].start()
    gather_qr.b1[0].start()
    round_qr(1)
    gather_qr.a0[1].start()
    gather_qr.b1[1].start()
    with jax.named_scope("s004"):
        gather_qr.later()
    with jax.named_scope("s005"):
        gather_qr.to_partner()
    gather_ql = Gather4(lambda s, h: ql_row.at[s, h], lambda h: ql_row.at[col, h], lambda n: ql_row.at[pl.ds(0, n)], snd_small, new("recv"))
    with jax.named_scope("s006"):
        load_ql.wait()
    ql_row[col] = ql_f[...].astype(BF16).reshape(2, hr, lb)
    with jax.named_scope("s007"):
        gather_ql.start()
    loaded(grow.at[pl.ds(0, 2)], sem_g)
    gather_g = Gather4(lambda s, h: grow.at[2 * s + h], lambda h: grow.at[2 * col + h],
                       lambda n: grow.at[pl.ds(0, 2 * n)], snd_g)
    with jax.named_scope("s008"):
        gather_g.start()

    local(m_ref, mbuf, sem_mid)
    local(v_ref, vbuf, sem_mid)
    local(w_ref, wbuf, sem_mid)
    with jax.named_scope("s009"):
        for h in (0, 1):
            local(g_ref.at[:, pl.ds(h * kb, kb)], gy.at[row, h], sem_mid)
            local(r_ref.at[:, pl.ds(h * kb, kb)], or_ref.at[h], sem_r)
    load_l = local(l_ref, ol_ref)

    def cast_block(s):
        growb[s] = grow[s].astype(BF16)

    with jax.named_scope("s010"):
        for h in (0, 1):
            cast_block(2 * col + h)

    lft_c, rgt_c, far_c = wrap(col - 1, ny), wrap(col + 1, ny), wrap(col + 2, ny)
    x_lft, x_rgt, x_far = wrap(x - 1, nx), wrap(x + 1, nx), wrap(x + 2, nx)
    half_l = lb // 2
    quarter = pl.ds(pl.multiple_of(col * qb, qb), qb)
    row_far = wrap(row + 4, nrow)
    prow_far = row_far + 1 - 2 * core
    with jax.named_scope("s011"):
        gather_ql.forward()
    with jax.named_scope("s012"):
        gather_g.forward()
    with jax.named_scope("s013"):
        gather_qr.forward()
    with jax.named_scope("s014"):
        gather_ql.rest()

    with jax.named_scope("s015"):
        for k in range(ny):
            block = ql_row[k].reshape(rb, lb)
            for h in (0, 1):
                ql_send[2 * k + h] = block[:, h * half_l:(h + 1) * half_l]
    ql_col[row, col] = ql_send[row, quarter]
    rcv_ql = new("recv")
    for r, _, _ in peers():
        remote(ql_send.at[r, quarter], ql_col.at[row, col], {"row": r}, snd_ql, rcv_ql).start()

    cast_block(2 * lft_c)
    cast_block(2 * rgt_c + 1)
    with jax.named_scope("s016"):
        gather_g.second()
    cast_block(2 * lft_c + 1)
    cast_block(2 * rgt_c)
    with jax.named_scope("s017"):
        gather_g.third()

    eb = qb // 2
    gx[row, col] = grow[row, quarter]
    rcv_gx, rest_gx = [new("recv") for _ in (0, 1)], new("recv")

    def send_gx(w):
        here = pl.ds(pl.multiple_of(col * qb + w * eb, eb), eb)
        for r, _, _ in peers():
            remote(grow.at[r, here], gx.at[row, col, pl.ds(w * eb, eb)], {"row": r}, snd_gx, rcv_gx[w]).start()

    def gather_wave(w):
        there, half = pl.ds(w * eb, eb), nrow // 2
        arrived(gx.at[pl.ds(0, nrow - 1), 0, pl.ds(0, eb)], rcv_gx[w])
        g = Gather4(lambda s, h: gx.at[pl.ds(h * half, half), s, there],
                    lambda h: gx.at[pl.ds(h * half, half), col, there],
                    lambda n: gx.at[:, pl.ds(0, n), there], snd_g, rest_gx)
        g.start()
        return g

    send_gx(0)

    def rows_of(w):
        return pl.ds(0, rb // 4) if w == 0 else pl.ds(rb // 4, rb - rb // 4)

    share_y = [new("recv") for _ in range(3)]

    gather_y = [Gather8(lambda s, h, w=w: gy.at[s, h, rows_of(w)], lambda h, w=w: grow.at[2 * col + h, rows_of(w)],
                        lambda n, w=w: gy.at[pl.ds(0, n), :, rows_of(w)], snd_rows, share=share_y) for w in (0, 1)]
    with jax.named_scope("s018"):
        for g in gather_y:
            g.to_partner()
    cast_block(2 * far_c)
    cast_block(2 * far_c + 1)

    def turn(k):
        for j in range(4):
            qr_t[k, j] = qr_b[2 * k + j // 2, j % 2].T

    def h_part(r):
        return dot(growb[r], qr_b[r].reshape(kb, cb), NN)

    with jax.named_scope("s019"):
        gather_qr.own_ready()
    acc[...] = h_part(2 * x) + h_part(2 * x + 1)
    with jax.named_scope("s020"):
        gather_qr.second()
    with jax.named_scope("s021"):
        gather_qr.near_ready()
    acc[...] += h_part(2 * x_lft) + h_part(2 * x_lft + 1)
    acc[...] += h_part(2 * x_rgt) + h_part(2 * x_rgt + 1)
    turn(x)
    turn(x_lft)
    turn(x_rgt)
    with jax.named_scope("s022"):
        gather_qr.third()
    acc[...] += h_part(row_far)
    with jax.named_scope("s023"):
        gather_qr.far_ready()
    with jax.named_scope("s024"):
        hb[row] = (acc[...] + h_part(prow_far)).astype(BF16).reshape(2, hr, cb)

    def halves(ref):
        return [ref.at[pl.ds(j * hr // 2, hr // 2)] for j in (0, 1)]

    gather_h = Gather8(lambda s, h: hb.at[s, h], lambda h: hb.at[row, h], lambda n: hb.at[pl.ds(0, n)], snd_rows, halves)
    with jax.named_scope("s025"):
        gather_h.start()

    arrived(ql_col.at[pl.ds(0, nrow - 1), 0], rcv_ql)
    gather_qc = Gather4(
        lambda s, h: ql_col.at[pl.ds(h * (nrow // 2), nrow // 2), s],
        lambda h: ql_col.at[pl.ds(h * (nrow // 2), nrow // 2), col],
        lambda n: ql_col.at[:, pl.ds(0, n)], snd_small, new("recv"))
    with jax.named_scope("s026"):
        gather_qc.start()
    with jax.named_scope("s027"):
        gather_qc.forward()
    gather_gx0 = gather_wave(0)

    def g_part(r):
        return dot(ql_col[r].reshape(rb, rb), hb[r].reshape(rb, cb), TN)

    def g_pair(cx):
        left = ql_col[pl.ds(2 * cx, 2)].reshape(2 * rb, rb)
        return dot(left, hb[pl.ds(2 * cx, 2)].reshape(2 * rb, cb), TN)

    with jax.named_scope("s028"):
        gather_h.forward()
    send_gx(1)
    gather_y[0].early()
    turn(x_far)
    with jax.named_scope("s029"):
        gather_qc.rest()
    with jax.named_scope("s030"):
        gather_h.own_ready()
    gacc[...] = g_pair(x)
    with jax.named_scope("s031"):
        gather_h.second()
    with jax.named_scope("s032"):
        gather_gx0.forward()
    with jax.named_scope("s033"):
        gather_h.near_ready()
    gacc[...] += g_pair(x_lft)
    gacc[...] += g_pair(x_rgt)
    with jax.named_scope("s034"):
        gather_h.third()
    gacc[...] += g_part(row_far)
    with jax.named_scope("s035"):
        gather_h.far_ready()
    rotated = gacc[...] + g_part(prow_far)

    loaded(gy.at[pl.ds(0, 4)], sem_mid)
    gacc[...] = rotated
    gather_n = Gather8(lambda s, h: nb.at[s, h], lambda h: nb.at[row, h], lambda n: nb.at[pl.ds(0, n)], snd_rows,
                       halves, halves)
    with jax.named_scope("s036"):
        for j in (0, 1):
            for h in (0, 1):
                part = pl.ds(h * hr + j * (hr // 2), hr // 2)
                turned = gacc[part]
                new_first = BETA1 * mbuf[part] + (1.0 - BETA1) * turned
                new_second = BETA2 * vbuf[part] + (1.0 - BETA2) * turned * turned
                below = BIAS_ONE * jnp.sqrt(new_second * (1.0 / BIAS_TWO)) + BIAS_ONE * EPS
                nb[row, h, pl.ds(j * (hr // 2), hr // 2)] = (new_first / below).astype(BF16)
                om_ref[part] = new_first
                ov_ref[part] = new_second
            gather_n.a0[j].start()
            gather_n.b1[j].start()
    with jax.named_scope("s037"):
        gather_n.later()
    with jax.named_scope("s038"):
        gather_n.to_partner()
    gather_gx1 = gather_wave(1)

    def k_part(r):
        return dot(ql_send[r], nb[r].reshape(rb, cb), NN)

    def k_pair(cx):
        return dot(ql_row[cx].reshape(rb, lb), nb[pl.ds(2 * cx, 2)].reshape(2 * rb, cb), NN)

    with jax.named_scope("s039"):
        gather_n.own_ready()
    acc[...] = k_pair(x)
    with jax.named_scope("s040"):
        gather_n.forward()
    gather_y[0].later()
    gather_y[1].early()
    gather_y[1].later()
    with jax.named_scope("s041"):
        gather_gx1.forward()
    with jax.named_scope("s042"):
        gather_n.second()
    with jax.named_scope("s043"):
        gather_n.near_ready()
    acc[...] += k_pair(x_lft)
    acc[...] += k_pair(x_rgt)
    with jax.named_scope("s044"):
        gather_n.third()
    acc[...] += k_part(row_far)
    with jax.named_scope("s045"):
        gather_n.far_ready()
    with jax.named_scope("s046"):
        back = (acc[...] + k_part(prow_far)).astype(BF16)

    rcv_u, rcv_f = new("recv"), [new("recv"), new("recv")]

    def half(k, h):
        return up.at[k, pl.ds(2 * h, 2)]

    u_far = [remote(half(far_c, 0), rin.at[0], y_plus, snd_u, rcv_f[0]),
             remote(half(far_c, 1), rin.at[1], y_minus, snd_u, rcv_f[1])]
    u_half = [remote(half(rgt_c, 1), rin.at[2], y_plus, snd_u, rcv_u),
              remote(half(lft_c, 0), rin.at[3], y_minus, snd_u, rcv_u)]
    u_sum = [remote(half(rgt_c, 0), rin.at[4], y_plus, snd_u, rcv_u),
             remote(half(lft_c, 1), rin.at[5], y_minus, snd_u, rcv_u)]

    def make_u(k):
        for j in range(4):
            up[k, j] = dot(back, qr_t[k, j], NN)

    with jax.named_scope("s047"):
        make_u(far_c)
    with jax.named_scope("s048"):
        for c in u_far:
            c.start()
    with jax.named_scope("s049"):
        make_u(rgt_c)
    u_half[0].start()
    with jax.named_scope("s050"):
        make_u(lft_c)
    u_half[1].start()
    gather_y[0].forward()
    with jax.named_scope("s051"):
        make_u(col)

    arrived(gx.at[:, pl.ds(0, 2)], rest_gx)
    right_g = gx[pl.ds(2 * col, 2)].reshape(2 * rb, kb)
    with jax.named_scope("s052"):
        lp[...] = dot(gx[...].reshape(nrow * rb, kb), right_g, NT, HIGHEST).reshape(nrow, rb, lb)
    rcv_s = new("recv")
    with jax.named_scope("s053"):
        for k in range(nx):
            remote(lp.at[2 * k + 1 - core], lrecv.at[k], partner, snd_small, rcv_s).start()

    def add_r(cx, first=False):
        left = gx[pl.ds(2 * cx, 2)].reshape(2 * rb, kb)

        def body(h, _):
            part = dot(left, gy[pl.ds(2 * cx, 2), h].reshape(2 * rb, kb), TN, HIGHEST)
            old = or_ref[h]
            if first:
                old = BETA2 * old
            or_ref[h] = old + (1.0 - BETA2) * part
            return 0

        lax.fori_loop(0, 2, body, 0)

    def add_r_block(r):
        left = gx[r].reshape(rb, kb)

        def body(h, _):
            or_ref[h] += (1.0 - BETA2) * dot(left, gy[r, h], TN, HIGHEST)
            return 0

        lax.fori_loop(0, 2, body, 0)

    gather_y[0].second()
    gather_y[1].forward()
    loaded(or_ref, sem_r)
    arrived(gy.at[pl.ds(0, 1)], share_y[0])
    with jax.named_scope("s054"):
        add_r(x, True)

    arrived(rin.at[0], rcv_f[0])
    up[rgt_c, :2] = up[rgt_c, :2] + rin[0]
    u_sum[0].start()
    arrived(rin.at[1], rcv_f[1])
    up[lft_c, 2:] = up[lft_c, 2:] + rin[1]
    u_sum[1].start()

    arrived(lrecv, rcv_s)
    with jax.named_scope("s055"):
        for k in range(nx):
            lp[2 * k + core] = lp[2 * k + core] + lrecv[k]
    rcv_l = new("recv")
    with jax.named_scope("s056"):
        for dx in (1, nx - 1, 2):
            to = 2 * wrap(x + dx, nx) + core
            remote(lp.at[to], lx.at[x], {"row": to}, snd_small, rcv_l).start()

    gather_y[1].second()
    arrived(gy.at[pl.ds(0, 2)], share_y[1])
    with jax.named_scope("s057"):
        add_r(x_lft)
    gather_y[0].third()
    with jax.named_scope("s058"):
        add_r(x_rgt)
    gather_y[1].third()
    with jax.named_scope("s059"):
        add_r_block(row_far)
    arrived(gy.at[pl.ds(0, 1)], share_y[2])
    with jax.named_scope("s060"):
        add_r_block(prow_far)

    with jax.named_scope("s061"):
        load_l.wait()
    arrived(lx.at[pl.ds(0, nx - 1)], rcv_l)
    total = lp[row]
    with jax.named_scope("s062"):
        for dx in (1, 2, 3):
            total = total + lx[wrap(x + dx, nx)]
    ol_ref[...] = BETA2 * ol_ref[...] + (1.0 - BETA2) * total

    arrived(rin.at[pl.ds(0, 4)], rcv_u)
    with jax.named_scope("s063"):
        for j in range(4):
            cols = pl.ds(j * (cb // 4), cb // 4)
            others_sum = (rin[3, j] + rin[4, j]) if j < 2 else (rin[2, j - 2] + rin[5, j - 2])
            ow_ref[:, cols] = wbuf[:, cols] - LR * (up[col, j] + others_sum)

    assert tuple(counts.values()) == COUNTS
    with jax.named_scope("s064"):
        for c in pending:
            c.wait_send()


def write_out(w_ref, m_ref, v_ref, l_ref, r_ref, ow_ref, om_ref, ov_ref, ol_ref, or_ref, sem):
    kb = r_ref.shape[1]
    moves = [(w_ref, ow_ref), (m_ref, om_ref), (v_ref, ov_ref), (l_ref, ol_ref)]
    moves += [(r_ref.at[h], or_ref.at[:, pl.ds(h * kb, kb)]) for h in (0, 1)]
    copies = [pltpu.make_async_copy(a, b, sem.at[i]) for i, (a, b) in enumerate(moves)]
    for c in copies:
        c.start()
    for c in copies:
        c.wait()


def solution(mesh):
    nx, ny = mesh.shape["row"] // 2, mesh.shape["col"]
    tile_spec = P(("layer", "row"), "col")

    def local_step(*args):
        rb, cb = args[0].shape
        kb = args[7].shape[0]
        lb = args[6].shape[1]
        hr, nr = rb // 2, 2 * nx
        vm = pltpu.VMEM
        shapes = [args[0], args[2], args[3], args[4], args[5]]
        held = pl.pallas_call(
            functools.partial(kernel, nx, ny),
            out_shape=tuple(vm(s, F32) for s in [(rb, cb)] * 3 + [(rb, lb), (2, kb, kb)]),
            in_specs=[pl.BlockSpec(memory_space=pl.ANY)] * 8,
            out_specs=tuple([pl.BlockSpec(memory_space=pltpu.VMEM)] * 5),
            scratch_shapes=[
                vm((2, kb // 2, cb), F32),
                vm((nr, 2, kb // 2, cb), BF16),
                vm((nx, 4, cb, kb // 2), BF16),
                vm((nr, rb, kb), F32),
                vm((nr, rb, kb), BF16),
                vm((rb, lb), F32),
                vm((ny, 2, hr, lb), BF16),
                vm((nr, rb, lb // 2), BF16),
                vm((nr, ny, rb // ny, lb // 2), BF16),
                vm((nr, ny, rb // ny, kb), F32),
                vm((nr, 2, rb, kb), F32),
                vm((nr, 2, hr, cb), BF16),
                vm((nr, 2, hr, cb), BF16),
                vm((rb, cb), F32),
                vm((rb, cb), F32),
                vm((ny, 4, rb, cb // 4), F32),
                vm((6, 2, rb, cb // 4), F32),
                vm((nr, rb, lb), F32),
                vm((nx, rb, lb), F32),
                vm((nx, rb, lb), F32),
                vm((rb, cb), F32),
                vm((rb, cb), F32),
                vm((rb, cb), F32),
                *[pltpu.SemaphoreType.DMA((n,)) for n in COUNTS],
            ],
            compiler_params=pltpu.CompilerParams(
                collective_id=0, has_side_effects=True, vmem_limit_bytes=61600 * 1024),
        )(*args)
        return pl.pallas_call(
            write_out,
            out_shape=tuple(jax.ShapeDtypeStruct(s.shape, s.dtype) for s in shapes),
            in_specs=[pl.BlockSpec(memory_space=pltpu.VMEM)] * 5,
            out_specs=tuple([pl.BlockSpec(memory_space=pl.ANY)] * 5),
            scratch_shapes=[pltpu.SemaphoreType.DMA((6,))],
            compiler_params=pltpu.CompilerParams(vmem_limit_bytes=4 * 1024 * 1024),
        )(*held)

    return jax.shard_map(local_step, mesh=mesh, in_specs=(tile_spec,) * 8, out_specs=(tile_spec,) * 5, check_vma=False)
```

```python
import functools

import jax
import jax.numpy as jnp
from jax import lax
from jax.experimental import pallas as pl
from jax.experimental.pallas import tpu as pltpu
from jax.sharding import PartitionSpec as P

BETA1 = 0.9
BETA2 = 0.9
EPS = 1e-8
LR = 0.1
STEP = 10
BIAS_ONE = 1.0 - BETA1 ** STEP
BIAS_TWO = 1.0 - BETA2 ** STEP
MESH = pl.DeviceIdType.MESH
HIGHEST = lax.Precision.HIGHEST
F32 = jnp.float32
BF16 = jnp.bfloat16
NN = (((1,), (0,)), ((), ()))
TN = (((0,), (0,)), ((), ()))
NT = (((1,), (1,)), ((), ()))
COUNTS = (7, 55, 7)


def dot(a, b, dims, precision=None):
    return lax.dot_general(a, b, dims, precision=precision, preferred_element_type=F32)


def kernel(nx, ny, w_ref, g_ref, m_ref, v_ref, l_ref, r_ref, ql_ref, qr_ref,
           ow_ref, om_ref, ov_ref, ol_ref, or_ref,
           qr_f, qr_b, qr_t, grow, growb, ql_f, ql_row, ql_send, ql_col, gx, gy, hb, nb,
           acc, gacc, up, rin, lp, lrecv, lx, wbuf, mbuf, vbuf,
           send_sem, recv_sem, local_sem):
    row = lax.axis_index("row")
    col = lax.axis_index("col")
    core = lax.rem(row, 2)
    x = lax.div(row, 2)
    nrow = 2 * nx
    rb, cb = w_ref.shape
    kb = qr_ref.shape[0]
    lb = ql_ref.shape[1]
    hr = rb // 2
    qb = rb // ny

    def wrap(v, n):
        return lax.rem(v + n, n)

    x_plus = {"row": wrap(row + 2, nrow)}
    x_minus = {"row": wrap(row - 2, nrow)}
    partner = {"row": row + 1 - 2 * core}
    y_plus = {"col": wrap(col + 1, ny)}
    y_minus = {"col": wrap(col - 1, ny)}
    prow = row + 1 - 2 * core
    counts = {"send": 0, "recv": 0, "local": 0}
    pending = []

    def new(kind):
        counts[kind] += 1
        return counts[kind] - 1

    def remote(src, dst, device, send, recv=None):
        recv = new("recv") if recv is None else recv
        return pltpu.make_async_remote_copy(
            src_ref=src, dst_ref=dst, send_sem=send_sem.at[send], recv_sem=recv_sem.at[recv],
            device_id=device, device_id_type=MESH)

    def sends(span):
        i = new("send")
        pending.append(remote(span, span, partner, i, 0))
        return i

    snd_qr, snd_rows = sends(qr_b.at[pl.ds(0, nrow - 1)]), sends(qr_b.at[pl.ds(0, nrow - 1)])
    snd_g, snd_small = sends(qr_b.at[pl.ds(0, 3)]), sends(gx.at[pl.ds(0, 5)])
    snd_ql, snd_gx = sends(ql_col.at[pl.ds(0, nrow - 1), 0]), sends(gx.at[pl.ds(0, nrow - 1), 0])
    snd_u = sends(rin)

    def arrived(span, recv):
        remote(span, span, partner, 0, recv).wait_recv()

    def local(src, dst, sem=None):
        copy = pltpu.make_async_copy(src, dst, local_sem.at[new("local") if sem is None else sem])
        copy.start()
        return copy

    class Gather8:
        def __init__(self, at, own, span, snd, cut=lambda ref: [ref], first=lambda ref: [ref], share=None):
            lft, rgt, far = wrap(row - 2, nrow), wrap(row + 2, nrow), wrap(row + 4, nrow)
            self.span = span
            self.at, self.lft, self.rgt = at, lft, rgt
            self.second_sem, self.a0_sem, self.b1_sem = (new("recv") for _ in range(3))
            self.own_sem, self.near_sem, self.far_sem = share or [new("recv") for _ in range(3)]
            self.a0 = [remote(c, d, x_plus, snd, self.a0_sem) for c, d in zip(first(own(0)), first(at(row, 0)))]
            self.b1 = [remote(c, d, x_minus, snd, self.b1_sem) for c, d in zip(first(own(1)), first(at(row, 1)))]
            self.a1 = remote(own(1), at(row, 1), x_plus, snd, self.second_sem)
            self.b0 = remote(own(0), at(row, 0), x_minus, snd, self.second_sem)
            self.p = [remote(own(h), at(row, h), partner, snd, self.own_sem) for h in (0, 1)]
            self.f_sem = [new("recv") for _ in cut(at(lft, 0))]
            self.f0 = [remote(c, c, x_plus, snd, i) for c, i in zip(cut(at(lft, 0)), self.f_sem)]
            self.f1 = [remote(c, c, x_minus, snd, i) for c, i in zip(cut(at(rgt, 1)), self.f_sem)]
            self.part = cut(at(far, 0))
            if len(self.part) > 1:
                self.two = at(far, 0).at[pl.ds(0, 2 * self.part[0].shape[0])]
            self.near = [remote(at(s, h), at(s, h), partner, snd, self.near_sem)
                         for s, h in ((lft, 0), (rgt, 1), (lft, 1), (rgt, 0))]
            self.last = [[remote(c, c, partner, snd, self.far_sem) for c in cut(at(far, h))] for h in (0, 1)]

        def early(self):
            for c in (*self.a0, *self.b1):
                c.start()

        def later(self):
            self.a1.start()
            self.b0.start()

        def to_partner(self):
            for c in self.p:
                c.start()

        def start(self):
            self.early()
            self.later()
            self.to_partner()

        def forward(self):
            arrived(self.at(self.lft, 0), self.a0_sem)
            for c in self.f0:
                c.start()
            self.near[0].start()
            arrived(self.at(self.rgt, 1), self.b1_sem)
            for c in self.f1:
                c.start()
            self.near[1].start()

        def second(self):
            arrived(self.span(1), self.second_sem)
            self.near[2].start()
            self.near[3].start()

        def third(self):
            for i, (c, d) in enumerate(zip(*self.last)):
                both = self.f_span(i)
                arrived(both, self.f_sem[i])
                c.start()
                d.start()

        def f_span(self, i):
            return self.span(1) if len(self.part) == 1 else self.two

        def own_ready(self):
            arrived(self.span(1), self.own_sem)

        def near_ready(self):
            arrived(self.span(2), self.near_sem)

        def far_ready(self):
            arrived(self.span(1), self.far_sem)

    class Gather4:
        def __init__(self, at, own, span, snd, share=None):
            lft, rgt = wrap(col - 1, ny), wrap(col + 1, ny)
            self.span = span
            first = new("recv")
            self.first_sem = first
            self.second_sem, self.third_sem = (new("recv"), new("recv")) if share is None else (share, share)
            self.a0 = remote(own(0), at(col, 0), y_plus, snd, first)
            self.b1 = remote(own(1), at(col, 1), y_minus, snd, first)
            self.a1 = remote(own(1), at(col, 1), y_plus, snd, self.second_sem)
            self.b0 = remote(own(0), at(col, 0), y_minus, snd, self.second_sem)
            self.f0 = remote(at(lft, 0), at(lft, 0), y_plus, snd, self.third_sem)
            self.f1 = remote(at(rgt, 1), at(rgt, 1), y_minus, snd, self.third_sem)

        def start(self):
            for c in (self.a0, self.b1, self.a1, self.b0):
                c.start()

        def forward(self):
            arrived(self.span(1), self.first_sem)
            self.f0.start()
            self.f1.start()

        def second(self):
            arrived(self.span(1), self.second_sem)

        def third(self):
            arrived(self.span(1), self.third_sem)

        def rest(self):
            arrived(self.span(2), self.second_sem)

    def peers():
        for dx in (1, nx - 1, 2, 0):
            for dc in (0, 1):
                if dx == 0 and dc == 0:
                    continue
                px = wrap(x + dx, nx)
                pc = core if dc == 0 else 1 - core
                yield 2 * px + pc, px, pc

    hk, qk = kb // 2, kb // 4
    sem_qr, sem_g, sem_mid, sem_r = [new("local"), new("local")], new("local"), new("local"), new("local")
    for i, (h, j) in enumerate(((0, 0), (1, 0), (0, 1), (1, 1))):
        local(qr_ref.at[pl.ds(h * hk + j * qk, qk)], qr_f.at[h, pl.ds(j * qk, qk)], sem_qr[i // 2])

    barrier = pltpu.get_barrier_semaphore()
    others = [r for r, _, _ in peers()]
    for r in others:
        pl.semaphore_signal(barrier, inc=1, device_id={"row": r}, device_id_type=MESH)
    for d in (y_plus, y_minus):
        pl.semaphore_signal(barrier, inc=1, device_id=d, device_id_type=MESH)

    load_ql = local(ql_ref, ql_f)
    for h in (0, 1):
        local(g_ref.at[:, pl.ds(h * kb, kb)], grow.at[2 * col + h], sem_g)

    def loaded(ref, sem):
        pltpu.make_async_remote_copy(
            src_ref=ref, dst_ref=ref, send_sem=send_sem.at[0], recv_sem=local_sem.at[sem],
            device_id=partner, device_id_type=MESH).wait_recv()

    def round_qr(j):
        loaded(qr_f.at[0], sem_qr[j])
        for h in (0, 1):
            qr_b[row, h, pl.ds(j * qk, qk)] = qr_f[h, pl.ds(j * qk, qk)].astype(BF16)

    round_qr(0)
    pl.semaphore_wait(barrier, len(others) + 2)

    gather_qr = Gather8(lambda s, h: qr_b.at[s, h], lambda h: qr_b.at[row, h], lambda n: qr_b.at[pl.ds(0, n)], snd_qr,
                        lambda ref: [ref.at[pl.ds(j * kb // 8, kb // 8)] for j in range(4)],
                        lambda ref: [ref.at[pl.ds(j * qk, qk)] for j in (0, 1)])
    gather_qr.a0[0].start()
    gather_qr.b1[0].start()
    round_qr(1)
    gather_qr.a0[1].start()
    gather_qr.b1[1].start()
    gather_qr.later()
    gather_qr.to_partner()
    gather_ql = Gather4(lambda s, h: ql_row.at[s, h], lambda h: ql_row.at[col, h], lambda n: ql_row.at[pl.ds(0, n)], snd_small, new("recv"))
    load_ql.wait()
    ql_row[col] = ql_f[...].astype(BF16).reshape(2, hr, lb)
    gather_ql.start()
    loaded(grow.at[pl.ds(0, 2)], sem_g)
    gather_g = Gather4(lambda s, h: grow.at[2 * s + h], lambda h: grow.at[2 * col + h],
                       lambda n: grow.at[pl.ds(0, 2 * n)], snd_g)
    gather_g.start()

    local(m_ref, mbuf, sem_mid)
    local(v_ref, vbuf, sem_mid)
    local(w_ref, wbuf, sem_mid)
    for h in (0, 1):
        local(g_ref.at[:, pl.ds(h * kb, kb)], gy.at[row, h], sem_mid)
        local(r_ref.at[:, pl.ds(h * kb, kb)], or_ref.at[h], sem_r)
    load_l = local(l_ref, ol_ref)

    def cast_block(s):
        growb[s] = grow[s].astype(BF16)

    for h in (0, 1):
        cast_block(2 * col + h)

    lft_c, rgt_c, far_c = wrap(col - 1, ny), wrap(col + 1, ny), wrap(col + 2, ny)
    x_lft, x_rgt, x_far = wrap(x - 1, nx), wrap(x + 1, nx), wrap(x + 2, nx)
    half_l = lb // 2
    quarter = pl.ds(pl.multiple_of(col * qb, qb), qb)
    row_far = wrap(row + 4, nrow)
    prow_far = row_far + 1 - 2 * core
    gather_ql.forward()
    gather_g.forward()
    gather_qr.forward()
    gather_ql.rest()

    for k in range(ny):
        block = ql_row[k].reshape(rb, lb)
        for h in (0, 1):
            ql_send[2 * k + h] = block[:, h * half_l:(h + 1) * half_l]
    ql_col[row, col] = ql_send[row, quarter]
    rcv_ql = new("recv")
    for r, _, _ in peers():
        remote(ql_send.at[r, quarter], ql_col.at[row, col], {"row": r}, snd_ql, rcv_ql).start()

    cast_block(2 * lft_c)
    cast_block(2 * rgt_c + 1)
    gather_g.second()
    cast_block(2 * lft_c + 1)
    cast_block(2 * rgt_c)
    gather_g.third()

    eb = qb // 2
    gx[row, col] = grow[row, quarter]
    rcv_gx, rest_gx = [new("recv") for _ in (0, 1)], new("recv")

    def send_gx(w):
        here = pl.ds(pl.multiple_of(col * qb + w * eb, eb), eb)
        for r, _, _ in peers():
            remote(grow.at[r, here], gx.at[row, col, pl.ds(w * eb, eb)], {"row": r}, snd_gx, rcv_gx[w]).start()

    def gather_wave(w):
        there, half = pl.ds(w * eb, eb), nrow // 2
        arrived(gx.at[pl.ds(0, nrow - 1), 0, pl.ds(0, eb)], rcv_gx[w])
        g = Gather4(lambda s, h: gx.at[pl.ds(h * half, half), s, there],
                    lambda h: gx.at[pl.ds(h * half, half), col, there],
                    lambda n: gx.at[:, pl.ds(0, n), there], snd_g, rest_gx)
        g.start()
        return g

    send_gx(0)

    def rows_of(w):
        return pl.ds(0, rb // 4) if w == 0 else pl.ds(rb // 4, rb - rb // 4)

    share_y = [new("recv") for _ in range(3)]

    gather_y = [Gather8(lambda s, h, w=w: gy.at[s, h, rows_of(w)], lambda h, w=w: grow.at[2 * col + h, rows_of(w)],
                        lambda n, w=w: gy.at[pl.ds(0, n), :, rows_of(w)], snd_rows, share=share_y) for w in (0, 1)]
    for g in gather_y:
        g.to_partner()
    cast_block(2 * far_c)
    cast_block(2 * far_c + 1)

    def turn(k):
        for j in range(4):
            qr_t[k, j] = qr_b[2 * k + j // 2, j % 2].T

    def h_part(r):
        return dot(growb[r], qr_b[r].reshape(kb, cb), NN)

    gather_qr.own_ready()
    acc[...] = h_part(2 * x) + h_part(2 * x + 1)
    gather_qr.second()
    gather_qr.near_ready()
    acc[...] += h_part(2 * x_lft) + h_part(2 * x_lft + 1)
    acc[...] += h_part(2 * x_rgt) + h_part(2 * x_rgt + 1)
    turn(x)
    turn(x_lft)
    turn(x_rgt)
    gather_qr.third()
    acc[...] += h_part(row_far)
    gather_qr.far_ready()
    hb[row] = (acc[...] + h_part(prow_far)).astype(BF16).reshape(2, hr, cb)

    def halves(ref):
        return [ref.at[pl.ds(j * hr // 2, hr // 2)] for j in (0, 1)]

    gather_h = Gather8(lambda s, h: hb.at[s, h], lambda h: hb.at[row, h], lambda n: hb.at[pl.ds(0, n)], snd_rows, halves)
    gather_h.start()

    arrived(ql_col.at[pl.ds(0, nrow - 1), 0], rcv_ql)
    gather_qc = Gather4(
        lambda s, h: ql_col.at[pl.ds(h * (nrow // 2), nrow // 2), s],
        lambda h: ql_col.at[pl.ds(h * (nrow // 2), nrow // 2), col],
        lambda n: ql_col.at[:, pl.ds(0, n)], snd_small, new("recv"))
    gather_qc.start()
    gather_qc.forward()
    gather_gx0 = gather_wave(0)

    def g_part(r):
        return dot(ql_col[r].reshape(rb, rb), hb[r].reshape(rb, cb), TN)

    def g_pair(cx):
        left = ql_col[pl.ds(2 * cx, 2)].reshape(2 * rb, rb)
        return dot(left, hb[pl.ds(2 * cx, 2)].reshape(2 * rb, cb), TN)

    gather_h.forward()
    send_gx(1)
    gather_y[0].early()
    turn(x_far)
    gather_qc.rest()
    gather_h.own_ready()
    gacc[...] = g_pair(x)
    gather_h.second()
    gather_gx0.forward()
    gather_h.near_ready()
    gacc[...] += g_pair(x_lft)
    gacc[...] += g_pair(x_rgt)
    gather_h.third()
    gacc[...] += g_part(row_far)
    gather_h.far_ready()
    rotated = gacc[...] + g_part(prow_far)

    loaded(gy.at[pl.ds(0, 4)], sem_mid)
    gacc[...] = rotated
    gather_n = Gather8(lambda s, h: nb.at[s, h], lambda h: nb.at[row, h], lambda n: nb.at[pl.ds(0, n)], snd_rows,
                       halves, halves)
    for j in (0, 1):
        for h in (0, 1):
            part = pl.ds(h * hr + j * (hr // 2), hr // 2)
            turned = gacc[part]
            new_first = BETA1 * mbuf[part] + (1.0 - BETA1) * turned
            new_second = BETA2 * vbuf[part] + (1.0 - BETA2) * turned * turned
            below = BIAS_ONE * jnp.sqrt(new_second * (1.0 / BIAS_TWO)) + BIAS_ONE * EPS
            nb[row, h, pl.ds(j * (hr // 2), hr // 2)] = (new_first / below).astype(BF16)
            om_ref[part] = new_first
            ov_ref[part] = new_second
        gather_n.a0[j].start()
        gather_n.b1[j].start()
    gather_n.later()
    gather_n.to_partner()
    gather_gx1 = gather_wave(1)

    def k_part(r):
        return dot(ql_send[r], nb[r].reshape(rb, cb), NN)

    def k_pair(cx):
        return dot(ql_row[cx].reshape(rb, lb), nb[pl.ds(2 * cx, 2)].reshape(2 * rb, cb), NN)

    gather_n.own_ready()
    acc[...] = k_pair(x)
    gather_n.forward()
    gather_y[0].later()
    gather_y[1].early()
    gather_y[1].later()
    gather_gx1.forward()
    gather_n.second()
    gather_n.near_ready()
    acc[...] += k_pair(x_lft)
    acc[...] += k_pair(x_rgt)
    gather_n.third()
    acc[...] += k_part(row_far)
    gather_n.far_ready()
    back = (acc[...] + k_part(prow_far)).astype(BF16)

    rcv_u, rcv_f = new("recv"), [new("recv"), new("recv")]

    def half(k, h):
        return up.at[k, pl.ds(2 * h, 2)]

    u_far = [remote(half(far_c, 0), rin.at[0], y_plus, snd_u, rcv_f[0]),
             remote(half(far_c, 1), rin.at[1], y_minus, snd_u, rcv_f[1])]
    u_half = [remote(half(rgt_c, 1), rin.at[2], y_plus, snd_u, rcv_u),
              remote(half(lft_c, 0), rin.at[3], y_minus, snd_u, rcv_u)]
    u_sum = [remote(half(rgt_c, 0), rin.at[4], y_plus, snd_u, rcv_u),
             remote(half(lft_c, 1), rin.at[5], y_minus, snd_u, rcv_u)]

    def make_u(k):
        for j in range(4):
            up[k, j] = dot(back, qr_t[k, j], NN)

    make_u(far_c)
    for c in u_far:
        c.start()
    make_u(rgt_c)
    u_half[0].start()
    make_u(lft_c)
    u_half[1].start()
    gather_y[0].forward()
    make_u(col)

    arrived(gx.at[:, pl.ds(0, 2)], rest_gx)
    right_g = gx[pl.ds(2 * col, 2)].reshape(2 * rb, kb)
    lp[...] = dot(gx[...].reshape(nrow * rb, kb), right_g, NT, HIGHEST).reshape(nrow, rb, lb)
    rcv_s = new("recv")
    for k in range(nx):
        remote(lp.at[2 * k + 1 - core], lrecv.at[k], partner, snd_small, rcv_s).start()

    def add_r(cx, first=False):
        left = gx[pl.ds(2 * cx, 2)].reshape(2 * rb, kb)

        def body(h, _):
            part = dot(left, gy[pl.ds(2 * cx, 2), h].reshape(2 * rb, kb), TN, HIGHEST)
            old = or_ref[h]
            if first:
                old = BETA2 * old
            or_ref[h] = old + (1.0 - BETA2) * part
            return 0

        lax.fori_loop(0, 2, body, 0)

    gather_y[0].second()
    gather_y[1].forward()
    loaded(or_ref, sem_r)
    arrived(gy.at[pl.ds(0, 1)], share_y[0])
    add_r(x, True)

    arrived(rin.at[0], rcv_f[0])
    up[rgt_c, :2] = up[rgt_c, :2] + rin[0]
    u_sum[0].start()
    arrived(rin.at[1], rcv_f[1])
    up[lft_c, 2:] = up[lft_c, 2:] + rin[1]
    u_sum[1].start()

    arrived(lrecv, rcv_s)
    for k in range(nx):
        lp[2 * k + core] = lp[2 * k + core] + lrecv[k]
    rcv_l = new("recv")
    for dx in (1, nx - 1, 2):
        to = 2 * wrap(x + dx, nx) + core
        remote(lp.at[to], lx.at[x], {"row": to}, snd_small, rcv_l).start()

    gather_y[1].second()
    arrived(gy.at[pl.ds(0, 2)], share_y[1])
    add_r(x_lft)
    gather_y[0].third()
    add_r(x_rgt)
    gather_y[1].third()
    arrived(gy.at[pl.ds(0, 1)], share_y[2])
    add_r(x_far)

    load_l.wait()
    arrived(lx.at[pl.ds(0, nx - 1)], rcv_l)
    total = lp[row]
    for dx in (1, 2, 3):
        total = total + lx[wrap(x + dx, nx)]
    ol_ref[...] = BETA2 * ol_ref[...] + (1.0 - BETA2) * total

    arrived(rin.at[pl.ds(0, 4)], rcv_u)
    for j in range(4):
        cols = pl.ds(j * (cb // 4), cb // 4)
        others_sum = (rin[3, j] + rin[4, j]) if j < 2 else (rin[2, j - 2] + rin[5, j - 2])
        ow_ref[:, cols] = wbuf[:, cols] - LR * (up[col, j] + others_sum)

    assert tuple(counts.values()) == COUNTS
    for c in pending:
        c.wait_send()


def write_out(w_ref, m_ref, v_ref, l_ref, r_ref, ow_ref, om_ref, ov_ref, ol_ref, or_ref, sem):
    kb = r_ref.shape[1]
    moves = [(w_ref, ow_ref), (m_ref, om_ref), (v_ref, ov_ref), (l_ref, ol_ref)]
    moves += [(r_ref.at[h], or_ref.at[:, pl.ds(h * kb, kb)]) for h in (0, 1)]
    copies = [pltpu.make_async_copy(a, b, sem.at[i]) for i, (a, b) in enumerate(moves)]
    for c in copies:
        c.start()
    for c in copies:
        c.wait()


def solution(mesh):
    nx, ny = mesh.shape["row"] // 2, mesh.shape["col"]
    tile_spec = P(("layer", "row"), "col")

    def local_step(*args):
        rb, cb = args[0].shape
        kb = args[7].shape[0]
        lb = args[6].shape[1]
        hr, nr = rb // 2, 2 * nx
        vm = pltpu.VMEM
        shapes = [args[0], args[2], args[3], args[4], args[5]]
        held = pl.pallas_call(
            functools.partial(kernel, nx, ny),
            out_shape=tuple(vm(s, F32) for s in [(rb, cb)] * 3 + [(rb, lb), (2, kb, kb)]),
            in_specs=[pl.BlockSpec(memory_space=pl.ANY)] * 8,
            out_specs=tuple([pl.BlockSpec(memory_space=pltpu.VMEM)] * 5),
            scratch_shapes=[
                vm((2, kb // 2, cb), F32),
                vm((nr, 2, kb // 2, cb), BF16),
                vm((nx, 4, cb, kb // 2), BF16),
                vm((nr, rb, kb), F32),
                vm((nr, rb, kb), BF16),
                vm((rb, lb), F32),
                vm((ny, 2, hr, lb), BF16),
                vm((nr, rb, lb // 2), BF16),
                vm((nr, ny, rb // ny, lb // 2), BF16),
                vm((nr, ny, rb // ny, kb), F32),
                vm((nr, 2, rb, kb), F32),
                vm((nr, 2, hr, cb), BF16),
                vm((nr, 2, hr, cb), BF16),
                vm((rb, cb), F32),
                vm((rb, cb), F32),
                vm((ny, 4, rb, cb // 4), F32),
                vm((6, 2, rb, cb // 4), F32),
                vm((nr, rb, lb), F32),
                vm((nx, rb, lb), F32),
                vm((nx, rb, lb), F32),
                vm((rb, cb), F32),
                vm((rb, cb), F32),
                vm((rb, cb), F32),
                *[pltpu.SemaphoreType.DMA((n,)) for n in COUNTS],
            ],
            compiler_params=pltpu.CompilerParams(
                collective_id=0, has_side_effects=True, vmem_limit_bytes=61600 * 1024),
        )(*args)
        return pl.pallas_call(
            write_out,
            out_shape=tuple(jax.ShapeDtypeStruct(s.shape, s.dtype) for s in shapes),
            in_specs=[pl.BlockSpec(memory_space=pltpu.VMEM)] * 5,
            out_specs=tuple([pl.BlockSpec(memory_space=pl.ANY)] * 5),
            scratch_shapes=[pltpu.SemaphoreType.DMA((6,))],
            compiler_params=pltpu.CompilerParams(vmem_limit_bytes=4 * 1024 * 1024),
        )(*held)

    return jax.shard_map(local_step, mesh=mesh, in_specs=(tile_spec,) * 8, out_specs=(tile_spec,) * 5, check_vma=False)
```

```python
import functools

import jax
import jax.numpy as jnp
from jax import lax
from jax.experimental import pallas as pl
from jax.experimental.pallas import tpu as pltpu
from jax.sharding import PartitionSpec as P

BETA1 = 0.9
BETA2 = 0.9
EPS = 1e-8
LR = 0.1
STEP = 10
BIAS_ONE = 1.0 - BETA1 ** STEP
BIAS_TWO = 1.0 - BETA2 ** STEP
MESH = pl.DeviceIdType.MESH
HIGHEST = lax.Precision.HIGHEST
F32 = jnp.float32
BF16 = jnp.bfloat16
NN = (((1,), (0,)), ((), ()))
TN = (((0,), (0,)), ((), ()))
NT = (((1,), (1,)), ((), ()))
COUNTS = (7, 55, 7)


def dot(a, b, dims, precision=None):
    return lax.dot_general(a, b, dims, precision=precision, preferred_element_type=F32)


def kernel(nx, ny, w_ref, g_ref, m_ref, v_ref, l_ref, r_ref, ql_ref, qr_ref,
           ow_ref, om_ref, ov_ref, ol_ref, or_ref,
           qr_f, qr_b, qr_t, grow, growb, ql_f, ql_row, ql_send, ql_col, gx, gy, hb, nb,
           acc, gacc, up, rin, lp, lrecv, lx, wbuf, mbuf, vbuf,
           send_sem, recv_sem, local_sem):
    row = lax.axis_index("row")
    col = lax.axis_index("col")
    core = lax.rem(row, 2)
    x = lax.div(row, 2)
    nrow = 2 * nx
    rb, cb = w_ref.shape
    kb = qr_ref.shape[0]
    lb = ql_ref.shape[1]
    hr = rb // 2
    qb = rb // ny

    def wrap(v, n):
        return lax.rem(v + n, n)

    x_plus = {"row": wrap(row + 2, nrow)}
    x_minus = {"row": wrap(row - 2, nrow)}
    partner = {"row": row + 1 - 2 * core}
    y_plus = {"col": wrap(col + 1, ny)}
    y_minus = {"col": wrap(col - 1, ny)}
    prow = row + 1 - 2 * core
    counts = {"send": 0, "recv": 0, "local": 0}
    pending = []

    def new(kind):
        counts[kind] += 1
        return counts[kind] - 1

    def remote(src, dst, device, send, recv=None):
        recv = new("recv") if recv is None else recv
        return pltpu.make_async_remote_copy(
            src_ref=src, dst_ref=dst, send_sem=send_sem.at[send], recv_sem=recv_sem.at[recv],
            device_id=device, device_id_type=MESH)

    def sends(span):
        i = new("send")
        pending.append(remote(span, span, partner, i, 0))
        return i

    snd_qr, snd_rows = sends(qr_b.at[pl.ds(0, nrow - 1)]), sends(qr_b.at[pl.ds(0, nrow - 1)])
    snd_g, snd_small = sends(qr_b.at[pl.ds(0, 3)]), sends(gx.at[pl.ds(0, 5)])
    snd_ql, snd_gx = sends(ql_col.at[pl.ds(0, nrow - 1), 0]), sends(gx.at[pl.ds(0, nrow - 1), 0])
    snd_u = sends(rin)

    def arrived(span, recv):
        remote(span, span, partner, 0, recv).wait_recv()

    def local(src, dst, sem=None):
        copy = pltpu.make_async_copy(src, dst, local_sem.at[new("local") if sem is None else sem])
        copy.start()
        return copy

    class Gather8:
        def __init__(self, at, own, span, snd, cut=lambda ref: [ref], first=lambda ref: [ref], share=None):
            lft, rgt, far = wrap(row - 2, nrow), wrap(row + 2, nrow), wrap(row + 4, nrow)
            self.span = span
            self.at, self.lft, self.rgt = at, lft, rgt
            self.second_sem, self.a0_sem, self.b1_sem = (new("recv") for _ in range(3))
            self.own_sem, self.near_sem, self.far_sem = share or [new("recv") for _ in range(3)]
            self.a0 = [remote(c, d, x_plus, snd, self.a0_sem) for c, d in zip(first(own(0)), first(at(row, 0)))]
            self.b1 = [remote(c, d, x_minus, snd, self.b1_sem) for c, d in zip(first(own(1)), first(at(row, 1)))]
            self.a1 = remote(own(1), at(row, 1), x_plus, snd, self.second_sem)
            self.b0 = remote(own(0), at(row, 0), x_minus, snd, self.second_sem)
            self.p = [remote(own(h), at(row, h), partner, snd, self.own_sem) for h in (0, 1)]
            self.f_sem = [new("recv") for _ in cut(at(lft, 0))]
            self.f0 = [remote(c, c, x_plus, snd, i) for c, i in zip(cut(at(lft, 0)), self.f_sem)]
            self.f1 = [remote(c, c, x_minus, snd, i) for c, i in zip(cut(at(rgt, 1)), self.f_sem)]
            self.part = cut(at(far, 0))
            if len(self.part) > 1:
                self.two = at(far, 0).at[pl.ds(0, 2 * self.part[0].shape[0])]
            self.near = [remote(at(s, h), at(s, h), partner, snd, self.near_sem)
                         for s, h in ((lft, 0), (rgt, 1), (lft, 1), (rgt, 0))]
            self.last = [[remote(c, c, partner, snd, self.far_sem) for c in cut(at(far, h))] for h in (0, 1)]

        def early(self):
            for c in (*self.a0, *self.b1):
                c.start()

        def later(self):
            self.a1.start()
            self.b0.start()

        def to_partner(self):
            for c in self.p:
                c.start()

        def start(self):
            self.early()
            self.later()
            self.to_partner()

        def forward(self):
            arrived(self.at(self.lft, 0), self.a0_sem)
            for c in self.f0:
                c.start()
            self.near[0].start()
            arrived(self.at(self.rgt, 1), self.b1_sem)
            for c in self.f1:
                c.start()
            self.near[1].start()

        def second(self):
            arrived(self.span(1), self.second_sem)
            self.near[2].start()
            self.near[3].start()

        def third(self):
            for i, (c, d) in enumerate(zip(*self.last)):
                both = self.f_span(i)
                arrived(both, self.f_sem[i])
                c.start()
                d.start()

        def f_span(self, i):
            return self.span(1) if len(self.part) == 1 else self.two

        def own_ready(self):
            arrived(self.span(1), self.own_sem)

        def near_ready(self):
            arrived(self.span(2), self.near_sem)

        def far_ready(self):
            arrived(self.span(1), self.far_sem)

    class Gather4:
        def __init__(self, at, own, span, snd, share=None):
            lft, rgt = wrap(col - 1, ny), wrap(col + 1, ny)
            self.span = span
            first = new("recv")
            self.first_sem = first
            self.second_sem, self.third_sem = (new("recv"), new("recv")) if share is None else (share, share)
            self.a0 = remote(own(0), at(col, 0), y_plus, snd, first)
            self.b1 = remote(own(1), at(col, 1), y_minus, snd, first)
            self.a1 = remote(own(1), at(col, 1), y_plus, snd, self.second_sem)
            self.b0 = remote(own(0), at(col, 0), y_minus, snd, self.second_sem)
            self.f0 = remote(at(lft, 0), at(lft, 0), y_plus, snd, self.third_sem)
            self.f1 = remote(at(rgt, 1), at(rgt, 1), y_minus, snd, self.third_sem)

        def start(self):
            for c in (self.a0, self.b1, self.a1, self.b0):
                c.start()

        def forward(self):
            arrived(self.span(1), self.first_sem)
            self.f0.start()
            self.f1.start()

        def second(self):
            arrived(self.span(1), self.second_sem)

        def third(self):
            arrived(self.span(1), self.third_sem)

        def rest(self):
            arrived(self.span(2), self.second_sem)

    def peers():
        for dx in (1, nx - 1, 2, 0):
            for dc in (0, 1):
                if dx == 0 and dc == 0:
                    continue
                px = wrap(x + dx, nx)
                pc = core if dc == 0 else 1 - core
                yield 2 * px + pc, px, pc

    hk, qk = kb // 2, kb // 4
    sem_qr, sem_g, sem_mid, sem_r = [new("local"), new("local")], new("local"), new("local"), new("local")
    for i, (h, j) in enumerate(((0, 0), (1, 0), (0, 1), (1, 1))):
        local(qr_ref.at[pl.ds(h * hk + j * qk, qk)], qr_f.at[h, pl.ds(j * qk, qk)], sem_qr[i // 2])

    barrier = pltpu.get_barrier_semaphore()
    others = [r for r, _, _ in peers()]
    for r in others:
        pl.semaphore_signal(barrier, inc=1, device_id={"row": r}, device_id_type=MESH)
    for d in (y_plus, y_minus):
        pl.semaphore_signal(barrier, inc=1, device_id=d, device_id_type=MESH)

    load_ql = local(ql_ref, ql_f)
    for h in (0, 1):
        local(g_ref.at[:, pl.ds(h * kb, kb)], grow.at[2 * col + h], sem_g)

    def loaded(ref, sem):
        pltpu.make_async_remote_copy(
            src_ref=ref, dst_ref=ref, send_sem=send_sem.at[0], recv_sem=local_sem.at[sem],
            device_id=partner, device_id_type=MESH).wait_recv()

    def round_qr(j):
        loaded(qr_f.at[0], sem_qr[j])
        for h in (0, 1):
            qr_b[row, h, pl.ds(j * qk, qk)] = qr_f[h, pl.ds(j * qk, qk)].astype(BF16)

    round_qr(0)
    pl.semaphore_wait(barrier, len(others) + 2)

    gather_qr = Gather8(lambda s, h: qr_b.at[s, h], lambda h: qr_b.at[row, h], lambda n: qr_b.at[pl.ds(0, n)], snd_qr,
                        lambda ref: [ref.at[pl.ds(j * kb // 8, kb // 8)] for j in range(4)],
                        lambda ref: [ref.at[pl.ds(j * qk, qk)] for j in (0, 1)])
    gather_qr.a0[0].start()
    gather_qr.b1[0].start()
    round_qr(1)
    gather_qr.a0[1].start()
    gather_qr.b1[1].start()
    gather_qr.later()
    gather_qr.to_partner()
    gather_ql = Gather4(lambda s, h: ql_row.at[s, h], lambda h: ql_row.at[col, h], lambda n: ql_row.at[pl.ds(0, n)], snd_small, new("recv"))
    load_ql.wait()
    ql_row[col] = ql_f[...].astype(BF16).reshape(2, hr, lb)
    gather_ql.start()
    loaded(grow.at[pl.ds(0, 2)], sem_g)
    gather_g = Gather4(lambda s, h: grow.at[2 * s + h], lambda h: grow.at[2 * col + h],
                       lambda n: grow.at[pl.ds(0, 2 * n)], snd_g)
    gather_g.start()

    local(m_ref, mbuf, sem_mid)
    local(v_ref, vbuf, sem_mid)
    local(w_ref, wbuf, sem_mid)
    for h in (0, 1):
        local(g_ref.at[:, pl.ds(h * kb, kb)], gy.at[row, h], sem_mid)
        local(r_ref.at[:, pl.ds(h * kb, kb)], or_ref.at[h], sem_r)
    load_l = local(l_ref, ol_ref)

    def cast_block(s):
        growb[s] = grow[s].astype(BF16)

    for h in (0, 1):
        cast_block(2 * col + h)

    lft_c, rgt_c, far_c = wrap(col - 1, ny), wrap(col + 1, ny), wrap(col + 2, ny)
    x_lft, x_rgt, x_far = wrap(x - 1, nx), wrap(x + 1, nx), wrap(x + 2, nx)
    half_l = lb // 2
    quarter = pl.ds(pl.multiple_of(col * qb, qb), qb)
    row_far = wrap(row + 4, nrow)
    prow_far = row_far + 1 - 2 * core
    gather_ql.forward()
    gather_g.forward()
    gather_qr.forward()
    gather_ql.rest()

    for k in range(ny):
        block = ql_row[k].reshape(rb, lb)
        for h in (0, 1):
            ql_send[2 * k + h] = block[:, h * half_l:(h + 1) * half_l]
    ql_col[row, col] = ql_send[row, quarter]
    rcv_ql = new("recv")
    for r, _, _ in peers():
        remote(ql_send.at[r, quarter], ql_col.at[row, col], {"row": r}, snd_ql, rcv_ql).start()

    cast_block(2 * lft_c)
    cast_block(2 * rgt_c + 1)
    gather_g.second()
    cast_block(2 * lft_c + 1)
    cast_block(2 * rgt_c)
    gather_g.third()

    eb = qb // 2
    gx[row, col] = grow[row, quarter]
    rcv_gx, rest_gx = [new("recv") for _ in (0, 1)], new("recv")

    def send_gx(w):
        here = pl.ds(pl.multiple_of(col * qb + w * eb, eb), eb)
        for r, _, _ in peers():
            remote(grow.at[r, here], gx.at[row, col, pl.ds(w * eb, eb)], {"row": r}, snd_gx, rcv_gx[w]).start()

    def gather_wave(w):
        there, half = pl.ds(w * eb, eb), nrow // 2
        arrived(gx.at[pl.ds(0, nrow - 1), 0, pl.ds(0, eb)], rcv_gx[w])
        g = Gather4(lambda s, h: gx.at[pl.ds(h * half, half), s, there],
                    lambda h: gx.at[pl.ds(h * half, half), col, there],
                    lambda n: gx.at[:, pl.ds(0, n), there], snd_g, rest_gx)
        g.start()
        return g

    send_gx(0)

    def rows_of(w):
        return pl.ds(0, rb // 4) if w == 0 else pl.ds(rb // 4, rb - rb // 4)

    share_y = [new("recv") for _ in range(3)]

    gather_y = [Gather8(lambda s, h, w=w: gy.at[s, h, rows_of(w)], lambda h, w=w: grow.at[2 * col + h, rows_of(w)],
                        lambda n, w=w: gy.at[pl.ds(0, n), :, rows_of(w)], snd_rows, share=share_y) for w in (0, 1)]
    for g in gather_y:
        g.to_partner()
    cast_block(2 * far_c)
    cast_block(2 * far_c + 1)

    def turn(k):
        for j in range(4):
            qr_t[k, j] = qr_b[2 * k + j // 2, j % 2].T

    def h_part(r):
        return dot(growb[r], qr_b[r].reshape(kb, cb), NN)

    gather_qr.own_ready()
    acc[...] = h_part(2 * x) + h_part(2 * x + 1)
    gather_qr.second()
    gather_qr.near_ready()
    acc[...] += h_part(2 * x_lft) + h_part(2 * x_lft + 1)
    acc[...] += h_part(2 * x_rgt) + h_part(2 * x_rgt + 1)
    gather_qr.third()
    acc[...] += h_part(row_far)
    gather_qr.far_ready()
    hb[row] = (acc[...] + h_part(prow_far)).astype(BF16).reshape(2, hr, cb)

    def halves(ref):
        return [ref.at[pl.ds(j * hr // 2, hr // 2)] for j in (0, 1)]

    gather_h = Gather8(lambda s, h: hb.at[s, h], lambda h: hb.at[row, h], lambda n: hb.at[pl.ds(0, n)], snd_rows, halves)
    gather_h.early()
    gather_h.to_partner()
    turn(x_lft)
    turn(x_rgt)
    gather_h.later()

    arrived(ql_col.at[pl.ds(0, nrow - 1), 0], rcv_ql)
    gather_qc = Gather4(
        lambda s, h: ql_col.at[pl.ds(h * (nrow // 2), nrow // 2), s],
        lambda h: ql_col.at[pl.ds(h * (nrow // 2), nrow // 2), col],
        lambda n: ql_col.at[:, pl.ds(0, n)], snd_small, new("recv"))
    gather_qc.start()
    gather_qc.forward()
    gather_gx0 = gather_wave(0)

    def g_part(r):
        return dot(ql_col[r].reshape(rb, rb), hb[r].reshape(rb, cb), TN)

    def g_pair(cx):
        left = ql_col[pl.ds(2 * cx, 2)].reshape(2 * rb, rb)
        return dot(left, hb[pl.ds(2 * cx, 2)].reshape(2 * rb, cb), TN)

    gather_h.forward()
    send_gx(1)
    gather_y[0].early()
    gather_qc.rest()
    gather_h.own_ready()
    gacc[...] = g_pair(x)
    gather_h.second()
    gather_gx0.forward()
    gather_h.near_ready()
    gacc[...] += g_pair(x_lft)
    gacc[...] += g_pair(x_rgt)
    gather_h.third()
    gacc[...] += g_part(row_far)
    gather_h.far_ready()
    rotated = gacc[...] + g_part(prow_far)

    loaded(gy.at[pl.ds(0, 4)], sem_mid)
    gacc[...] = rotated
    gather_n = Gather8(lambda s, h: nb.at[s, h], lambda h: nb.at[row, h], lambda n: nb.at[pl.ds(0, n)], snd_rows,
                       halves, halves)
    for j in (0, 1):
        for h in (0, 1):
            part = pl.ds(h * hr + j * (hr // 2), hr // 2)
            turned = gacc[part]
            new_first = BETA1 * mbuf[part] + (1.0 - BETA1) * turned
            new_second = BETA2 * vbuf[part] + (1.0 - BETA2) * turned * turned
            below = BIAS_ONE * jnp.sqrt(new_second * (1.0 / BIAS_TWO)) + BIAS_ONE * EPS
            nb[row, h, pl.ds(j * (hr // 2), hr // 2)] = (new_first / below).astype(BF16)
            om_ref[part] = new_first
            ov_ref[part] = new_second
        gather_n.a0[j].start()
        gather_n.b1[j].start()
    gather_n.to_partner()
    turn(x)
    turn(x_far)
    gather_n.later()
    gather_gx1 = gather_wave(1)

    def k_part(r):
        return dot(ql_send[r], nb[r].reshape(rb, cb), NN)

    def k_pair(cx):
        return dot(ql_row[cx].reshape(rb, lb), nb[pl.ds(2 * cx, 2)].reshape(2 * rb, cb), NN)

    gather_n.own_ready()
    acc[...] = k_pair(x)
    gather_n.forward()
    gather_y[0].later()
    gather_y[1].early()
    gather_y[1].later()
    gather_gx1.forward()
    gather_n.second()
    gather_n.near_ready()
    acc[...] += k_pair(x_lft)
    acc[...] += k_pair(x_rgt)
    gather_n.third()
    acc[...] += k_part(row_far)
    gather_n.far_ready()
    back = (acc[...] + k_part(prow_far)).astype(BF16)

    rcv_u, rcv_f = new("recv"), [new("recv"), new("recv")]

    def half(k, h):
        return up.at[k, pl.ds(2 * h, 2)]

    u_far = [remote(half(far_c, 0), rin.at[0], y_plus, snd_u, rcv_f[0]),
             remote(half(far_c, 1), rin.at[1], y_minus, snd_u, rcv_f[1])]
    u_half = [remote(half(rgt_c, 1), rin.at[2], y_plus, snd_u, rcv_u),
              remote(half(lft_c, 0), rin.at[3], y_minus, snd_u, rcv_u)]
    u_sum = [remote(half(rgt_c, 0), rin.at[4], y_plus, snd_u, rcv_u),
             remote(half(lft_c, 1), rin.at[5], y_minus, snd_u, rcv_u)]

    def make_u(k):
        for j in range(4):
            up[k, j] = dot(back, qr_t[k, j], NN)

    make_u(far_c)
    for c in u_far:
        c.start()
    make_u(rgt_c)
    u_half[0].start()
    make_u(lft_c)
    u_half[1].start()
    gather_y[0].forward()
    make_u(col)

    arrived(gx.at[:, pl.ds(0, 2)], rest_gx)
    right_g = gx[pl.ds(2 * col, 2)].reshape(2 * rb, kb)
    lp[...] = dot(gx[...].reshape(nrow * rb, kb), right_g, NT, HIGHEST).reshape(nrow, rb, lb)
    rcv_s = new("recv")
    for k in range(nx):
        remote(lp.at[2 * k + 1 - core], lrecv.at[k], partner, snd_small, rcv_s).start()

    def add_r(cx, first=False):
        left = gx[pl.ds(2 * cx, 2)].reshape(2 * rb, kb)

        def body(h, _):
            part = dot(left, gy[pl.ds(2 * cx, 2), h].reshape(2 * rb, kb), TN, HIGHEST)
            old = or_ref[h]
            if first:
                old = BETA2 * old
            or_ref[h] = old + (1.0 - BETA2) * part
            return 0

        lax.fori_loop(0, 2, body, 0)

    gather_y[0].second()
    gather_y[1].forward()
    loaded(or_ref, sem_r)
    arrived(gy.at[pl.ds(0, 1)], share_y[0])
    add_r(x, True)

    arrived(rin.at[0], rcv_f[0])
    up[rgt_c, :2] = up[rgt_c, :2] + rin[0]
    u_sum[0].start()
    arrived(rin.at[1], rcv_f[1])
    up[lft_c, 2:] = up[lft_c, 2:] + rin[1]
    u_sum[1].start()

    arrived(lrecv, rcv_s)
    for k in range(nx):
        lp[2 * k + core] = lp[2 * k + core] + lrecv[k]
    rcv_l = new("recv")
    for dx in (1, nx - 1, 2):
        to = 2 * wrap(x + dx, nx) + core
        remote(lp.at[to], lx.at[x], {"row": to}, snd_small, rcv_l).start()

    gather_y[1].second()
    arrived(gy.at[pl.ds(0, 2)], share_y[1])
    add_r(x_lft)
    gather_y[0].third()
    add_r(x_rgt)
    gather_y[1].third()
    arrived(gy.at[pl.ds(0, 1)], share_y[2])
    add_r(x_far)

    load_l.wait()
    arrived(lx.at[pl.ds(0, nx - 1)], rcv_l)
    total = lp[row]
    for dx in (1, 2, 3):
        total = total + lx[wrap(x + dx, nx)]
    ol_ref[...] = BETA2 * ol_ref[...] + (1.0 - BETA2) * total

    arrived(rin.at[pl.ds(0, 4)], rcv_u)
    for j in range(4):
        cols = pl.ds(j * (cb // 4), cb // 4)
        others_sum = (rin[3, j] + rin[4, j]) if j < 2 else (rin[2, j - 2] + rin[5, j - 2])
        ow_ref[:, cols] = wbuf[:, cols] - LR * (up[col, j] + others_sum)

    assert tuple(counts.values()) == COUNTS
    for c in pending:
        c.wait_send()


def write_out(w_ref, m_ref, v_ref, l_ref, r_ref, ow_ref, om_ref, ov_ref, ol_ref, or_ref, sem):
    kb = r_ref.shape[1]
    part = kb // 4
    moves = [(r_ref.at[h, pl.ds(j * part, part)], or_ref.at[pl.ds(j * part, part), pl.ds(h * kb, kb)])
             for j in range(4) for h in (0, 1)]
    moves += [(w_ref, ow_ref), (m_ref, om_ref), (v_ref, ov_ref), (l_ref, ol_ref)]
    copies = [pltpu.make_async_copy(a, b, sem.at[i]) for i, (a, b) in enumerate(moves)]
    for c in copies:
        c.start()
    for c in copies:
        c.wait()


def solution(mesh):
    nx, ny = mesh.shape["row"] // 2, mesh.shape["col"]
    tile_spec = P(("layer", "row"), "col")

    def local_step(*args):
        rb, cb = args[0].shape
        kb = args[7].shape[0]
        lb = args[6].shape[1]
        hr, nr = rb // 2, 2 * nx
        vm = pltpu.VMEM
        shapes = [args[0], args[2], args[3], args[4], args[5]]
        held = pl.pallas_call(
            functools.partial(kernel, nx, ny),
            out_shape=tuple(vm(s, F32) for s in [(rb, cb)] * 3 + [(rb, lb), (2, kb, kb)]),
            in_specs=[pl.BlockSpec(memory_space=pl.ANY)] * 8,
            out_specs=tuple([pl.BlockSpec(memory_space=pltpu.VMEM)] * 5),
            scratch_shapes=[
                vm((2, kb // 2, cb), F32),
                vm((nr, 2, kb // 2, cb), BF16),
                vm((nx, 4, cb, kb // 2), BF16),
                vm((nr, rb, kb), F32),
                vm((nr, rb, kb), BF16),
                vm((rb, lb), F32),
                vm((ny, 2, hr, lb), BF16),
                vm((nr, rb, lb // 2), BF16),
                vm((nr, ny, rb // ny, lb // 2), BF16),
                vm((nr, ny, rb // ny, kb), F32),
                vm((nr, 2, rb, kb), F32),
                vm((nr, 2, hr, cb), BF16),
                vm((nr, 2, hr, cb), BF16),
                vm((rb, cb), F32),
                vm((rb, cb), F32),
                vm((ny, 4, rb, cb // 4), F32),
                vm((6, 2, rb, cb // 4), F32),
                vm((nr, rb, lb), F32),
                vm((nx, rb, lb), F32),
                vm((nx, rb, lb), F32),
                vm((rb, cb), F32),
                vm((rb, cb), F32),
                vm((rb, cb), F32),
                *[pltpu.SemaphoreType.DMA((n,)) for n in COUNTS],
            ],
            compiler_params=pltpu.CompilerParams(
                collective_id=0, has_side_effects=True, vmem_limit_bytes=61600 * 1024),
        )(*args)
        return pl.pallas_call(
            write_out,
            out_shape=tuple(jax.ShapeDtypeStruct(s.shape, s.dtype) for s in shapes),
            in_specs=[pl.BlockSpec(memory_space=pltpu.VMEM)] * 5,
            out_specs=tuple([pl.BlockSpec(memory_space=pl.ANY)] * 5),
            scratch_shapes=[pltpu.SemaphoreType.DMA((12,))],
            compiler_params=pltpu.CompilerParams(vmem_limit_bytes=4 * 1024 * 1024),
        )(*held)

    return jax.shard_map(local_step, mesh=mesh, in_specs=(tile_spec,) * 8, out_specs=(tile_spec,) * 5, check_vma=False)
```

```python
import functools

import jax
import jax.numpy as jnp
from jax import lax
from jax.experimental import pallas as pl
from jax.experimental.pallas import tpu as pltpu
from jax.sharding import PartitionSpec as P

BETA1 = 0.9
BETA2 = 0.9
EPS = 1e-8
LR = 0.1
STEP = 10
BIAS_ONE = 1.0 - BETA1 ** STEP
BIAS_TWO = 1.0 - BETA2 ** STEP
MESH = pl.DeviceIdType.MESH
HIGHEST = lax.Precision.HIGHEST
F32 = jnp.float32
BF16 = jnp.bfloat16
NN = (((1,), (0,)), ((), ()))
TN = (((0,), (0,)), ((), ()))
NT = (((1,), (1,)), ((), ()))
COUNTS = (7, 55, 7)


def dot(a, b, dims, precision=None):
    return lax.dot_general(a, b, dims, precision=precision, preferred_element_type=F32)


def kernel(nx, ny, w_ref, g_ref, m_ref, v_ref, l_ref, r_ref, ql_ref, qr_ref,
           ow_ref, om_ref, ov_ref, ol_ref, or_ref,
           qr_f, qr_b, qr_t, grow, growb, ql_f, ql_row, ql_send, ql_col, gx, gy, hb, nb,
           acc, gacc, up, rin, lp, lrecv, lx, wbuf, mbuf, vbuf,
           send_sem, recv_sem, local_sem):
    row = lax.axis_index("row")
    col = lax.axis_index("col")
    core = lax.rem(row, 2)
    x = lax.div(row, 2)
    nrow = 2 * nx
    rb, cb = w_ref.shape
    kb = qr_ref.shape[0]
    lb = ql_ref.shape[1]
    hr = rb // 2
    qb = rb // ny

    def wrap(v, n):
        return lax.rem(v + n, n)

    x_plus = {"row": wrap(row + 2, nrow)}
    x_minus = {"row": wrap(row - 2, nrow)}
    partner = {"row": row + 1 - 2 * core}
    y_plus = {"col": wrap(col + 1, ny)}
    y_minus = {"col": wrap(col - 1, ny)}
    prow = row + 1 - 2 * core
    counts = {"send": 0, "recv": 0, "local": 0}
    pending = []

    def new(kind):
        counts[kind] += 1
        return counts[kind] - 1

    def remote(src, dst, device, send, recv=None):
        recv = new("recv") if recv is None else recv
        return pltpu.make_async_remote_copy(
            src_ref=src, dst_ref=dst, send_sem=send_sem.at[send], recv_sem=recv_sem.at[recv],
            device_id=device, device_id_type=MESH)

    def sends(span):
        i = new("send")
        pending.append(remote(span, span, partner, i, 0))
        return i

    snd_qr, snd_rows = sends(qr_b.at[pl.ds(0, nrow - 1)]), sends(qr_b.at[pl.ds(0, nrow - 1)])
    snd_g, snd_small = sends(qr_b.at[pl.ds(0, 3)]), sends(gx.at[pl.ds(0, 5)])
    snd_ql, snd_gx = sends(ql_col.at[pl.ds(0, nrow - 1), 0]), sends(gx.at[pl.ds(0, nrow - 1), 0])
    snd_u = sends(rin)

    def arrived(span, recv):
        remote(span, span, partner, 0, recv).wait_recv()

    def local(src, dst, sem=None):
        copy = pltpu.make_async_copy(src, dst, local_sem.at[new("local") if sem is None else sem])
        copy.start()
        return copy

    class Gather8:
        def __init__(self, at, own, span, snd, cut=lambda ref: [ref], first=lambda ref: [ref], share=None):
            lft, rgt, far = wrap(row - 2, nrow), wrap(row + 2, nrow), wrap(row + 4, nrow)
            self.span = span
            self.at, self.lft, self.rgt = at, lft, rgt
            self.second_sem, self.a0_sem, self.b1_sem = (new("recv") for _ in range(3))
            self.own_sem, self.near_sem, self.far_sem = share or [new("recv") for _ in range(3)]
            self.a0 = [remote(c, d, x_plus, snd, self.a0_sem) for c, d in zip(first(own(0)), first(at(row, 0)))]
            self.b1 = [remote(c, d, x_minus, snd, self.b1_sem) for c, d in zip(first(own(1)), first(at(row, 1)))]
            self.a1 = remote(own(1), at(row, 1), x_plus, snd, self.second_sem)
            self.b0 = remote(own(0), at(row, 0), x_minus, snd, self.second_sem)
            self.p = [remote(own(h), at(row, h), partner, snd, self.own_sem) for h in (0, 1)]
            self.f_sem = [new("recv") for _ in cut(at(lft, 0))]
            self.f0 = [remote(c, c, x_plus, snd, i) for c, i in zip(cut(at(lft, 0)), self.f_sem)]
            self.f1 = [remote(c, c, x_minus, snd, i) for c, i in zip(cut(at(rgt, 1)), self.f_sem)]
            self.part = cut(at(far, 0))
            if len(self.part) > 1:
                self.two = at(far, 0).at[pl.ds(0, 2 * self.part[0].shape[0])]
            self.near = [remote(at(s, h), at(s, h), partner, snd, self.near_sem)
                         for s, h in ((lft, 0), (rgt, 1), (lft, 1), (rgt, 0))]
            self.last = [[remote(c, c, partner, snd, self.far_sem) for c in cut(at(far, h))] for h in (0, 1)]

        def early(self):
            for c in (*self.a0, *self.b1):
                c.start()

        def later(self):
            self.a1.start()
            self.b0.start()

        def to_partner(self):
            for c in self.p:
                c.start()

        def start(self):
            self.early()
            self.later()
            self.to_partner()

        def forward(self):
            arrived(self.at(self.lft, 0), self.a0_sem)
            for c in self.f0:
                c.start()
            self.near[0].start()
            arrived(self.at(self.rgt, 1), self.b1_sem)
            for c in self.f1:
                c.start()
            self.near[1].start()

        def second(self):
            arrived(self.span(1), self.second_sem)
            self.near[2].start()
            self.near[3].start()

        def third(self):
            for i, (c, d) in enumerate(zip(*self.last)):
                both = self.f_span(i)
                arrived(both, self.f_sem[i])
                c.start()
                d.start()

        def f_span(self, i):
            return self.span(1) if len(self.part) == 1 else self.two

        def own_ready(self):
            arrived(self.span(1), self.own_sem)

        def near_ready(self):
            arrived(self.span(2), self.near_sem)

        def far_ready(self):
            arrived(self.span(1), self.far_sem)

    class Gather4:
        def __init__(self, at, own, span, snd, share=None):
            lft, rgt = wrap(col - 1, ny), wrap(col + 1, ny)
            self.span = span
            first = new("recv")
            self.first_sem = first
            self.second_sem, self.third_sem = (new("recv"), new("recv")) if share is None else (share, share)
            self.a0 = remote(own(0), at(col, 0), y_plus, snd, first)
            self.b1 = remote(own(1), at(col, 1), y_minus, snd, first)
            self.a1 = remote(own(1), at(col, 1), y_plus, snd, self.second_sem)
            self.b0 = remote(own(0), at(col, 0), y_minus, snd, self.second_sem)
            self.f0 = remote(at(lft, 0), at(lft, 0), y_plus, snd, self.third_sem)
            self.f1 = remote(at(rgt, 1), at(rgt, 1), y_minus, snd, self.third_sem)

        def start(self):
            for c in (self.a0, self.b1, self.a1, self.b0):
                c.start()

        def forward(self):
            arrived(self.span(1), self.first_sem)
            self.f0.start()
            self.f1.start()

        def second(self):
            arrived(self.span(1), self.second_sem)

        def third(self):
            arrived(self.span(1), self.third_sem)

        def rest(self):
            arrived(self.span(2), self.second_sem)

    def peers():
        for dx in (1, nx - 1, 2, 0):
            for dc in (0, 1):
                if dx == 0 and dc == 0:
                    continue
                px = wrap(x + dx, nx)
                pc = core if dc == 0 else 1 - core
                yield 2 * px + pc, px, pc

    hk, qk = kb // 2, kb // 4
    sem_qr, sem_g, sem_mid, sem_r = [new("local"), new("local")], new("local"), new("local"), new("local")
    for i, (h, j) in enumerate(((0, 0), (1, 0), (0, 1), (1, 1))):
        local(qr_ref.at[pl.ds(h * hk + j * qk, qk)], qr_f.at[h, pl.ds(j * qk, qk)], sem_qr[i // 2])

    barrier = pltpu.get_barrier_semaphore()
    others = [r for r, _, _ in peers()]
    for r in others:
        pl.semaphore_signal(barrier, inc=1, device_id={"row": r}, device_id_type=MESH)
    for d in (y_plus, y_minus):
        pl.semaphore_signal(barrier, inc=1, device_id=d, device_id_type=MESH)

    load_ql = local(ql_ref, ql_f)
    for h in (0, 1):
        local(g_ref.at[:, pl.ds(h * kb, kb)], grow.at[2 * col + h], sem_g)

    def loaded(ref, sem):
        pltpu.make_async_remote_copy(
            src_ref=ref, dst_ref=ref, send_sem=send_sem.at[0], recv_sem=local_sem.at[sem],
            device_id=partner, device_id_type=MESH).wait_recv()

    def round_qr(j):
        loaded(qr_f.at[0], sem_qr[j])
        for h in (0, 1):
            qr_b[row, h, pl.ds(j * qk, qk)] = qr_f[h, pl.ds(j * qk, qk)].astype(BF16)

    round_qr(0)
    pl.semaphore_wait(barrier, len(others) + 2)

    gather_qr = Gather8(lambda s, h: qr_b.at[s, h], lambda h: qr_b.at[row, h], lambda n: qr_b.at[pl.ds(0, n)], snd_qr,
                        lambda ref: [ref.at[pl.ds(j * kb // 8, kb // 8)] for j in range(4)],
                        lambda ref: [ref.at[pl.ds(j * qk, qk)] for j in (0, 1)])
    gather_qr.a0[0].start()
    gather_qr.b1[0].start()
    round_qr(1)
    gather_qr.a0[1].start()
    gather_qr.b1[1].start()
    gather_qr.later()
    gather_qr.to_partner()
    gather_ql = Gather4(lambda s, h: ql_row.at[s, h], lambda h: ql_row.at[col, h], lambda n: ql_row.at[pl.ds(0, n)], snd_small, new("recv"))
    load_ql.wait()
    ql_row[col] = ql_f[...].astype(BF16).reshape(2, hr, lb)
    gather_ql.start()
    loaded(grow.at[pl.ds(0, 2)], sem_g)
    gather_g = Gather4(lambda s, h: grow.at[2 * s + h], lambda h: grow.at[2 * col + h],
                       lambda n: grow.at[pl.ds(0, 2 * n)], snd_g)
    gather_g.start()

    local(m_ref, mbuf, sem_mid)
    local(v_ref, vbuf, sem_mid)
    local(w_ref, wbuf, sem_mid)
    for h in (0, 1):
        local(g_ref.at[:, pl.ds(h * kb, kb)], gy.at[row, h], sem_mid)
        local(r_ref.at[:, pl.ds(h * kb, kb)], or_ref.at[h], sem_r)
    load_l = local(l_ref, ol_ref)

    def cast_block(s):
        growb[s] = grow[s].astype(BF16)

    for h in (0, 1):
        cast_block(2 * col + h)

    lft_c, rgt_c, far_c = wrap(col - 1, ny), wrap(col + 1, ny), wrap(col + 2, ny)
    x_lft, x_rgt, x_far = wrap(x - 1, nx), wrap(x + 1, nx), wrap(x + 2, nx)
    half_l = lb // 2
    quarter = pl.ds(pl.multiple_of(col * qb, qb), qb)
    row_far = wrap(row + 4, nrow)
    prow_far = row_far + 1 - 2 * core
    gather_ql.forward()
    gather_g.forward()
    gather_qr.forward()
    gather_ql.rest()

    for k in range(ny):
        block = ql_row[k].reshape(rb, lb)
        for h in (0, 1):
            ql_send[2 * k + h] = block[:, h * half_l:(h + 1) * half_l]
    ql_col[row, col] = ql_send[row, quarter]
    rcv_ql = new("recv")
    for r, _, _ in peers():
        remote(ql_send.at[r, quarter], ql_col.at[row, col], {"row": r}, snd_ql, rcv_ql).start()

    cast_block(2 * lft_c)
    cast_block(2 * rgt_c + 1)
    gather_g.second()
    cast_block(2 * lft_c + 1)
    cast_block(2 * rgt_c)
    gather_g.third()

    eb = qb // 2
    gx[row, col] = grow[row, quarter]
    rcv_gx, rest_gx = [new("recv") for _ in (0, 1)], new("recv")

    def send_gx(w):
        here = pl.ds(pl.multiple_of(col * qb + w * eb, eb), eb)
        for r, _, _ in peers():
            remote(grow.at[r, here], gx.at[row, col, pl.ds(w * eb, eb)], {"row": r}, snd_gx, rcv_gx[w]).start()

    def gather_wave(w):
        there, half = pl.ds(w * eb, eb), nrow // 2
        arrived(gx.at[pl.ds(0, nrow - 1), 0, pl.ds(0, eb)], rcv_gx[w])
        g = Gather4(lambda s, h: gx.at[pl.ds(h * half, half), s, there],
                    lambda h: gx.at[pl.ds(h * half, half), col, there],
                    lambda n: gx.at[:, pl.ds(0, n), there], snd_g, rest_gx)
        g.start()
        return g

    send_gx(0)

    def rows_of(w):
        return pl.ds(w * hr, hr)

    share_y = [new("recv") for _ in range(3)]

    gather_y = [Gather8(lambda s, h, w=w: gy.at[s, h, rows_of(w)], lambda h, w=w: grow.at[2 * col + h, rows_of(w)],
                        lambda n, w=w: gy.at[pl.ds(0, n), :, rows_of(w)], snd_rows, share=share_y) for w in (0, 1)]
    for g in gather_y:
        g.to_partner()
    cast_block(2 * far_c)
    cast_block(2 * far_c + 1)

    def turn(k):
        for j in range(4):
            qr_t[k, j] = qr_b[2 * k + j // 2, j % 2].T

    def h_part(r):
        return dot(growb[r], qr_b[r].reshape(kb, cb), NN)

    gather_qr.own_ready()
    acc[...] = h_part(2 * x) + h_part(2 * x + 1)
    gather_qr.second()
    gather_qr.near_ready()
    acc[...] += h_part(2 * x_lft) + h_part(2 * x_lft + 1)
    acc[...] += h_part(2 * x_rgt) + h_part(2 * x_rgt + 1)
    turn(x)
    turn(x_lft)
    turn(x_rgt)
    gather_qr.third()
    acc[...] += h_part(row_far)
    gather_qr.far_ready()
    hb[row] = (acc[...] + h_part(prow_far)).astype(BF16).reshape(2, hr, cb)

    def halves(ref):
        return [ref.at[pl.ds(j * hr // 2, hr // 2)] for j in (0, 1)]

    gather_h = Gather8(lambda s, h: hb.at[s, h], lambda h: hb.at[row, h], lambda n: hb.at[pl.ds(0, n)], snd_rows, halves)
    gather_h.start()

    arrived(ql_col.at[pl.ds(0, nrow - 1), 0], rcv_ql)
    gather_qc = Gather4(
        lambda s, h: ql_col.at[pl.ds(h * (nrow // 2), nrow // 2), s],
        lambda h: ql_col.at[pl.ds(h * (nrow // 2), nrow // 2), col],
        lambda n: ql_col.at[:, pl.ds(0, n)], snd_small, new("recv"))
    gather_qc.start()
    gather_qc.forward()
    gather_gx0 = gather_wave(0)

    def g_part(r):
        return dot(ql_col[r].reshape(rb, rb), hb[r].reshape(rb, cb), TN)

    def g_pair(cx):
        left = ql_col[pl.ds(2 * cx, 2)].reshape(2 * rb, rb)
        return dot(left, hb[pl.ds(2 * cx, 2)].reshape(2 * rb, cb), TN)

    gather_h.forward()
    send_gx(1)
    gather_y[0].early()
    turn(x_far)
    gather_qc.rest()
    gather_h.own_ready()
    gacc[...] = g_pair(x)
    gather_h.second()
    gather_gx0.forward()
    gather_h.near_ready()
    gacc[...] += g_pair(x_lft)
    gacc[...] += g_pair(x_rgt)
    gather_h.third()
    gacc[...] += g_part(row_far)
    gather_h.far_ready()
    rotated = gacc[...] + g_part(prow_far)

    loaded(gy.at[pl.ds(0, 4)], sem_mid)
    gacc[...] = rotated
    gather_n = Gather8(lambda s, h: nb.at[s, h], lambda h: nb.at[row, h], lambda n: nb.at[pl.ds(0, n)], snd_rows,
                       halves, halves)
    for j in (0, 1):
        for h in (0, 1):
            part = pl.ds(h * hr + j * (hr // 2), hr // 2)
            turned = gacc[part]
            new_first = BETA1 * mbuf[part] + (1.0 - BETA1) * turned
            new_second = BETA2 * vbuf[part] + (1.0 - BETA2) * turned * turned
            below = BIAS_ONE * jnp.sqrt(new_second * (1.0 / BIAS_TWO)) + BIAS_ONE * EPS
            nb[row, h, pl.ds(j * (hr // 2), hr // 2)] = (new_first / below).astype(BF16)
            om_ref[part] = new_first
            ov_ref[part] = new_second
        gather_n.a0[j].start()
        gather_n.b1[j].start()
    gather_n.later()
    gather_n.to_partner()
    gather_gx1 = gather_wave(1)

    def k_part(r):
        return dot(ql_send[r], nb[r].reshape(rb, cb), NN)

    def k_pair(cx):
        return dot(ql_row[cx].reshape(rb, lb), nb[pl.ds(2 * cx, 2)].reshape(2 * rb, cb), NN)

    gather_n.own_ready()
    acc[...] = k_pair(x)
    gather_n.forward()
    gather_y[0].later()
    gather_y[1].early()
    gather_y[1].later()
    gather_gx1.forward()
    gather_n.second()
    gather_n.near_ready()
    acc[...] += k_pair(x_lft)
    acc[...] += k_pair(x_rgt)
    gather_n.third()
    acc[...] += k_part(row_far)
    gather_n.far_ready()
    back = (acc[...] + k_part(prow_far)).astype(BF16)

    rcv_u, rcv_f = new("recv"), [new("recv"), new("recv")]

    def half(k, h):
        return up.at[k, pl.ds(2 * h, 2)]

    u_far = [remote(half(far_c, 0), rin.at[0], y_plus, snd_u, rcv_f[0]),
             remote(half(far_c, 1), rin.at[1], y_minus, snd_u, rcv_f[1])]
    u_half = [remote(half(rgt_c, 1), rin.at[2], y_plus, snd_u, rcv_u),
              remote(half(lft_c, 0), rin.at[3], y_minus, snd_u, rcv_u)]
    u_sum = [remote(half(rgt_c, 0), rin.at[4], y_plus, snd_u, rcv_u),
             remote(half(lft_c, 1), rin.at[5], y_minus, snd_u, rcv_u)]

    def make_u(k):
        for j in range(4):
            up[k, j] = dot(back, qr_t[k, j], NN)

    make_u(far_c)
    for c in u_far:
        c.start()
    make_u(rgt_c)
    u_half[0].start()
    make_u(lft_c)
    u_half[1].start()
    gather_y[0].forward()
    make_u(col)

    arrived(gx.at[:, pl.ds(0, 2)], rest_gx)
    right_g = gx[pl.ds(2 * col, 2)].reshape(2 * rb, kb)
    lp[...] = dot(gx[...].reshape(nrow * rb, kb), right_g, NT, HIGHEST).reshape(nrow, rb, lb)
    rcv_s = new("recv")
    for k in range(nx):
        remote(lp.at[2 * k + 1 - core], lrecv.at[k], partner, snd_small, rcv_s).start()

    def add_r(cx, first=False):
        left = gx[pl.ds(2 * cx, 2)].reshape(2 * rb, kb)

        def body(h, _):
            part = dot(left, gy[pl.ds(2 * cx, 2), h].reshape(2 * rb, kb), TN, HIGHEST)
            old = or_ref[h]
            if first:
                old = BETA2 * old
            or_ref[h] = old + (1.0 - BETA2) * part
            return 0

        lax.fori_loop(0, 2, body, 0)

    gather_y[0].second()
    gather_y[1].forward()
    loaded(or_ref, sem_r)
    arrived(gy.at[pl.ds(0, 1)], share_y[0])
    add_r(x, True)

    arrived(rin.at[0], rcv_f[0])
    up[rgt_c, :2] = up[rgt_c, :2] + rin[0]
    u_sum[0].start()
    arrived(rin.at[1], rcv_f[1])
    up[lft_c, 2:] = up[lft_c, 2:] + rin[1]
    u_sum[1].start()

    arrived(lrecv, rcv_s)
    for k in range(nx):
        lp[2 * k + core] = lp[2 * k + core] + lrecv[k]
    rcv_l = new("recv")
    for dx in (1, nx - 1, 2):
        to = 2 * wrap(x + dx, nx) + core
        remote(lp.at[to], lx.at[x], {"row": to}, snd_small, rcv_l).start()

    gather_y[1].second()
    arrived(gy.at[pl.ds(0, 2)], share_y[1])
    add_r(x_lft)
    gather_y[0].third()
    add_r(x_rgt)
    gather_y[1].third()
    arrived(gy.at[pl.ds(0, 1)], share_y[2])
    add_r(x_far)

    load_l.wait()
    arrived(lx.at[pl.ds(0, nx - 1)], rcv_l)
    total = lp[row]
    for dx in (1, 2, 3):
        total = total + lx[wrap(x + dx, nx)]
    ol_ref[...] = BETA2 * ol_ref[...] + (1.0 - BETA2) * total

    arrived(rin.at[pl.ds(0, 4)], rcv_u)
    for j in range(4):
        cols = pl.ds(j * (cb // 4), cb // 4)
        others_sum = (rin[3, j] + rin[4, j]) if j < 2 else (rin[2, j - 2] + rin[5, j - 2])
        ow_ref[:, cols] = wbuf[:, cols] - LR * (up[col, j] + others_sum)

    assert tuple(counts.values()) == COUNTS
    for c in pending:
        c.wait_send()


def write_out(w_ref, m_ref, v_ref, l_ref, r_ref, ow_ref, om_ref, ov_ref, ol_ref, or_ref, sem):
    kb = r_ref.shape[1]
    moves = [(w_ref, ow_ref), (m_ref, om_ref), (v_ref, ov_ref), (l_ref, ol_ref)]
    moves += [(r_ref.at[h], or_ref.at[:, pl.ds(h * kb, kb)]) for h in (0, 1)]
    copies = [pltpu.make_async_copy(a, b, sem.at[i]) for i, (a, b) in enumerate(moves)]
    for c in copies:
        c.start()
    for c in copies:
        c.wait()


def solution(mesh):
    nx, ny = mesh.shape["row"] // 2, mesh.shape["col"]
    tile_spec = P(("layer", "row"), "col")

    def local_step(*args):
        rb, cb = args[0].shape
        kb = args[7].shape[0]
        lb = args[6].shape[1]
        hr, nr = rb // 2, 2 * nx
        vm = pltpu.VMEM
        shapes = [args[0], args[2], args[3], args[4], args[5]]
        held = pl.pallas_call(
            functools.partial(kernel, nx, ny),
            out_shape=tuple(vm(s, F32) for s in [(rb, cb)] * 3 + [(rb, lb), (2, kb, kb)]),
            in_specs=[pl.BlockSpec(memory_space=pl.ANY)] * 8,
            out_specs=tuple([pl.BlockSpec(memory_space=pltpu.VMEM)] * 5),
            scratch_shapes=[
                vm((2, kb // 2, cb), F32),
                vm((nr, 2, kb // 2, cb), BF16),
                vm((nx, 4, cb, kb // 2), BF16),
                vm((nr, rb, kb), F32),
                vm((nr, rb, kb), BF16),
                vm((rb, lb), F32),
                vm((ny, 2, hr, lb), BF16),
                vm((nr, rb, lb // 2), BF16),
                vm((nr, ny, rb // ny, lb // 2), BF16),
                vm((nr, ny, rb // ny, kb), F32),
                vm((nr, 2, rb, kb), F32),
                vm((nr, 2, hr, cb), BF16),
                vm((nr, 2, hr, cb), BF16),
                vm((rb, cb), F32),
                vm((rb, cb), F32),
                vm((ny, 4, rb, cb // 4), F32),
                vm((6, 2, rb, cb // 4), F32),
                vm((nr, rb, lb), F32),
                vm((nx, rb, lb), F32),
                vm((nx, rb, lb), F32),
                vm((rb, cb), F32),
                vm((rb, cb), F32),
                vm((rb, cb), F32),
                *[pltpu.SemaphoreType.DMA((n,)) for n in COUNTS],
            ],
            compiler_params=pltpu.CompilerParams(
                collective_id=0, has_side_effects=True, vmem_limit_bytes=61600 * 1024),
        )(*args)
        return pl.pallas_call(
            write_out,
            out_shape=tuple(jax.ShapeDtypeStruct(s.shape, s.dtype) for s in shapes),
            in_specs=[pl.BlockSpec(memory_space=pltpu.VMEM)] * 5,
            out_specs=tuple([pl.BlockSpec(memory_space=pl.ANY)] * 5),
            scratch_shapes=[pltpu.SemaphoreType.DMA((6,))],
            compiler_params=pltpu.CompilerParams(vmem_limit_bytes=4 * 1024 * 1024),
        )(*held)

    return jax.shard_map(local_step, mesh=mesh, in_specs=(tile_spec,) * 8, out_specs=(tile_spec,) * 5, check_vma=False)
```
